32 devices in a mesh: dp: 8 (over z, x), ctx: 4 (over y, core).
Axes of the slice: x: 2, y: 2, z: 4, core: 2. Of those that a mesh axis runs over, the one named last changes fastest.
Arguments:
- inputs: bfloat16 [16, 1024, 1536], P('dp', 'ctx'), may hold values from -6 to 6
- segments: int32 [16, 1024], P('dp', 'ctx'), may hold values from 0 to 5, never falling along the last dimension, each value on 1 to 512 neighbouring positions
- cotangent: bfloat16 [16, 1024, 1536], P('dp', 'ctx'), may hold values from -6 to 6
- w_query: bfloat16 [1536, 1536], P(('dp', 'ctx')), may hold values from -4 to 4
- w_key: bfloat16 [1536, 768], P(('dp', 'ctx')), may hold values from -0.15625 to 0.15625
- w_value: bfloat16 [1536, 768], P(('dp', 'ctx')), may hold values from -0.15625 to 0.15625
- w_out: bfloat16 [1536, 1536], P(('dp', 'ctx')), may hold values from -0.625 to 0.625
- w_gate: bfloat16 [1536, 4096], P(('dp', 'ctx')), may hold values from -0.15625 to 0.15625
- w_up: bfloat16 [1536, 4096], P(('dp', 'ctx')), may hold values from -0.15625 to 0.15625
- w_down: bfloat16 [4096, 1536], P(('dp', 'ctx')), may hold values from -0.09375 to 0.09375
- gain_attn: bfloat16 [1536], P(('dp', 'ctx')), may hold values from 0.5 to 1.5
- gain_ffn: bfloat16 [1536], P(('dp', 'ctx')), may hold values from 0.5 to 1.5
Outputs:
- outputs: float32 [16, 1024, 1536], P('dp', 'ctx')
- input_grad: float32 [16, 1024, 1536], P('dp', 'ctx')
- grad_query: float32 [1536, 1536], P(('dp', 'ctx'))
- grad_key: float32 [1536, 768], P(('dp', 'ctx'))
- grad_value: float32 [1536, 768], P(('dp', 'ctx'))
- grad_out: float32 [1536, 1536], P(('dp', 'ctx'))
- grad_gate: float32 [1536, 4096], P(('dp', 'ctx'))
- grad_up: float32 [1536, 4096], P(('dp', 'ctx'))
- grad_down: float32 [4096, 1536], P(('dp', 'ctx'))
- grad_gain_attn: float32 [1536], P(('dp', 'ctx'))
- grad_gain_ffn: float32 [1536], P(('dp', 'ctx'))
The draws below stay inside these ranges and needn't reach their ends.
Inputs may be any that keep to these rules, and one draw needn't show every extreme that they name: `segments`: within each sequence the ids never fall; each document spans 1 to 512 tokens, and one spans exactly 512.
All inputs are finite; a program needn't handle non-finite values.
Results may differ from the reference program's by a relative error of at most 0.02.
The reference program's roundings to bfloat16 on the way (of `normed_attn`, `probs`, `attended`, `normed_ffn`, `hidden`, `d_mid_low`, `d_attended` and `d_scores`) count: a program that leaves them out, or rounds other values in their place, can miss the bound.
Values may be sent and summed in bfloat16 or wider, within the bound.
A program may use at most 384 MiB of HBM per device.

```python
import math
import jax
import jax.numpy as jnp
import numpy as np
from jax import lax

D = 1536
FF = 4096
H = 16
KV = 8
HD = 96
LENGTH = 1024
DOCS = 6
SEQS = 16


def draw_w_query(key, part):
    base = jax.random.normal(jax.random.fold_in(key, 11), (D, H * HD), jnp.float32)
    head_scale = jnp.exp(jax.random.uniform(jax.random.fold_in(key, 12), (H,), jnp.float32, math.log(0.5), math.log(2.0)))
    columns = jnp.repeat(head_scale, HD)
    scaled = base * columns[None, :] * D ** (-0.5)
    return jnp.clip(scaled, -4.0, 4.0).astype(jnp.bfloat16)


def block_levels(own_key, extent, pieces, low, high):
    loudness, own = 1.0, jax.random.fold_in(own_key, 6)
    for position, parts in pieces:
        steps = jnp.exp(jax.random.uniform(jax.random.fold_in(own, position), (parts,), jnp.float32, low / len(pieces), high / len(pieces)))
        loudness = loudness * jnp.repeat(steps, extent[position] // parts).reshape([-1 if axis == position else 1 for axis in range(len(extent))])
    return loudness


def split_up(count, total, reach, lean):
    portions = [(1 << 20) // math.isqrt(rank ** lean) + 1 for rank in range(2, count + 1)]
    surplus, counts = total - reach - (count - 1), [1] * (count - 1)
    while surplus > 0:
        movable = [i for i in range(count - 1) if counts[i] < reach]
        pool, remaining = sum([portions[i] for i in movable]), surplus
        for i in movable:
            more = min(reach - counts[i], max(1, remaining * portions[i] // pool), surplus)
            counts[i] = counts[i] + more
            surplus = surplus - more
    return np.array([reach] + counts)


def uneven_parts(key, number_of, total, most, slope):
    if number_of == 2:
        one = jax.random.randint(key, (), max(1, total - most), min(most, total - 1) + 1)
        return jnp.stack([one, total - one])
    tallies = jnp.asarray(split_up(number_of, total, most, slope), jnp.int32)
    pairs = (number_of - 1) // 2
    source_of, sink = tallies[1:1 + 2 * pairs:2], tallies[2:2 + 2 * pairs:2]
    room = jnp.minimum(source_of - 1, most - sink)
    shifted = jax.random.randint(jax.random.fold_in(key, 1), (pairs,), 0, 1 << 20) % (room + 1)
    tallies = tallies.at[1:1 + 2 * pairs:2].set(source_of - shifted).at[2:2 + 2 * pairs:2].set(sink + shifted)
    return tallies[jax.random.permutation(jax.random.fold_in(key, 2), number_of)]


def normal_values(rng, shape, width, limit, split=(), kind=jnp.bfloat16):
    level = block_levels(rng, shape, split, -0.22, 0.18) if split else 1.0
    values = jax.random.normal(rng, shape, jnp.float32) * width * level
    return jnp.minimum(jnp.maximum(values, -limit), limit).astype(kind)


def setup_inputs(seed: int = 0) -> dict:
    streams_of = jax.random.split(jax.random.key(seed), 13)
    inputs = normal_values(streams_of[0], (SEQS, LENGTH, D), 1.0, 6.0, ((0, 8), (1, 4)))
    segments = jax.vmap(lambda own: jnp.searchsorted(jnp.cumsum(uneven_parts(own, DOCS, LENGTH, LENGTH // 2, 1)), jnp.arange(LENGTH), side="right"))(jax.random.split(streams_of[1], SEQS)).reshape((SEQS, LENGTH)).astype(jnp.int32)
    cotangent = normal_values(streams_of[2], (SEQS, LENGTH, D), 1.0, 6.0, ((0, 8), (1, 4)))
    w_query = draw_w_query(jax.random.fold_in(streams_of[12], 71), 0)
    w_key = normal_values(streams_of[4], (D, KV * HD), D ** -0.5, 0.15625, ((0, 32),))
    w_value = normal_values(streams_of[5], (D, KV * HD), D ** -0.5, 0.15625, ((0, 32),))
    w_out = normal_values(streams_of[6], (H * HD, D), (H * HD // 16) ** -0.5, 0.625, ((0, 32),))
    w_gate = normal_values(streams_of[7], (D, FF), D ** -0.5, 0.15625, ((0, 32),))
    w_up = normal_values(streams_of[8], (D, FF), D ** -0.5, 0.15625, ((0, 32),))
    w_down = normal_values(streams_of[9], (FF, D), FF ** -0.5, 0.09375, ((0, 32),))
    gain_attn = jnp.clip(1.0 + 0.1 * jax.random.normal(streams_of[10], (D,), jnp.float32), 0.5, 1.5).astype(jnp.bfloat16)
    gain_ffn = jnp.clip(1.0 + 0.1 * jax.random.normal(streams_of[11], (D,), jnp.float32), 0.5, 1.5).astype(jnp.bfloat16)
    return dict(inputs=inputs, segments=segments, cotangent=cotangent, w_query=w_query, w_key=w_key, w_value=w_value, w_out=w_out, w_gate=w_gate, w_up=w_up, w_down=w_down, gain_attn=gain_attn, gain_ffn=gain_ffn)


EPS = 1e-05
THETA = 100000.0
MASKED = -1e+30

def matmul(left, right):
    return jnp.dot(left, right, preferred_element_type=jnp.float32)

def rope_tables(positions):
    half_dim = HD // 2
    frequency = THETA ** (-(jnp.arange(half_dim, dtype=jnp.float32) * (2.0 / HD)))
    angles = positions.astype(jnp.float32)[:, None] * frequency[None, :]
    return (jnp.cos(angles), jnp.sin(angles))

def rotate(vectors, cosine, sine_values):
    half_dim = HD // 2
    first_half = vectors[..., :half_dim]
    second_half = vectors[..., half_dim:]
    cos_b = cosine[:, None, :]
    sin_b = sine_values[:, None, :]
    return jnp.concatenate([first_half * cos_b - second_half * sin_b, second_half * cos_b + first_half * sin_b], axis=-1)

def rms_scale(values):
    return lax.rsqrt(lax.optimization_barrier(jnp.mean(values * values, axis=-1, keepdims=True)) + EPS)

def norm_back(d_normed, values, scale, gain):
    weighted = d_normed * gain.astype(jnp.float32)
    return scale * weighted - values * (scale * scale * scale) * lax.optimization_barrier(jnp.mean(weighted * values, axis=-1, keepdims=True))

def allowed_pairs(positions, doc_ids, key_positions, key_docs):
    return (doc_ids[:, None] == key_docs[None, :]) & (key_positions[None, :] <= positions[:, None])

def block_scores(queries, keys_all, allowed):
    scores = jnp.einsum('rkgd,lkd->kgrl', queries.astype(jnp.float32), keys_all.astype(jnp.float32)) * HD ** (-0.5)
    return jnp.where(allowed[None, None], scores, MASKED)

def attend_block(queries, keys_all, values_all, allowed):
    scores = block_scores(queries, keys_all, allowed)
    row_max = lax.optimization_barrier(jnp.max(scores, axis=-1, keepdims=True))
    summed = lax.optimization_barrier(jnp.sum(jnp.exp(scores - row_max), axis=-1, keepdims=True))
    log_total = row_max + jnp.log(summed)
    probs_low = lax.optimization_barrier(jnp.exp(scores - log_total).astype(jnp.bfloat16))
    attended = jnp.einsum('kgrl,lkd->rkgd', probs_low.astype(jnp.float32), values_all.astype(jnp.float32))
    return (attended.astype(jnp.bfloat16), log_total[..., 0])

def attend_back(queries, keys_all, values_all, allowed, log_total, attended, d_attended):
    scores = block_scores(queries, keys_all, allowed)
    probs = jnp.exp(scores - log_total[..., None])
    probs_low = lax.optimization_barrier(probs.astype(jnp.bfloat16)).astype(jnp.float32)
    d_wide = d_attended.astype(jnp.float32)
    row_delta = jnp.einsum('rkgd,rkgd->kgr', d_wide, attended.astype(jnp.float32))
    d_probs = jnp.einsum('rkgd,lkd->kgrl', d_wide, values_all.astype(jnp.float32))
    d_scores = lax.optimization_barrier((probs * (d_probs - row_delta[..., None]) * HD ** (-0.5)).astype(jnp.bfloat16))
    d_scores = d_scores.astype(jnp.float32)
    d_query = jnp.einsum('kgrl,lkd->rkgd', d_scores, keys_all.astype(jnp.float32))
    d_keys = jnp.einsum('kgrl,rkgd->lkd', d_scores, queries.astype(jnp.float32))
    d_values = jnp.einsum('kgrl,rkgd->lkd', probs_low, d_wide)
    return (d_query, d_keys, d_values)

def attention_forward(queries, keys_all, values_all, positions, doc_ids, key_positions, key_docs):
    row_count = queries.shape[0]
    block_rows = math.gcd(row_count, 512)

    def one_block(step_index):
        row_start = (step_index * block_rows).astype(jnp.int32)
        piece_q = lax.dynamic_slice_in_dim(queries, row_start, block_rows, 0)
        allowed = allowed_pairs(lax.dynamic_slice_in_dim(positions, row_start, block_rows, 0), lax.dynamic_slice_in_dim(doc_ids, row_start, block_rows, 0), key_positions, key_docs)
        return attend_block(piece_q, keys_all, values_all, allowed)
    attended, log_total = lax.map(one_block, jnp.arange(row_count // block_rows, dtype=jnp.int32))
    return (attended.reshape(queries.shape), log_total)

def attention_backward(queries, keys_all, values_all, positions, doc_ids, key_positions, key_docs, log_total, attended, d_attended):
    row_count = queries.shape[0]
    block_rows = math.gcd(row_count, 512)

    def step_fn(carried, step_index):
        key_sum, value_sum = carried
        row_start = (step_index * block_rows).astype(jnp.int32)

        def piece_of(array):
            return lax.dynamic_slice_in_dim(array, row_start, block_rows, 0)
        allowed = allowed_pairs(piece_of(positions), piece_of(doc_ids), key_positions, key_docs)
        d_query, d_keys, d_values = attend_back(piece_of(queries), keys_all, values_all, allowed, log_total[step_index], piece_of(attended), piece_of(d_attended))
        return ((key_sum + d_keys, value_sum + d_values), d_query)
    zero_sums = jnp.zeros(keys_all.shape, jnp.float32)
    (key_sum, value_sum), d_queries = lax.scan(step_fn, (zero_sums, zero_sums), jnp.arange(row_count // block_rows, dtype=jnp.int32))
    return (d_queries.reshape(queries.shape), key_sum, value_sum)

def layer(tokens, doc_ids, cotangent, weights):
    w_query, w_key, w_value, w_out, w_gate, w_up, w_down, gain_attn, gain_ffn = weights
    length = tokens.shape[0]
    groups = H // KV
    positions = jnp.arange(length, dtype=jnp.int32)
    cosine, sine_values = rope_tables(positions)
    residual = tokens.astype(jnp.float32)
    scale_attn = rms_scale(residual)
    normed_attn = (residual * scale_attn * gain_attn.astype(jnp.float32)).astype(jnp.bfloat16)
    queries = rotate(matmul(normed_attn, w_query).reshape(length, H, HD), cosine, sine_values).astype(jnp.bfloat16).reshape(length, KV, groups, HD)
    keys_all = rotate(matmul(normed_attn, w_key).reshape(length, KV, HD), cosine, sine_values).astype(jnp.bfloat16)
    values_all = matmul(normed_attn, w_value).astype(jnp.bfloat16).reshape(length, KV, HD)
    attended, log_total = attention_forward(queries, keys_all, values_all, positions, doc_ids, positions, doc_ids)
    attended_flat = attended.reshape(length, H * HD)
    mid = residual + matmul(attended_flat, w_out)
    scale_ffn = rms_scale(mid)
    normed_ffn = (mid * scale_ffn * gain_ffn.astype(jnp.float32)).astype(jnp.bfloat16)
    gate_act = matmul(normed_ffn, w_gate)
    up_act = matmul(normed_ffn, w_up)
    sigmoid_gate = jax.nn.sigmoid(gate_act)
    hidden = (gate_act * sigmoid_gate * up_act).astype(jnp.bfloat16)
    outputs = mid + matmul(hidden, w_down)
    grad_down = matmul(hidden.T, cotangent)
    d_hidden = matmul(cotangent, w_down.T)
    d_gate = (d_hidden * up_act * sigmoid_gate * (1.0 + gate_act * (1.0 - sigmoid_gate))).astype(jnp.bfloat16)
    d_up = (d_hidden * gate_act * sigmoid_gate).astype(jnp.bfloat16)
    grad_gate = matmul(normed_ffn.T, d_gate)
    grad_up = matmul(normed_ffn.T, d_up)
    d_normed_ffn = matmul(d_gate, w_gate.T) + matmul(d_up, w_up.T)
    grad_gain_ffn = lax.optimization_barrier(jnp.sum(d_normed_ffn * mid * scale_ffn, axis=0))
    d_mid = cotangent.astype(jnp.float32) + norm_back(d_normed_ffn, mid, scale_ffn, gain_ffn)
    d_mid_low = d_mid.astype(jnp.bfloat16)
    grad_out = matmul(attended_flat.T, d_mid_low)
    d_attended = matmul(d_mid_low, w_out.T).astype(jnp.bfloat16).reshape(length, KV, groups, HD)
    d_query_rot, d_key_rot, d_value_sum = attention_backward(queries, keys_all, values_all, positions, doc_ids, positions, doc_ids, log_total, attended, d_attended)
    d_query = rotate(d_query_rot.reshape(length, H, HD), cosine, -sine_values).astype(jnp.bfloat16).reshape(length, H * HD)
    d_key = rotate(d_key_rot, cosine, -sine_values).astype(jnp.bfloat16).reshape(length, KV * HD)
    d_value = d_value_sum.astype(jnp.bfloat16).reshape(length, KV * HD)
    grad_query = matmul(normed_attn.T, d_query)
    grad_key = matmul(normed_attn.T, d_key)
    grad_value = matmul(normed_attn.T, d_value)
    d_normed_attn = matmul(d_query, w_query.T) + matmul(d_key, w_key.T) + matmul(d_value, w_value.T)
    grad_gain_attn = lax.optimization_barrier(jnp.sum(d_normed_attn * residual * scale_attn, axis=0))
    input_grad = d_mid + norm_back(d_normed_attn, residual, scale_attn, gain_attn)
    grads = (grad_query, grad_key, grad_value, grad_out, grad_gate, grad_up, grad_down, grad_gain_attn, grad_gain_ffn)
    return (outputs, input_grad, grads)

def reference(inputs, segments, cotangent, w_query, w_key, w_value, w_out, w_gate, w_up, w_down, gain_attn, gain_ffn):
    weights = (w_query, w_key, w_value, w_out, w_gate, w_up, w_down, gain_attn, gain_ffn)

    def step_fn(totals, sequence_item):
        tokens, doc_ids, cot_rows = sequence_item
        outputs, input_grad, grads = layer(tokens, doc_ids, cot_rows, weights)
        return (tuple((summed + grad_term for summed, grad_term in zip(totals, grads))), (outputs, input_grad))
    initial = tuple((jnp.zeros(weight.shape, jnp.float32) for weight in weights))
    totals, (outputs, input_grad) = lax.scan(step_fn, initial, (inputs, segments, cotangent))
    return (outputs, input_grad, totals[0], totals[1], totals[2], totals[3], totals[4], totals[5], totals[6], totals[7], totals[8])
```

```python
import functools

import jax
import jax.numpy as jnp
from jax import lax
from jax.experimental import pallas as pl
from jax.experimental.pallas import tpu as pltpu
from jax.sharding import PartitionSpec as P

H = 16
KV = 8
HD = 96
HALF = HD // 2
LANES = 128
SPAN = 512

EPS = 1e-05
THETA = 100000.0
MASKED = -1e30

BF = jnp.bfloat16
F32 = jnp.float32
MESH = pl.DeviceIdType.MESH
VMEM_LIMIT = 60 * 1024 * 1024


def sds(shape, dtype=BF):
    return jax.ShapeDtypeStruct(tuple(shape), dtype)


def dot_nn(a, b):
    return lax.dot_general(a, b, (((1,), (0,)), ((), ())), preferred_element_type=F32)


def dot_nt(a, b):
    return lax.dot_general(a, b, (((1,), (1,)), ((), ())), preferred_element_type=F32)


def dot_tn(a, b):
    return lax.dot_general(a, b, (((0,), (0,)), ((), ())), preferred_element_type=F32)


class Sizes:
    def __init__(self, dp, ctx):
        self.dp, self.ctx = dp, ctx
        self.outer = 4 if dp % 4 == 0 else dp
        self.inner = dp // self.outer
        self.ys = ctx // 2


class Link:
    def __init__(self, z, send_sems, recv_sems, local_sems):
        self.z = z
        self.d = lax.axis_index("dp")
        self.c = lax.axis_index("ctx")
        self.o, self.i = lax.div(self.d, z.inner), lax.rem(self.d, z.inner)
        self.y, self.k = lax.div(self.c, 2), lax.rem(self.c, 2)
        self.sems = (send_sems, recv_sems, local_sems)
        self.sent, self.inflight, self.local = 0, [], []

    def ctx_dev(self, y, k):
        return (self.d, y * 2 + k)

    def ctx_peers(self):
        n = self.z.ctx
        return [lax.rem(self.c + j, n) for j in range(1, n)]

    def y_peers(self):
        n = self.z.ys
        return [lax.rem(self.y + j, n) for j in range(1, n)]

    def outer_to(self, j):
        return lax.rem(self.o + j, self.z.outer)

    def outer_from(self, j):
        return lax.rem(self.o + self.z.outer - j, self.z.outer)

    def inner_to(self, j):
        return lax.rem(self.i + j, self.z.inner)

    def dp_dev(self, o, i):
        return (o * self.z.inner + i, self.c)

    def barrier(self):
        devices = [(self.d, c) for c in self.ctx_peers()]
        devices += [self.dp_dev(self.outer_to(j), self.i) for j in range(1, self.z.outer)]
        devices += [self.dp_dev(self.o, self.inner_to(j)) for j in range(1, self.z.inner)]
        barrier = pltpu.get_barrier_semaphore()
        for device in devices:
            pl.semaphore_signal(barrier, inc=1, device_id=device, device_id_type=MESH)
        pl.semaphore_wait(barrier, len(devices))

    def put(self, src, dst, device):
        n = self.sent
        self.sent += 1
        copy = pltpu.make_async_remote_copy(
            src_ref=src,
            dst_ref=dst,
            send_sem=self.sems[0].at[n],
            recv_sem=self.sems[1].at[n],
            device_id=device,
            device_id_type=MESH,
        )
        copy.start()
        self.inflight.append(copy)
        return copy

    def keep(self, src, dst):
        copy = pltpu.make_async_copy(src, dst, self.sems[2].at[len(self.local)])
        copy.start()
        self.local.append(copy)
        return copy

    def arrived(self, copy):
        copy.wait_recv()
        self.inflight = [other for other in self.inflight if other is not copy]
        self.landed.append(copy)

    def finish(self):
        for copy in self.inflight:
            copy.wait_recv()
        for copy in self.landed + self.inflight:
            copy.wait_send()
        for copy in self.local:
            copy.wait()

    landed = None


def communicate(z, name, cid, script, ins, outs, scratch=()):
    n_in, n_out = len(ins), len(outs)

    def kernel(*refs):
        in_refs, out_refs = refs[:n_in], refs[n_in : n_in + n_out]
        send, recv, local = refs[n_in + n_out : n_in + n_out + 3]
        link = Link(z, send, recv, local)
        link.landed = []
        link.barrier()
        script(link, in_refs, out_refs, refs[n_in + n_out + 3 :])
        link.finish()

    hbm = pl.BlockSpec(memory_space=pltpu.HBM)
    return pl.pallas_call(
        kernel,
        name=name,
        out_shape=list(outs),
        in_specs=[hbm] * n_in,
        out_specs=[hbm] * n_out,
        scratch_shapes=[
            pltpu.SemaphoreType.DMA((64,)),
            pltpu.SemaphoreType.DMA((64,)),
            pltpu.SemaphoreType.DMA((16,)),
        ]
        + list(scratch),
        compiler_params=pltpu.CompilerParams(
            collective_id=cid, has_side_effects=True, vmem_limit_bytes=VMEM_LIMIT
        ),
    )(*ins)


def gather_ctx_start(link, src, buf, wait_src=None):
    slot = buf.at[link.c]
    ways = []
    for j in range(1, link.z.ys):
        to = lax.rem(link.y + j, link.z.ys)
        frm = lax.rem(link.y + link.z.ys - j, link.z.ys)
        ways.append((frm, link.put(src, slot, link.ctx_dev(to, link.k))))
    link.put(src, slot, link.ctx_dev(link.y, 1 - link.k))
    return ways


def gather_ctx_forward(link, buf, ways):
    for frm, copy in ways:
        link.arrived(copy)
        slot = buf.at[frm * 2 + link.k]
        link.put(slot, slot, link.ctx_dev(link.y, 1 - link.k))


def exchange_ctx(link, pack, slot_of):
    return [link.put(pack.at[c], slot_of(link.c), (link.d, c)) for c in link.ctx_peers()]


def gather_dp_start(link, slot_of):
    own = slot_of(link.d)
    ways = []
    for j in range(1, link.z.outer):
        copy = link.put(own, own, link.dp_dev(link.outer_to(j), link.i))
        ways.append((link.outer_from(j), copy))
    for j in range(1, link.z.inner):
        link.put(own, own, link.dp_dev(link.o, link.inner_to(j)))
    return ways


def gather_dp_forward(link, slot_of, ways):
    for frm, copy in ways:
        link.arrived(copy)
        slot = slot_of(frm * link.z.inner + link.i)
        for j in range(1, link.z.inner):
            link.put(slot, slot, link.dp_dev(link.o, link.inner_to(j)))


def scatter_inner(link, src, dst):
    for j in range(1, link.z.inner):
        to = link.inner_to(j)
        link.put(src.at[:, to], dst.at[j - 1], link.dp_dev(link.o, to))


def scatter_outer(link, src, dst):
    for j in range(1, link.z.outer):
        to = link.outer_to(j)
        link.put(src.at[to], dst.at[j - 1], link.dp_dev(to, link.i))


def scatter_core(link, src, dst):
    link.put(src.at[:, 1 - link.k], dst, link.ctx_dev(link.y, 1 - link.k))


def scatter_y(link, src, dst):
    for j in range(1, link.z.ys):
        to = lax.rem(link.y + j, link.z.ys)
        link.put(src.at[to], dst.at[j - 1], link.ctx_dev(to, link.k))


def rotated(u, cos, sin):
    return u * cos + pltpu.roll(u, LANES // 2, 1) * sin


def qkv_kernel(hc, kvc, x_ref, gain_ref, w_ref, cos_ref, sin_ref, n_ref, q_ref, k_ref, v_ref):
    x = x_ref[0, 0].astype(F32)
    scale = lax.rsqrt(jnp.mean(x * x, axis=-1, keepdims=True) + EPS)
    normed = (x * scale * gain_ref[...]).astype(BF)
    n_ref[0, 0] = normed
    full = dot_nn(normed, w_ref[...])
    cos, sin = cos_ref[0], sin_ref[0]
    for h in range(hc + kvc):
        piece = rotated(full[:, h * LANES : (h + 1) * LANES], cos, sin).astype(BF)
        if h < hc:
            q_ref[0, 0, :, h * LANES : (h + 1) * LANES] = piece
        else:
            k_ref[0, 0, :, (h - hc) * LANES : (h - hc + 1) * LANES] = piece
    v_ref[0, 0] = full[:, (hc + kvc) * LANES :].astype(BF)


def qkv_call(z, x_all, gain, w, cos, sin, hc, kvc):
    ctx, m, r, d = x_all.shape
    row = lambda s, b: (s, b, 0, 0)
    whole = lambda s, b: (0, 0)
    table = pl.BlockSpec((1, r, LANES), lambda s, b: (s, 0, 0))
    return pl.pallas_call(
        functools.partial(qkv_kernel, hc, kvc),
        name="qkv",
        grid=(ctx, m),
        in_specs=[
            pl.BlockSpec((1, 1, r, d), row),
            pl.BlockSpec((1, d), whole),
            pl.BlockSpec(w.shape, whole, pipeline_mode=pl.Buffered(1)),
            table,
            table,
        ],
        out_specs=[
            pl.BlockSpec((1, 1, r, d), row),
            pl.BlockSpec((1, 1, r, hc * LANES), row),
            pl.BlockSpec((1, 1, r, kvc * LANES), row),
            pl.BlockSpec((1, 1, r, kvc * LANES), row),
        ],
        out_shape=[
            sds((ctx, m, r, d)),
            sds((ctx, m, r, hc * LANES)),
            sds((ctx, m, r, kvc * LANES)),
            sds((ctx, m, r, kvc * LANES)),
        ],
        compiler_params=pltpu.CompilerParams(vmem_limit_bytes=VMEM_LIMIT),
    )(x_all, gain, w, cos, sin)


def window_of(s, r, ctx):
    blocks = min(ctx, SPAN // r + 1)
    return jnp.maximum(s - (blocks - 1), 0), blocks


def bias_of(s, first, blocks, r, qdoc_ref, kdoc_ref):
    qdoc = qdoc_ref[0, 0]
    pieces = []
    for b in range(blocks):
        kdoc = kdoc_ref[first + b, 0]
        rows = lax.broadcasted_iota(jnp.int32, (r, r), 0) + s * r
        cols = lax.broadcasted_iota(jnp.int32, (r, r), 1) + (first + b) * r
        pieces.append(jnp.where((qdoc == kdoc) & (cols <= rows), 0.0, MASKED))
    return jnp.concatenate(pieces, axis=1)


def attend_kernel(hc, kvc, ctx, q_ref, k_ref, v_ref, qdoc_ref, kdoc_ref, out_ref, lse_ref):
    s = pl.program_id(1)
    r = q_ref.shape[2]
    first, blocks = window_of(s, r, ctx)
    bias = bias_of(s, first, blocks, r, qdoc_ref, kdoc_ref)
    lane = lax.broadcasted_iota(jnp.int32, (r, LANES), 1)
    lse_all = jnp.zeros((r, LANES), F32)
    outs = []
    for h in range(hc):
        g = h * kvc // hc
        q = q_ref[0, 0, :, h * LANES : (h + 1) * LANES]
        k = k_ref[pl.ds(first, blocks), 0, :, g * LANES : (g + 1) * LANES].reshape(blocks * r, LANES)
        v = v_ref[pl.ds(first, blocks), 0, :, g * LANES : (g + 1) * LANES].reshape(blocks * r, LANES)
        scores = dot_nt(q, k) * HD ** (-0.5) + bias
        top = jnp.max(scores, axis=-1, keepdims=True)
        e = jnp.exp(scores - top)
        total = jnp.sum(e, axis=-1, keepdims=True)
        probs = (e * (1.0 / total)).astype(BF)
        outs.append(dot_nn(probs, v)[:, :HD])
        lse_all = jnp.where(lane == h, top + jnp.log(total), lse_all)
    out_ref[0, 0] = jnp.concatenate(outs, axis=1).astype(BF)
    lse_ref[0, 0] = lse_all


def attend_call(z, q, k, v, qdoc, kdoc, hc, kvc):
    ctx, m, r, _ = q.shape
    row = lambda b, s: (s, b, 0, 0)
    seq = lambda b, s: (0, b, 0, 0)
    return pl.pallas_call(
        functools.partial(attend_kernel, hc, kvc, ctx),
        name="attend",
        grid=(m, ctx),
        in_specs=[
            pl.BlockSpec((1, 1, r, hc * LANES), row),
            pl.BlockSpec((ctx, 1, r, kvc * LANES), seq),
            pl.BlockSpec((ctx, 1, r, kvc * LANES), seq),
            pl.BlockSpec((1, 1, r, 1), row),
            pl.BlockSpec((ctx, 1, 1, r), seq),
        ],
        out_specs=[pl.BlockSpec((1, 1, r, hc * HD), row), pl.BlockSpec((1, 1, r, LANES), row)],
        out_shape=[sds((ctx, m, r, hc * HD)), sds((ctx, m, r, LANES), F32)],
        compiler_params=pltpu.CompilerParams(vmem_limit_bytes=VMEM_LIMIT),
    )(q, k, v, qdoc, kdoc)


def attend_back_kernel(
    hc, kvc, ctx, q_ref, k_ref, v_ref, qdoc_ref, kdoc_ref, o_ref, do_ref, lse_ref, cos_ref, sin_ref,
    out_ref, dk_acc, dv_acc,
):
    s = pl.program_id(1)
    r = q_ref.shape[2]
    first, blocks = window_of(s, r, ctx)
    bias = bias_of(s, first, blocks, r, qdoc_ref, kdoc_ref)

    @pl.when(s == 0)
    def _():
        dk_acc[...] = jnp.zeros_like(dk_acc)
        dv_acc[...] = jnp.zeros_like(dv_acc)

    cos, sin = cos_ref[s], sin_ref[s]
    lse_all = lse_ref[0, 0]
    for h in range(hc):
        g = h * kvc // hc
        q = q_ref[0, 0, :, h * LANES : (h + 1) * LANES]
        k = k_ref[pl.ds(first, blocks), 0, :, g * LANES : (g + 1) * LANES].reshape(blocks * r, LANES)
        v = v_ref[pl.ds(first, blocks), 0, :, g * LANES : (g + 1) * LANES].reshape(blocks * r, LANES)
        o = o_ref[0, 0, :, h * HD : (h + 1) * HD].astype(F32)
        do = do_ref[0, 0, :, h * HD : (h + 1) * HD]
        delta = jnp.sum(o * do.astype(F32), axis=-1, keepdims=True)
        do = jnp.concatenate([do, jnp.zeros((r, LANES - HD), BF)], axis=1)
        scores = dot_nt(q, k) * HD ** (-0.5) + bias
        probs = jnp.exp(scores - lse_all[:, h : h + 1])
        d_probs = dot_nt(do, v)
        d_scores = (probs * (d_probs - delta) * HD ** (-0.5)).astype(BF)
        dq = dot_nn(d_scores, k)
        out_ref[s, 0, :, h * LANES : (h + 1) * LANES] = rotated(dq, cos, -sin).astype(BF)
        dk = dot_tn(d_scores, q).reshape(blocks, r, LANES)
        dv = dot_tn(probs.astype(BF), do).reshape(blocks, r, LANES)
        here = slice(g * LANES, (g + 1) * LANES)
        dk_acc[pl.ds(first, blocks), :, here] += dk
        dv_acc[pl.ds(first, blocks), :, here] += dv

    @pl.when(s == ctx - 1)
    def _():
        for b in range(ctx):
            for g in range(kvc):
                here = slice(g * LANES, (g + 1) * LANES)
                at = (hc + g) * LANES
                dk = rotated(dk_acc[b, :, here], cos_ref[b], -sin_ref[b])
                out_ref[b, 0, :, at : at + LANES] = dk.astype(BF)
                at += kvc * LANES
                out_ref[b, 0, :, at : at + LANES] = dv_acc[b, :, here].astype(BF)


def attend_back_call(z, q, k, v, qdoc, kdoc, o, do, lse, cos, sin, hc, kvc):
    ctx, m, r, _ = q.shape
    row = lambda b, s: (s, b, 0, 0)
    seq = lambda b, s: (0, b, 0, 0)
    table = pl.BlockSpec((ctx, r, LANES), lambda b, s: (0, 0, 0))
    width = (hc + 2 * kvc) * LANES
    return pl.pallas_call(
        functools.partial(attend_back_kernel, hc, kvc, ctx),
        name="attend_back",
        grid=(m, ctx),
        in_specs=[
            pl.BlockSpec((1, 1, r, hc * LANES), row),
            pl.BlockSpec((ctx, 1, r, kvc * LANES), seq),
            pl.BlockSpec((ctx, 1, r, kvc * LANES), seq),
            pl.BlockSpec((1, 1, r, 1), row),
            pl.BlockSpec((ctx, 1, 1, r), seq),
            pl.BlockSpec((1, 1, r, hc * HD), row),
            pl.BlockSpec((1, 1, r, hc * HD), row),
            pl.BlockSpec((1, 1, r, LANES), row),
            table,
            table,
        ],
        out_specs=pl.BlockSpec((ctx, 1, r, width), seq),
        out_shape=sds((ctx, m, r, width)),
        scratch_shapes=[
            pltpu.VMEM((ctx, r, kvc * LANES), F32),
            pltpu.VMEM((ctx, r, kvc * LANES), F32),
        ],
        compiler_params=pltpu.CompilerParams(vmem_limit_bytes=VMEM_LIMIT),
    )(q, k, v, qdoc, kdoc, o, do, lse, cos, sin)


def mlp_kernel(x_ref, cot_ref, gu_ref, down_ref, hid_ref, dgu_ref, out_ref, dn_ref):
    x, cot = x_ref[0, 0], cot_ref[0, 0]
    f = down_ref.shape[0]
    both = dot_nn(x, gu_ref[...])
    gate, up = both[:, :f], both[:, f:]
    d_hidden = dot_nt(cot, down_ref[...])
    sg = jax.nn.sigmoid(gate)
    act = gate * sg
    hidden = (act * up).astype(BF)
    hid_ref[0, 0] = hidden
    d_gate = (d_hidden * up * sg * (1.0 + gate * (1.0 - sg))).astype(BF)
    d_up = (d_hidden * act).astype(BF)
    dgu_ref[0, 0, :, :f] = d_gate
    dgu_ref[0, 0, :, f:] = d_up
    out_ref[0, 0] = dot_nn(hidden, down_ref[...]).astype(BF)
    dn_ref[0, 0] = (dot_nt(d_gate, gu_ref[:, :f]) + dot_nt(d_up, gu_ref[:, f:])).astype(BF)


def mlp_call(z, x, cot, gu, down):
    ctx, m, r, d = x.shape
    f = down.shape[0]
    row = lambda s, b: (s, b, 0, 0)
    whole = lambda s, b: (0, 0)
    return pl.pallas_call(
        mlp_kernel,
        name="mlp",
        grid=(ctx, m),
        in_specs=[
            pl.BlockSpec((1, 1, r, d), row),
            pl.BlockSpec((1, 1, r, d), row),
            pl.BlockSpec(gu.shape, whole, pipeline_mode=pl.Buffered(1)),
            pl.BlockSpec(down.shape, whole, pipeline_mode=pl.Buffered(1)),
        ],
        out_specs=[
            pl.BlockSpec((1, 1, r, f), row),
            pl.BlockSpec((1, 1, r, 2 * f), row),
            pl.BlockSpec((1, 1, r, d), row),
            pl.BlockSpec((1, 1, r, d), row),
        ],
        out_shape=[
            sds((ctx, m, r, f)),
            sds((ctx, m, r, 2 * f)),
            sds((ctx, m, r, d)),
            sds((ctx, m, r, d)),
        ],
        compiler_params=pltpu.CompilerParams(vmem_limit_bytes=VMEM_LIMIT),
    )(x, cot, gu, down)


def pad_heads(w, heads, split):
    rows = w.shape[0]
    if split:
        w = jnp.pad(w.reshape(rows, heads, 2, HALF), ((0, 0), (0, 0), (0, 0), (0, LANES // 2 - HALF)))
    else:
        w = jnp.pad(w.reshape(rows, heads, HD), ((0, 0), (0, 0), (0, LANES - HD)))
    return w.reshape(rows, heads * LANES)


def unpad_heads(w, heads, split):
    if split:
        w = w.reshape(w.shape[:-1] + (heads, 2, LANES // 2))[..., :HALF]
    else:
        w = w.reshape(w.shape[:-1] + (heads, LANES))[..., :HD]
    return w.reshape(w.shape[: w.ndim - (3 if split else 2)] + (heads * HD,))


def rope_tables(ctx, r):
    frequency = THETA ** (-(jnp.arange(HALF, dtype=F32) * (2.0 / HD)))
    angles = jnp.arange(ctx * r, dtype=jnp.int32).astype(F32)[:, None] * frequency[None, :]
    pad = ((0, 0), (0, LANES // 2 - HALF))
    cos, sin = jnp.pad(jnp.cos(angles), pad), jnp.pad(jnp.sin(angles), pad)
    cos = jnp.concatenate([cos, cos], axis=1).reshape(ctx, r, LANES)
    sin = jnp.concatenate([-sin, sin], axis=1).reshape(ctx, r, LANES)
    return cos, sin


def per_device(
    inputs, segments, cotangent, w_query, w_key, w_value, w_out, w_gate, w_up, w_down, gain_attn, gain_ffn
):
    z = Sizes(lax.axis_size("dp"), lax.axis_size("ctx"))
    dp, ctx, outer, inner, ys = z.dp, z.ctx, z.outer, z.inner, z.ys
    m, r, d = inputs.shape
    rows = w_query.shape[0]
    frows, ff = w_down.shape[0], w_gate.shape[1]
    f = ff // ctx
    hc, kvc = H // ctx, KV // ctx
    width = (hc + 2 * kvc) * LANES
    c = lax.axis_index("ctx")
    di = lax.axis_index("dp")
    oi, ii = di // inner, di % inner
    yi, ki = c // 2, c % 2
    dyn = lambda a, at, axis: lax.dynamic_index_in_dim(a, at, axis, keepdims=False)

    pack_qkv = jnp.concatenate(
        [
            pad_heads(w_query, H, True).reshape(rows, ctx, hc * LANES),
            pad_heads(w_key, KV, True).reshape(rows, ctx, kvc * LANES),
            pad_heads(w_value, KV, False).reshape(rows, ctx, kvc * LANES),
        ],
        axis=2,
    ).transpose(1, 0, 2)
    by_rank = lambda w: w.reshape(rows, dp, ctx, frows).transpose(2, 0, 1, 3).reshape(ctx, rows, f)
    pack_gu = jnp.concatenate([by_rank(w_gate), by_rank(w_up)], axis=2)
    gains = jnp.stack([gain_attn, gain_ffn]).astype(F32)
    gains = jnp.pad(gains, ((0, 6), (0, LANES - rows)))

    def first_script(link, ins, outs, scratch):
        x, seg, qkv, gain = ins
        x_all, seg_all, g_qkv, g_gain = outs
        (hold,) = scratch
        load = pltpu.make_async_copy(x, hold, link.sems[2].at[15])
        load.start()
        link.keep(qkv.at[link.c], g_qkv.at[link.d, link.c])
        link.keep(gain, g_gain.at[link.d, link.c])
        link.keep(seg, seg_all.at[link.c])
        a2a = exchange_ctx(link, qkv, lambda s: g_qkv.at[link.d, s])
        a2a += [link.put(gain, g_gain.at[link.d, link.c], (link.d, p)) for p in link.ctx_peers()]
        for p in link.ctx_peers():
            link.put(seg, seg_all.at[link.c], (link.d, p))
        ways_x = gather_ctx_start(link, x, x_all)
        for copy in a2a:
            link.arrived(copy)
        for copy in link.local:
            copy.wait()
        link.local = []
        slots = (lambda s: g_qkv.at[s], lambda s: g_gain.at[s])
        ways = [gather_dp_start(link, slot) for slot in slots]
        load.wait()
        store = pltpu.make_async_copy(hold, x_all.at[link.c], link.sems[2].at[14])
        store.start()
        for slot, way in zip(slots, ways):
            gather_dp_forward(link, slot, way)
        gather_ctx_forward(link, x_all, ways_x)
        store.wait()

    x_all, seg_all, g_qkv, g_gain = communicate(
        z,
        "gather_first",
        1,
        first_script,
        (inputs, segments, pack_qkv, gains),
        (
            sds((ctx, m, r, d)),
            sds((ctx, m, r), jnp.int32),
            sds((dp, ctx, rows, width)),
            sds((dp, ctx, 8, LANES), F32),
        ),
        [pltpu.VMEM((m, r, d), BF)],
    )
    gain_a = g_gain[:, :, 0, :rows].reshape(1, d)
    gain_f = g_gain[:, :, 1, :rows].reshape(1, d)
    wqkv = g_qkv.reshape(d, width)
    cos, sin = rope_tables(ctx, r)
    qdoc = seg_all.reshape(ctx, m, r, 1)
    kdoc = seg_all.reshape(ctx, m, 1, r)

    normed_a, q, k, v = qkv_call(z, x_all, gain_a, wqkv, cos, sin, hc, kvc)
    att, lse = attend_call(z, q, k, v, qdoc, kdoc, hc, kvc)

    def second_script(link, ins, outs, scratch):
        att, wo, gu, wd, cot = ins
        att_all, g_out, g_gu, g_down, cot_all = outs
        (hold,) = scratch
        load = pltpu.make_async_copy(cot, hold, link.sems[2].at[15])
        load.start()
        link.keep(gu.at[link.c], g_gu.at[link.d, link.c])
        link.keep(wo, g_out.at[link.d, link.y, link.k])
        link.keep(wd, g_down.at[link.d])
        link.keep(att.at[link.c], att_all.at[link.c])
        exchange_ctx(link, att, lambda s: att_all.at[s])
        a2a = exchange_ctx(link, gu, lambda s: g_gu.at[link.d, s])
        for p in link.y_peers():
            a2a.append(link.put(wo, g_out.at[link.d, link.y, link.k], link.ctx_dev(p, link.k)))
        ways_c = gather_ctx_start(link, cot, cot_all)
        load.wait()
        store = pltpu.make_async_copy(hold, cot_all.at[link.c], link.sems[2].at[14])
        store.start()
        for copy in link.local:
            copy.wait()
        link.local = []
        slots = [
            lambda s: g_down.at[s],
            lambda s: g_gu.at[s],
            lambda s: g_out.at[s, :, link.k],
        ]
        ways = [gather_dp_start(link, slots[0])]
        for copy in a2a:
            link.arrived(copy)
        ways += [gather_dp_start(link, slot) for slot in slots[1:]]
        gather_ctx_forward(link, cot_all, ways_c)
        done = 0
        for slot, way in zip(slots, ways):
            gather_dp_forward(link, slot, way)
        for copy in list(link.inflight):
            link.arrived(copy)
        mine = g_out.at[:, :, link.k]
        link.put(mine, mine, link.ctx_dev(link.y, 1 - link.k))
        store.wait()

    att_all, g_out, g_gu, g_down, cot_all = communicate(
        z,
        "gather_second",
        2,
        second_script,
        (att, w_out, pack_gu, w_down, cotangent),
        (
            sds(att.shape),
            sds((dp, ys, 2, rows, d)),
            sds((dp, ctx, rows, 2 * f)),
            sds((dp, frows, d)),
            sds((ctx, m, r, d)),
        ),
        [pltpu.VMEM((m, r, d), BF)],
    )
    wo = g_out.reshape(d, d)
    wgu = g_gu.reshape(d, 2 * f)
    wd = g_down.reshape(f, d)

    att_rows = att_all.transpose(1, 2, 0, 3).reshape(m * r, H * HD)
    residual = inputs.astype(F32)
    mid = residual + dot_nn(att_rows, wo).reshape(m, r, d)
    scale_f = lax.rsqrt(jnp.mean(mid * mid, axis=-1, keepdims=True) + EPS)
    normed = (mid * scale_f * gain_f).astype(BF)

    def third_script(link, ins, outs, scratch):
        (x,), (x_all,), (hold,) = ins, outs, scratch
        load = pltpu.make_async_copy(x, hold, link.sems[2].at[15])
        load.start()
        ways = gather_ctx_start(link, x, x_all)
        load.wait()
        store = pltpu.make_async_copy(hold, x_all.at[link.c], link.sems[2].at[14])
        store.start()
        gather_ctx_forward(link, x_all, ways)
        store.wait()

    (normed_all,) = communicate(
        z, "gather_third", 3, third_script, (normed,), (sds((ctx, m, r, d)),), [pltpu.VMEM((m, r, d), BF)]
    )

    hidden, dgu, out_part, dn_part = mlp_call(z, normed_all, cot_all, wgu, wd)

    flat = lambda a: a.reshape(ctx * m * r, a.shape[-1])
    part_down = dot_tn(flat(hidden), flat(cot_all)).astype(BF).reshape(outer, inner, frows, d)
    part_gu = dot_tn(flat(normed_all), flat(dgu)).astype(BF).reshape(outer, inner, ctx, rows, 2 * f)

    halves = lambda a: a.reshape((ys, 2) + a.shape[1:])
    out_part, dn_part = halves(out_part), halves(dn_part)
    shape_y = (ys, m, r, d)

    def core_script(link, ins, outs, scratch):
        for src, dst in zip(ins, outs):
            scatter_core(link, src, dst)

    def y_script(link, ins, outs, scratch):
        for src, dst in zip(ins, outs):
            scatter_y(link, src, dst)

    dn_in, out_in = communicate(
        z, "reduce_core", 4, core_script, (dn_part, out_part), (sds(shape_y), sds(shape_y))
    )
    pair = lambda part, got: (dyn(part, ki, 1).astype(F32) + got.astype(F32)).astype(BF)
    dn_pair, out_pair = pair(dn_part, dn_in), pair(out_part, out_in)
    shape_y = (ys - 1, m, r, d)
    dn_in, out_in = communicate(
        z, "reduce_y", 5, y_script, (dn_pair, out_pair), (sds(shape_y), sds(shape_y))
    )
    total = lambda part, got, at: dyn(part, at, 0).astype(F32) + jnp.sum(got.astype(F32), axis=0)
    d_normed = total(dn_pair, dn_in, yi)
    outputs = mid + total(out_pair, out_in, yi)

    grad_gain_f = jnp.sum(d_normed * mid * scale_f, axis=(0, 1))
    cot32 = cotangent.astype(F32)
    e = d_normed * gain_f
    d_mid = cot32 + (
        scale_f * e - mid * (scale_f * scale_f * scale_f) * jnp.mean(e * mid, axis=-1, keepdims=True)
    )
    d_mid_low = d_mid.astype(BF).reshape(m * r, d)
    d_att = dot_nt(d_mid_low, wo).astype(BF)
    d_att = d_att.reshape(m, r, ctx, hc * HD).transpose(2, 0, 1, 3)
    part_out = dot_tn(att_rows, d_mid_low).astype(BF).reshape(dp, ys, 2, rows, d)

    def fourth_script(link, ins, outs, scratch):
        link.keep(ins[0].at[link.c], outs[0].at[link.c])
        exchange_ctx(link, ins[0], lambda s: outs[0].at[s])
        link.put(ins[1].at[:, :, 1 - link.k], outs[1], link.ctx_dev(link.y, 1 - link.k))

    d_att_all, po_in = communicate(
        z,
        "exchange_back",
        6,
        fourth_script,
        (d_att, part_out),
        (sds(d_att.shape), sds((dp, ys, rows, d))),
    )
    po_pair = (dyn(part_out, ki, 2).astype(F32) + po_in.astype(F32)).astype(BF)
    po_pair = po_pair.transpose(1, 0, 2, 3)

    dqkv = attend_back_call(z, q, k, v, qdoc, kdoc, att, d_att_all, lse, cos, sin, hc, kvc)
    part_qkv = dot_tn(flat(normed_a), flat(dqkv)).astype(BF).reshape(outer, inner, ctx, rows, width)
    da_part = halves(dot_nt(flat(dqkv), wqkv).astype(BF).reshape(ctx, m, r, d))

    def fifth_script(link, ins, outs, scratch):
        scatter_core(link, ins[0], outs[0])
        scatter_y(link, ins[1], outs[1])
        for n in (2, 3, 4):
            scatter_inner(link, ins[n], outs[n])

    da_in, po_y, down_in, gu_in, qkv_in = communicate(
        z,
        "reduce_inner",
        7,
        fifth_script,
        (da_part, po_pair, part_down, part_gu, part_qkv),
        (
            sds((ys, m, r, d)),
            sds((ys - 1, dp, rows, d)),
            sds((inner - 1, outer, frows, d)),
            sds((inner - 1, outer, ctx, rows, 2 * f)),
            sds((inner - 1, outer, ctx, rows, width)),
        ),
    )
    da_pair = pair(da_part, da_in)
    po_quarter = total(po_pair, po_y, yi).astype(BF).reshape(outer, inner, rows, d)
    column = lambda part, got: (dyn(part, ii, 1).astype(F32) + jnp.sum(got.astype(F32), axis=0)).astype(BF)
    down_col, gu_col, qkv_col = column(part_down, down_in), column(part_gu, gu_in), column(part_qkv, qkv_in)

    def sixth_script(link, ins, outs, scratch):
        scatter_y(link, ins[0], outs[0])
        scatter_inner(link, ins[1], outs[1])
        for n in (2, 3, 4):
            scatter_outer(link, ins[n], outs[n])

    da_in, po_in, down_in, gu_in, qkv_in = communicate(
        z,
        "reduce_outer",
        8,
        sixth_script,
        (da_pair, po_quarter, down_col, gu_col, qkv_col),
        (
            sds((ys - 1, m, r, d)),
            sds((inner - 1, outer, rows, d)),
            sds((outer - 1, frows, d)),
            sds((outer - 1, ctx, rows, 2 * f)),
            sds((outer - 1, ctx, rows, width)),
        ),
    )
    d_normed_a = total(da_pair, da_in, yi)
    scale_a = lax.rsqrt(jnp.mean(residual * residual, axis=-1, keepdims=True) + EPS)
    grad_gain_a = jnp.sum(d_normed_a * residual * scale_a, axis=(0, 1))
    e = d_normed_a * gain_a
    input_grad = d_mid + (
        scale_a * e - residual * (scale_a * scale_a * scale_a) * jnp.mean(e * residual, axis=-1, keepdims=True)
    )
    grad_down = total(down_col, down_in, oi)
    gu_mine = total(gu_col, gu_in, oi).astype(BF)
    qkv_mine = total(qkv_col, qkv_in, oi).astype(BF)
    po_col = column(po_quarter, po_in)

    def seventh_script(link, ins, outs, scratch):
        for n in (0, 1):
            link.keep(ins[n].at[link.c], outs[n].at[link.c])
            exchange_ctx(link, ins[n], lambda s: outs[n].at[s])
        scatter_outer(link, ins[2], outs[2])

    gu_all, qkv_all, po_in = communicate(
        z,
        "reduce_last",
        9,
        seventh_script,
        (gu_mine, qkv_mine, po_col),
        (sds((ctx, rows, 2 * f)), sds((ctx, rows, width)), sds((outer - 1, rows, d))),
    )
    grad_out = total(po_col, po_in, oi)
    gu_all = gu_all.astype(F32)
    spread = lambda a: a.reshape(ctx, rows, dp, frows).transpose(1, 2, 0, 3).reshape(rows, ff)
    grad_gate, grad_up = spread(gu_all[:, :, :f]), spread(gu_all[:, :, f:])
    qkv_all = qkv_all.astype(F32)
    cols = lambda a, heads, split: unpad_heads(a, heads, split).transpose(1, 0, 2).reshape(rows, ctx * heads * HD)
    grad_query = cols(qkv_all[:, :, : hc * LANES], hc, True)
    grad_key = cols(qkv_all[:, :, hc * LANES : (hc + kvc) * LANES], kvc, True)
    grad_value = cols(qkv_all[:, :, (hc + kvc) * LANES :], kvc, False)
    both = lax.psum_scatter(
        jnp.stack([grad_gain_a, grad_gain_f], axis=1), ("dp", "ctx"), scatter_dimension=0, tiled=True
    )
    return (
        outputs,
        input_grad,
        grad_query,
        grad_key,
        grad_value,
        grad_out,
        grad_gate,
        grad_up,
        grad_down,
        both[:, 0],
        both[:, 1],
    )


def solution(mesh):
    rows, vec, tok = P(("dp", "ctx"), None), P(("dp", "ctx")), P("dp", "ctx", None)
    return jax.shard_map(
        per_device,
        mesh=mesh,
        in_specs=(tok, P("dp", "ctx"), tok) + (rows,) * 7 + (vec, vec),
        out_specs=(tok, tok) + (rows,) * 7 + (vec, vec),
        check_vma=False,
    )
```

```python
import functools

import jax
import jax.numpy as jnp
from jax import lax
from jax.experimental import pallas as pl
from jax.experimental.pallas import tpu as pltpu
from jax.sharding import PartitionSpec as P

H = 16
KV = 8
HD = 96
HALF = HD // 2
LANES = 128
SPAN = 512

EPS = 1e-05
THETA = 100000.0
MASKED = -1e30

BF = jnp.bfloat16
F32 = jnp.float32
MESH = pl.DeviceIdType.MESH
VMEM_LIMIT = 60 * 1024 * 1024


def sds(shape, dtype=BF):
    return jax.ShapeDtypeStruct(tuple(shape), dtype)


def dot_nn(a, b):
    return lax.dot_general(a, b, (((1,), (0,)), ((), ())), preferred_element_type=F32)


def dot_nt(a, b):
    return lax.dot_general(a, b, (((1,), (1,)), ((), ())), preferred_element_type=F32)


def dot_tn(a, b):
    return lax.dot_general(a, b, (((0,), (0,)), ((), ())), preferred_element_type=F32)


class Sizes:
    def __init__(self, dp, ctx):
        self.dp, self.ctx = dp, ctx
        self.outer = 4 if dp % 4 == 0 else dp
        self.inner = dp // self.outer
        self.ys = ctx // 2


class Link:
    def __init__(self, z, send_sems, recv_sems, local_sems):
        self.z = z
        self.d = lax.axis_index("dp")
        self.c = lax.axis_index("ctx")
        self.o, self.i = lax.div(self.d, z.inner), lax.rem(self.d, z.inner)
        self.y, self.k = lax.div(self.c, 2), lax.rem(self.c, 2)
        self.sems = (send_sems, recv_sems, local_sems)
        self.sent, self.inflight, self.local = 0, [], []

    def ctx_dev(self, y, k):
        return (self.d, y * 2 + k)

    def ctx_peers(self):
        n = self.z.ctx
        return [lax.rem(self.c + j, n) for j in range(1, n)]

    def y_peers(self):
        n = self.z.ys
        return [lax.rem(self.y + j, n) for j in range(1, n)]

    def outer_to(self, j):
        return lax.rem(self.o + j, self.z.outer)

    def outer_from(self, j):
        return lax.rem(self.o + self.z.outer - j, self.z.outer)

    def inner_to(self, j):
        return lax.rem(self.i + j, self.z.inner)

    def dp_dev(self, o, i):
        return (o * self.z.inner + i, self.c)

    def barrier(self):
        devices = [(self.d, c) for c in self.ctx_peers()]
        devices += [self.dp_dev(self.outer_to(j), self.i) for j in range(1, self.z.outer)]
        devices += [self.dp_dev(self.o, self.inner_to(j)) for j in range(1, self.z.inner)]
        barrier = pltpu.get_barrier_semaphore()
        for device in devices:
            pl.semaphore_signal(barrier, inc=1, device_id=device, device_id_type=MESH)
        pl.semaphore_wait(barrier, len(devices))

    def put(self, src, dst, device):
        n = self.sent
        self.sent += 1
        copy = pltpu.make_async_remote_copy(
            src_ref=src,
            dst_ref=dst,
            send_sem=self.sems[0].at[n],
            recv_sem=self.sems[1].at[n],
            device_id=device,
            device_id_type=MESH,
        )
        copy.start()
        self.inflight.append(copy)
        return copy

    def keep(self, src, dst):
        copy = pltpu.make_async_copy(src, dst, self.sems[2].at[len(self.local)])
        copy.start()
        self.local.append(copy)
        return copy

    def arrived(self, copy):
        copy.wait_recv()
        self.inflight = [other for other in self.inflight if other is not copy]
        self.landed.append(copy)

    def finish(self):
        for copy in self.inflight:
            copy.wait_recv()
        for copy in self.landed + self.inflight:
            copy.wait_send()
        for copy in self.local:
            copy.wait()

    landed = None


def communicate(z, name, cid, script, ins, outs, scratch=(), filled=()):
    filled = tuple(filled)
    outs = [sds(a.shape, a.dtype) for a in filled] + list(outs)
    ins = tuple(ins) + filled
    n_in, n_out = len(ins), len(outs)
    aliases = {n_in - len(filled) + n: n for n in range(len(filled))}

    def kernel(*refs):
        in_refs, out_refs = refs[:n_in], refs[n_in : n_in + n_out]
        send, recv, local = refs[n_in + n_out : n_in + n_out + 3]
        link = Link(z, send, recv, local)
        link.landed = []
        link.barrier()
        script(link, in_refs, out_refs, refs[n_in + n_out + 3 :])
        link.finish()

    hbm = pl.BlockSpec(memory_space=pltpu.HBM)
    return pl.pallas_call(
        kernel,
        name=name,
        out_shape=list(outs),
        in_specs=[hbm] * n_in,
        out_specs=[hbm] * n_out,
        input_output_aliases=aliases,
        scratch_shapes=[
            pltpu.SemaphoreType.DMA((64,)),
            pltpu.SemaphoreType.DMA((64,)),
            pltpu.SemaphoreType.DMA((16,)),
        ]
        + list(scratch),
        compiler_params=pltpu.CompilerParams(
            collective_id=cid, has_side_effects=True, vmem_limit_bytes=VMEM_LIMIT
        ),
    )(*ins)


def gather_ctx_start(link, src, buf, wait_src=None):
    slot = buf.at[link.c]
    ways = []
    for j in range(1, link.z.ys):
        to = lax.rem(link.y + j, link.z.ys)
        frm = lax.rem(link.y + link.z.ys - j, link.z.ys)
        ways.append((frm, link.put(src, slot, link.ctx_dev(to, link.k))))
    link.put(src, slot, link.ctx_dev(link.y, 1 - link.k))
    return ways


def gather_ctx_forward(link, buf, ways):
    for frm, copy in ways:
        link.arrived(copy)
        slot = buf.at[frm * 2 + link.k]
        link.put(slot, slot, link.ctx_dev(link.y, 1 - link.k))


def exchange_ctx(link, pack, slot_of):
    return [link.put(pack.at[c], slot_of(link.c), (link.d, c)) for c in link.ctx_peers()]


def gather_dp_start(link, slot_of):
    own = slot_of(link.d)
    ways = []
    for j in range(1, link.z.outer):
        copy = link.put(own, own, link.dp_dev(link.outer_to(j), link.i))
        ways.append((link.outer_from(j), copy))
    for j in range(1, link.z.inner):
        link.put(own, own, link.dp_dev(link.o, link.inner_to(j)))
    return ways


def gather_dp_forward(link, slot_of, ways):
    for frm, copy in ways:
        link.arrived(copy)
        slot = slot_of(frm * link.z.inner + link.i)
        for j in range(1, link.z.inner):
            link.put(slot, slot, link.dp_dev(link.o, link.inner_to(j)))


def scatter_inner(link, src, dst):
    for j in range(1, link.z.inner):
        to = link.inner_to(j)
        link.put(src.at[:, to], dst.at[j - 1], link.dp_dev(link.o, to))


def scatter_outer(link, src, dst):
    for j in range(1, link.z.outer):
        to = link.outer_to(j)
        link.put(src.at[to], dst.at[j - 1], link.dp_dev(to, link.i))


def scatter_core(link, src, dst):
    link.put(src.at[:, 1 - link.k], dst, link.ctx_dev(link.y, 1 - link.k))


def scatter_y(link, src, dst):
    for j in range(1, link.z.ys):
        to = lax.rem(link.y + j, link.z.ys)
        link.put(src.at[to], dst.at[j - 1], link.ctx_dev(to, link.k))


class Cargo(Link):
    def put(self, src, dst, device):
        n = self.sent
        self.sent += 1
        copy = pltpu.make_async_remote_copy(
            src_ref=src,
            dst_ref=dst,
            send_sem=self.sems[0].at[n],
            recv_sem=self.sems[1].at[n],
            device_id=device,
            device_id_type=MESH,
        )
        self.inflight.append(copy)
        return copy


def fused_call(z, name, cid, body, grid, in_specs, out_specs, out_shape, args, script, moved, new=(), filled=(), scratch=()):
    filled, moved = tuple(filled), tuple(moved)
    n_arg, n_moved, n_fill = len(args), len(moved), len(filled)
    n_cargo = n_fill + len(new)
    n_out = n_cargo + len(out_shape)
    steps = 1
    for extent in grid:
        steps *= extent

    def kernel(*refs):
        step = 0
        for axis, extent in enumerate(grid):
            step = step * extent + pl.program_id(axis)
        n_in = n_arg + n_moved + n_fill
        arg_refs, moved_refs = refs[:n_arg], refs[n_arg : n_arg + n_moved]
        cargo_refs, out_refs = refs[n_in : n_in + n_cargo], refs[n_in + n_cargo : n_in + n_out]
        send, recv = refs[n_in + n_out : n_in + n_out + 2]
        cargo = Cargo(z, send, recv, None)
        script(cargo, moved_refs, cargo_refs)

        @pl.when(step == 0)
        def _():
            cargo.barrier()
            for copy in cargo.inflight:
                copy.start()

        body(*arg_refs, *out_refs, *refs[n_in + n_out + 2 :])

        @pl.when(step == steps - 1)
        def _():
            for copy in cargo.inflight:
                copy.wait_recv()
            for copy in cargo.inflight:
                copy.wait_send()

    hbm = pl.BlockSpec(memory_space=pltpu.HBM)
    first = n_arg + n_moved
    return pl.pallas_call(
        kernel,
        name=name,
        grid=grid,
        in_specs=list(in_specs) + [hbm] * (n_moved + n_fill),
        out_specs=[hbm] * n_cargo + list(out_specs),
        out_shape=[sds(a.shape, a.dtype) for a in filled] + list(new) + list(out_shape),
        input_output_aliases={first + n: n for n in range(n_fill)},
        scratch_shapes=[pltpu.SemaphoreType.DMA((32,)), pltpu.SemaphoreType.DMA((32,))] + list(scratch),
        compiler_params=pltpu.CompilerParams(
            collective_id=cid, has_side_effects=True, vmem_limit_bytes=VMEM_LIMIT
        ),
    )(*args, *moved, *filled)


def own_outer(link, buf, js):
    for j in js:
        link.put(buf.at[link.d], buf.at[link.d], link.dp_dev(link.outer_to(j), link.i))


def own_inner(link, buf):
    for j in range(1, link.z.inner):
        link.put(buf.at[link.d], buf.at[link.d], link.dp_dev(link.o, link.inner_to(j)))


def pass_inner(link, buf, js):
    for from_j in js:
        slot = buf.at[link.outer_from(from_j) * link.z.inner + link.i]
        for j in range(1, link.z.inner):
            link.put(slot, slot, link.dp_dev(link.o, link.inner_to(j)))


def pass_core(link, buf, parts):
    for j in range(1, link.z.ys):
        at = lax.rem(link.y + link.z.ys - j, link.z.ys) * 2 + link.k
        for part in parts:
            link.put(buf.at[at, part], buf.at[at, part], link.ctx_dev(link.y, 1 - link.k))


def own_y(link, src, buf, parts):
    for part in parts:
        for j in range(1, link.z.ys):
            to = lax.rem(link.y + j, link.z.ys)
            link.put(src.at[part], buf.at[link.c, part], link.ctx_dev(to, link.k))
        link.put(src.at[part], buf.at[link.c, part], link.ctx_dev(link.y, 1 - link.k))


def rotated(u, cos, sin):
    return u * cos + pltpu.roll(u, LANES // 2, 1) * sin


def qkv_kernel(hc, kvc, x_ref, gain_ref, w_ref, cos_ref, sin_ref, n_ref, q_ref, k_ref, v_ref):
    x = x_ref[0, 0].astype(F32)
    scale = lax.rsqrt(jnp.mean(x * x, axis=-1, keepdims=True) + EPS)
    normed = (x * scale * gain_ref[...]).astype(BF)
    n_ref[0, 0] = normed
    full = dot_nn(normed, w_ref[...])
    cos, sin = cos_ref[0], sin_ref[0]
    for h in range(hc + kvc):
        piece = rotated(full[:, h * LANES : (h + 1) * LANES], cos, sin).astype(BF)
        if h < hc:
            q_ref[0, 0, :, h * LANES : (h + 1) * LANES] = piece
        else:
            k_ref[0, 0, :, (h - hc) * LANES : (h - hc + 1) * LANES] = piece
    v_ref[0, 0] = full[:, (hc + kvc) * LANES :].astype(BF)


def qkv_call(z, x_all, gain, w, cos, sin, hc, kvc, script, moved, new, filled):
    ctx, m, r, d = x_all.shape
    row = lambda s, b: (s, b, 0, 0)
    whole = lambda s, b: (0, 0)
    table = pl.BlockSpec((1, r, LANES), lambda s, b: (s, 0, 0))
    return fused_call(
        z,
        "qkv",
        11,
        functools.partial(qkv_kernel, hc, kvc),
        (ctx, m),
        [
            pl.BlockSpec((1, 1, r, d), row),
            pl.BlockSpec((1, d), whole),
            pl.BlockSpec(w.shape, whole, pipeline_mode=pl.Buffered(1)),
            table,
            table,
        ],
        [
            pl.BlockSpec((1, 1, r, d), row),
            pl.BlockSpec((1, 1, r, hc * LANES), row),
            pl.BlockSpec((1, 1, r, kvc * LANES), row),
            pl.BlockSpec((1, 1, r, kvc * LANES), row),
        ],
        [
            sds((ctx, m, r, d)),
            sds((ctx, m, r, hc * LANES)),
            sds((ctx, m, r, kvc * LANES)),
            sds((ctx, m, r, kvc * LANES)),
        ],
        (x_all, gain, w, cos, sin),
        script,
        moved,
        new,
        filled,
    )


def window_of(s, r, ctx):
    blocks = min(ctx, SPAN // r + 1)
    return jnp.maximum(s - (blocks - 1), 0), blocks


def bias_of(s, first, blocks, r, qdoc_ref, kdoc_ref):
    qdoc = qdoc_ref[0, 0]
    pieces = []
    for b in range(blocks):
        kdoc = kdoc_ref[first + b, 0]
        rows = lax.broadcasted_iota(jnp.int32, (r, r), 0) + s * r
        cols = lax.broadcasted_iota(jnp.int32, (r, r), 1) + (first + b) * r
        pieces.append(jnp.where((qdoc == kdoc) & (cols <= rows), 0.0, MASKED))
    return jnp.concatenate(pieces, axis=1)


def attend_kernel(hc, kvc, ctx, q_ref, k_ref, v_ref, qdoc_ref, kdoc_ref, out_ref, lse_ref):
    s = pl.program_id(1)
    r = q_ref.shape[2]
    first, blocks = window_of(s, r, ctx)
    bias = bias_of(s, first, blocks, r, qdoc_ref, kdoc_ref)
    lane = lax.broadcasted_iota(jnp.int32, (r, LANES), 1)
    lse_all = jnp.zeros((r, LANES), F32)
    outs = []
    for h in range(hc):
        g = h * kvc // hc
        q = q_ref[0, 0, :, h * LANES : (h + 1) * LANES]
        k = k_ref[pl.ds(first, blocks), 0, :, g * LANES : (g + 1) * LANES].reshape(blocks * r, LANES)
        v = v_ref[pl.ds(first, blocks), 0, :, g * LANES : (g + 1) * LANES].reshape(blocks * r, LANES)
        scores = dot_nt(q, k) * HD ** (-0.5) + bias
        top = jnp.max(scores, axis=-1, keepdims=True)
        e = jnp.exp(scores - top)
        total = jnp.sum(e, axis=-1, keepdims=True)
        probs = (e * (1.0 / total)).astype(BF)
        outs.append(dot_nn(probs, v)[:, :HD])
        lse_all = jnp.where(lane == h, top + jnp.log(total), lse_all)
    out_ref[0, 0] = jnp.concatenate(outs, axis=1).astype(BF)
    lse_ref[0, 0] = lse_all


def attend_call(z, q, k, v, qdoc, kdoc, hc, kvc, script, moved, new, filled):
    ctx, m, r, _ = q.shape
    row = lambda b, s: (s, b, 0, 0)
    seq = lambda b, s: (0, b, 0, 0)
    return fused_call(
        z,
        "attend",
        12,
        functools.partial(attend_kernel, hc, kvc, ctx),
        (m, ctx),
        [
            pl.BlockSpec((1, 1, r, hc * LANES), row),
            pl.BlockSpec((ctx, 1, r, kvc * LANES), seq),
            pl.BlockSpec((ctx, 1, r, kvc * LANES), seq),
            pl.BlockSpec((1, 1, r, 1), row),
            pl.BlockSpec((ctx, 1, 1, r), seq),
        ],
        [pl.BlockSpec((1, 1, r, hc * HD), row), pl.BlockSpec((1, 1, r, LANES), row)],
        [sds((ctx, m, r, hc * HD)), sds((ctx, m, r, LANES), F32)],
        (q, k, v, qdoc, kdoc),
        script,
        moved,
        new,
        filled,
    )


def attend_back_kernel(
    hc, kvc, ctx, q_ref, k_ref, v_ref, qdoc_ref, kdoc_ref, o_ref, do_ref, lse_ref, cos_ref, sin_ref,
    dq_ref, dkv_ref, dk_acc, dv_acc,
):
    s = pl.program_id(1)
    r = q_ref.shape[2]
    first, blocks = window_of(s, r, ctx)
    bias = bias_of(s, first, blocks, r, qdoc_ref, kdoc_ref)

    @pl.when(s == 0)
    def _():
        dk_acc[...] = jnp.zeros_like(dk_acc)
        dv_acc[...] = jnp.zeros_like(dv_acc)

    cos, sin = cos_ref[s], sin_ref[s]
    lse_all = lse_ref[0, 0]
    for h in range(hc):
        g = h * kvc // hc
        q = q_ref[0, 0, :, h * LANES : (h + 1) * LANES]
        k = k_ref[pl.ds(first, blocks), 0, :, g * LANES : (g + 1) * LANES].reshape(blocks * r, LANES)
        v = v_ref[pl.ds(first, blocks), 0, :, g * LANES : (g + 1) * LANES].reshape(blocks * r, LANES)
        o = o_ref[0, 0, :, h * HD : (h + 1) * HD].astype(F32)
        do = do_ref[0, 0, :, h * HD : (h + 1) * HD]
        delta = jnp.sum(o * do.astype(F32), axis=-1, keepdims=True)
        do = jnp.concatenate([do, jnp.zeros((r, LANES - HD), BF)], axis=1)
        scores = dot_nt(q, k) * HD ** (-0.5) + bias
        probs = jnp.exp(scores - lse_all[:, h : h + 1])
        d_probs = dot_nt(do, v)
        d_scores = (probs * (d_probs - delta) * HD ** (-0.5)).astype(BF)
        dq = dot_nn(d_scores, k)
        dq_ref[0, 0, :, h * LANES : (h + 1) * LANES] = rotated(dq, cos, -sin).astype(BF)
        dk = dot_tn(d_scores, q).reshape(blocks, r, LANES)
        dv = dot_tn(probs.astype(BF), do).reshape(blocks, r, LANES)
        here = slice(g * LANES, (g + 1) * LANES)
        dk_acc[pl.ds(first, blocks), :, here] += dk
        dv_acc[pl.ds(first, blocks), :, here] += dv

    @pl.when(s == ctx - 1)
    def _():
        for b in range(ctx):
            for g in range(kvc):
                here = slice(g * LANES, (g + 1) * LANES)
                at = g * LANES
                dk = rotated(dk_acc[b, :, here], cos_ref[b], -sin_ref[b])
                dkv_ref[b, 0, :, at : at + LANES] = dk.astype(BF)
                at += kvc * LANES
                dkv_ref[b, 0, :, at : at + LANES] = dv_acc[b, :, here].astype(BF)


def attend_back_call(z, q, k, v, qdoc, kdoc, o, do, lse, cos, sin, hc, kvc):
    ctx, m, r, _ = q.shape
    row = lambda b, s: (s, b, 0, 0)
    seq = lambda b, s: (0, b, 0, 0)
    table = pl.BlockSpec((ctx, r, LANES), lambda b, s: (0, 0, 0))
    return pl.pallas_call(
        functools.partial(attend_back_kernel, hc, kvc, ctx),
        name="attend_back",
        grid=(m, ctx),
        in_specs=[
            pl.BlockSpec((1, 1, r, hc * LANES), row),
            pl.BlockSpec((ctx, 1, r, kvc * LANES), seq),
            pl.BlockSpec((ctx, 1, r, kvc * LANES), seq),
            pl.BlockSpec((1, 1, r, 1), row),
            pl.BlockSpec((ctx, 1, 1, r), seq),
            pl.BlockSpec((1, 1, r, hc * HD), row),
            pl.BlockSpec((1, 1, r, hc * HD), row),
            pl.BlockSpec((1, 1, r, LANES), row),
            table,
            table,
        ],
        out_specs=[
            pl.BlockSpec((1, 1, r, hc * LANES), row),
            pl.BlockSpec((ctx, 1, r, 2 * kvc * LANES), seq),
        ],
        out_shape=[sds((ctx, m, r, hc * LANES)), sds((ctx, m, r, 2 * kvc * LANES))],
        scratch_shapes=[
            pltpu.VMEM((ctx, r, kvc * LANES), F32),
            pltpu.VMEM((ctx, r, kvc * LANES), F32),
        ],
        compiler_params=pltpu.CompilerParams(vmem_limit_bytes=VMEM_LIMIT),
    )(q, k, v, qdoc, kdoc, o, do, lse, cos, sin)


def mlp_kernel(
    k_ref, x_ref, cot_ref, gate_ref, up_ref, down_ref,
    hid_ref, dg_ref, du_ref, dn_other, dn_mine, out_other, out_mine,
):
    x, cot = x_ref[0, 0], cot_ref[0, 0]
    gate, up = dot_nn(x, gate_ref[...]), dot_nn(x, up_ref[...])
    d_hidden = dot_nt(cot, down_ref[...])
    sg = jax.nn.sigmoid(gate)
    act = gate * sg
    hidden = (act * up).astype(BF)
    hid_ref[0, 0] = hidden
    d_gate = (d_hidden * up * sg * (1.0 + gate * (1.0 - sg))).astype(BF)
    d_up = (d_hidden * act).astype(BF)
    dg_ref[0, 0] = d_gate
    du_ref[0, 0] = d_up
    out = dot_nn(hidden, down_ref[...]).astype(BF)
    dn = (dot_nt(d_gate, gate_ref[...]) + dot_nt(d_up, up_ref[...])).astype(BF)

    @pl.when(pl.program_id(0) == 0)
    def _():
        out_other[0, 0] = out
        dn_other[0, 0] = dn

    @pl.when(pl.program_id(0) == 1)
    def _():
        out_mine[0, 0] = out
        dn_mine[0, 0] = dn


def mlp_call(z, core, x, cot, gate, up, down):
    ctx, m, r, d = x.shape
    f = down.shape[0]
    row = lambda a, y, b, k: (y * 2 + a * k[0] + (1 - a) * (1 - k[0]), b, 0, 0)
    whole = lambda a, y, b, k: (0, 0)
    other = lambda a, y, b, k: (y + a * (z.ys - 1 - y), b + a * (m - 1 - b), 0, 0)
    mine = lambda a, y, b, k: (a * y, a * b, 0, 0)
    block = lambda width, at: pl.BlockSpec((1, 1, r, width), at)
    part = sds((z.ys, m, r, d))
    return pl.pallas_call(
        mlp_kernel,
        name="mlp",
        grid_spec=pltpu.PrefetchScalarGridSpec(
            num_scalar_prefetch=1,
            grid=(2, z.ys, m),
            in_specs=[
                block(d, row),
                block(d, row),
                pl.BlockSpec(gate.shape, whole, pipeline_mode=pl.Buffered(1)),
                pl.BlockSpec(up.shape, whole, pipeline_mode=pl.Buffered(1)),
                pl.BlockSpec(down.shape, whole, pipeline_mode=pl.Buffered(1)),
            ],
            out_specs=[block(f, row), block(f, row), block(f, row)]
            + [block(d, other), block(d, mine), block(d, other), block(d, mine)],
        ),
        out_shape=[sds((ctx, m, r, f))] * 3 + [part] * 4,
        compiler_params=pltpu.CompilerParams(vmem_limit_bytes=VMEM_LIMIT),
    )(core, x, cot, gate, up, down)


def pad_heads(w, heads, split):
    rows = w.shape[0]
    if split:
        w = jnp.pad(w.reshape(rows, heads, 2, HALF), ((0, 0), (0, 0), (0, 0), (0, LANES // 2 - HALF)))
    else:
        w = jnp.pad(w.reshape(rows, heads, HD), ((0, 0), (0, 0), (0, LANES - HD)))
    return w.reshape(rows, heads * LANES)


def unpad_heads(w, heads, split):
    if split:
        w = w.reshape(w.shape[:-1] + (heads, 2, LANES // 2))[..., :HALF]
    else:
        w = w.reshape(w.shape[:-1] + (heads, LANES))[..., :HD]
    return w.reshape(w.shape[: w.ndim - (3 if split else 2)] + (heads * HD,))


def rope_tables(ctx, r):
    frequency = THETA ** (-(jnp.arange(HALF, dtype=F32) * (2.0 / HD)))
    angles = jnp.arange(ctx * r, dtype=jnp.int32).astype(F32)[:, None] * frequency[None, :]
    pad = ((0, 0), (0, LANES // 2 - HALF))
    cos, sin = jnp.pad(jnp.cos(angles), pad), jnp.pad(jnp.sin(angles), pad)
    cos = jnp.concatenate([cos, cos], axis=1).reshape(ctx, r, LANES)
    sin = jnp.concatenate([-sin, sin], axis=1).reshape(ctx, r, LANES)
    return cos, sin


def per_device(
    inputs, segments, cotangent, w_query, w_key, w_value, w_out, w_gate, w_up, w_down, gain_attn, gain_ffn
):
    z = Sizes(lax.axis_size("dp"), lax.axis_size("ctx"))
    dp, ctx, outer, inner, ys = z.dp, z.ctx, z.outer, z.inner, z.ys
    m, r, d = inputs.shape
    rows = w_query.shape[0]
    frows, ff = w_down.shape[0], w_gate.shape[1]
    f = ff // ctx
    hc, kvc = H // ctx, KV // ctx
    width = (hc + 2 * kvc) * LANES
    c = lax.axis_index("ctx")
    di = lax.axis_index("dp")
    oi, ii = di // inner, di % inner
    yi, ki = c // 2, c % 2
    dyn = lambda a, at, axis: lax.dynamic_index_in_dim(a, at, axis, keepdims=False)

    pack_qkv = jnp.concatenate(
        [
            pad_heads(w_query, H, True).reshape(rows, ctx, hc * LANES),
            pad_heads(w_key, KV, True).reshape(rows, ctx, kvc * LANES),
            pad_heads(w_value, KV, False).reshape(rows, ctx, kvc * LANES),
        ],
        axis=2,
    ).transpose(1, 0, 2)
    by_rank = lambda w: w.reshape(rows, dp, ctx, frows).transpose(2, 0, 1, 3).reshape(ctx, rows, f)
    pack_gate, pack_up = by_rank(w_gate), by_rank(w_up)
    gains = jnp.stack([gain_attn, gain_ffn]).astype(F32)
    gains = jnp.pad(gains, ((0, 6), (0, LANES - rows)))

    far = list(range(1, outer))
    near = [j for j in far if j in (1, outer - 1)]
    mid_way = [j for j in far if j not in near]

    def first_script(link, ins, outs, scratch):
        x, seg, qkv, gain, wo, pg, pu, wd = ins
        x_all, seg_all, g_qkv, g_gain, g_out, g_gate, g_up, g_down = outs
        (hold,) = scratch
        load = pltpu.make_async_copy(x, hold, link.sems[2].at[15])
        load.start()
        mine = [
            link.keep(qkv.at[link.c], g_qkv.at[link.d, link.c]),
            link.keep(gain, g_gain.at[link.d, link.c]),
            link.keep(wo, g_out.at[link.d, link.y, link.k]),
            link.keep(seg, seg_all.at[link.c]),
        ]
        a2a = exchange_ctx(link, qkv, lambda s: g_qkv.at[link.d, s])
        a2a += [link.put(gain, g_gain.at[link.d, link.c], (link.d, p)) for p in link.ctx_peers()]
        for p in link.ctx_peers():
            link.put(seg, seg_all.at[link.c], (link.d, p))
        over_y = [
            link.put(wo, g_out.at[link.d, link.y, link.k], link.ctx_dev(p, link.k)) for p in link.y_peers()
        ]
        ways_x = gather_ctx_start(link, x, x_all)
        exchange_ctx(link, pg, lambda s: g_gate.at[link.d, s])
        exchange_ctx(link, pu, lambda s: g_up.at[link.d, s])
        for copy in a2a:
            link.arrived(copy)
        for copy in mine:
            copy.wait()
        link.local = []
        small = [lambda s: g_qkv.at[s], lambda s: g_gain.at[s]]
        ways = [gather_dp_start(link, slot) for slot in small]
        for copy in over_y:
            link.arrived(copy)
        out_slot = lambda s: g_out.at[s, :, link.k]
        ways_out = gather_dp_start(link, out_slot)
        load.wait()
        store = pltpu.make_async_copy(hold, x_all.at[link.c], link.sems[2].at[14])
        store.start()
        link.keep(pg.at[link.c], g_gate.at[link.d, link.c])
        link.keep(pu.at[link.c], g_up.at[link.d, link.c])
        link.keep(wd, g_down.at[link.d])
        for slot, way in zip(small, ways):
            gather_dp_forward(link, slot, way)
        gather_ctx_forward(link, x_all, ways_x)
        gather_dp_forward(link, out_slot, ways_out)
        for copy in list(link.inflight):
            link.arrived(copy)
        both = g_out.at[:, :, link.k]
        link.put(both, both, link.ctx_dev(link.y, 1 - link.k))
        store.wait()

    x_all, seg_all, g_qkv, g_gain, g_out, g_gate, g_up, g_down = communicate(
        z,
        "gather_first",
        1,
        first_script,
        (inputs, segments, pack_qkv, gains, w_out, pack_gate, pack_up, w_down),
        (
            sds((ctx, m, r, d)),
            sds((ctx, m, r), jnp.int32),
            sds((dp, ctx, rows, width)),
            sds((dp, ctx, 8, LANES), F32),
            sds((dp, ys, 2, rows, d)),
            sds((dp, ctx, rows, f)),
            sds((dp, ctx, rows, f)),
            sds((dp, frows, d)),
        ),
        [pltpu.VMEM((m, r, d), BF)],
    )
    gain_a = g_gain[:, :, 0, :rows].reshape(1, d)
    gain_f = g_gain[:, :, 1, :rows].reshape(1, d)
    wqkv = g_qkv.reshape(d, width)
    wo = g_out.reshape(d, d)
    cos, sin = rope_tables(ctx, r)
    qdoc = seg_all.reshape(ctx, m, r, 1)
    kdoc = seg_all.reshape(ctx, m, 1, r)
    early, late = range(m // 2), range(m // 2, m)

    def qkv_cargo(cargo, moved, bufs):
        (cot,), (g_gate, g_up, cot_all) = moved, bufs
        own_y(cargo, cot, cot_all, early)
        for buf in (g_gate, g_up):
            own_outer(cargo, buf, near[:1])
            own_inner(cargo, buf)

    g_gate, g_up, cot_all, normed_a, q, k, v = qkv_call(
        z, x_all, gain_a, wqkv, cos, sin, hc, kvc,
        qkv_cargo, (cotangent,), (sds((ctx, m, r, d)),), (g_gate, g_up),
    )

    def attend_cargo(cargo, moved, bufs):
        (cot,), (g_gate, g_up, cot_all) = moved, bufs
        own_y(cargo, cot, cot_all, late)
        pass_core(cargo, cot_all, early)
        for buf in (g_gate, g_up):
            own_outer(cargo, buf, near[1:])
            pass_inner(cargo, buf, near[:1])

    g_gate, g_up, cot_all, att, lse = attend_call(
        z, q, k, v, qdoc, kdoc, hc, kvc, attend_cargo, (cotangent,), (), (g_gate, g_up, cot_all)
    )

    def second_script(link, ins, outs, scratch):
        att, cot = ins[:2]
        g_gate, g_up, g_down, cot_all, att_all = outs
        (hold,) = scratch
        load = pltpu.make_async_copy(cot, hold, link.sems[2].at[15])
        load.start()
        link.keep(att.at[link.c], att_all.at[link.c])
        exchange_ctx(link, att, lambda s: att_all.at[s])
        own_outer(link, g_down, near)
        for buf in (g_gate, g_up):
            pass_inner(link, buf, near[1:])
        pass_core(link, cot_all, late)
        load.wait()
        store = pltpu.make_async_copy(hold, cot_all.at[link.c], link.sems[2].at[14])
        store.start()
        store.wait()

    g_gate, g_up, g_down, cot_all, att_all = communicate(
        z,
        "exchange_heads",
        2,
        second_script,
        (att, cotangent),
        (sds(att.shape),),
        [pltpu.VMEM((m, r, d), BF)],
        (g_gate, g_up, g_down, cot_all),
    )

    att_rows = att_all.transpose(1, 2, 0, 3).reshape(m * r, H * HD)
    residual = inputs.astype(F32)
    mid = residual + dot_nn(att_rows, wo).reshape(m, r, d)
    scale_f = lax.rsqrt(jnp.mean(mid * mid, axis=-1, keepdims=True) + EPS)
    normed = (mid * scale_f * gain_f).astype(BF)

    def third_script(link, ins, outs, scratch):
        x, (g_gate, g_up, g_down, x_all), (hold,) = ins[0], outs, scratch
        load = pltpu.make_async_copy(x, hold, link.sems[2].at[15])
        load.start()
        ways = gather_ctx_start(link, x, x_all)
        bufs = (g_gate, g_up, g_down)
        coming = []
        for buf in bufs:
            for j in mid_way:
                start = link.put(buf.at[link.d], buf.at[link.d], link.dp_dev(link.outer_to(j), link.i))
                coming.append((buf, j, start))
        own_inner(link, g_down)
        pass_inner(link, g_down, near)
        load.wait()
        store = pltpu.make_async_copy(hold, x_all.at[link.c], link.sems[2].at[14])
        store.start()
        for n, (buf, j, copy) in enumerate(coming):
            if n == len(coming) - 1:
                gather_ctx_forward(link, x_all, ways)
            link.arrived(copy)
            pass_inner(link, buf, [j])
        store.wait()

    g_gate, g_up, g_down, normed_all = communicate(
        z,
        "gather_third",
        3,
        third_script,
        (normed,),
        (sds((ctx, m, r, d)),),
        [pltpu.VMEM((m, r, d), BF)],
        (g_gate, g_up, g_down),
    )
    w_gate_c, w_up_c, w_down_c = g_gate.reshape(d, f), g_up.reshape(d, f), g_down.reshape(f, d)

    core = ki.astype(jnp.int32).reshape(1)
    hidden, d_gate, d_up, dn_other, dn_mine, out_other, out_mine = mlp_call(
        z, core, normed_all, cot_all, w_gate_c, w_up_c, w_down_c
    )

    dp_perm = lambda fn: [(o * inner + i, fn(o, i)) for o in range(outer) for i in range(inner)]
    ctx_perm = lambda fn: [(y * 2 + k, fn(y, k)) for y in range(ys) for k in range(2)]
    wide = lambda a: a.astype(F32)
    flat = lambda a: a.reshape(ctx * m * r, a.shape[-1])

    def after(a, dep):
        return lax.optimization_barrier((a, dep))[0]

    def to_core(a):
        return lax.ppermute(a, "ctx", ctx_perm(lambda y, k: y * 2 + 1 - k))

    def to_y(mine, got, dim=0):
        both = lambda at: wide(dyn(mine, at, dim)) + wide(dyn(got, at, dim))
        came = [
            lax.ppermute(
                both((yi + j) % ys).astype(BF), "ctx", ctx_perm(lambda y, k: (y + j) % ys * 2 + k)
            )
            for j in range(1, ys)
        ]
        return both(yi), came

    def to_inner(part):
        return [
            lax.ppermute(
                dyn(part, (ii + j) % inner, 1), "dp", dp_perm(lambda o, i: o * inner + (i + j) % inner)
            )
            for j in range(1, inner)
        ]

    def to_outer(part, came):
        both = lambda at: wide(part[at, ii]) + sum(wide(dyn(a, at, 0)) for a in came)
        got = [
            lax.ppermute(
                both((oi + j) % outer).astype(BF), "dp", dp_perm(lambda o, i: (o + j) % outer * inner + i)
            )
            for j in range(1, outer)
        ]
        return both(oi), got

    close = lambda own, came: own + sum(wide(a) for a in came)

    dn_got = to_core(dn_other)
    part_down = dot_tn(flat(hidden), flat(cot_all)).astype(BF).reshape(outer, inner, frows, d)
    down_x = to_inner(part_down)
    dn_own, dn_came = to_y(dn_mine, dn_got)
    shape_g = (outer, inner, ctx, rows, f)
    part_gate = dot_tn(flat(normed_all), flat(d_gate)).astype(BF).reshape(shape_g)
    gate_x = to_inner(part_gate)
    part_up = dot_tn(flat(normed_all), flat(d_up)).astype(BF).reshape(shape_g)
    up_x = to_inner(part_up)
    out_got = to_core(out_other)

    d_normed = close(dn_own, dn_came)
    cot32 = cotangent.astype(F32)
    e = d_normed * gain_f
    d_mid = cot32 + (
        scale_f * e - mid * (scale_f * scale_f * scale_f) * jnp.mean(e * mid, axis=-1, keepdims=True)
    )
    d_mid_low = d_mid.astype(BF).reshape(m * r, d)
    d_att = dot_nt(d_mid_low, wo).astype(BF)
    d_att = d_att.reshape(m, r, ctx, hc * HD).transpose(2, 0, 1, 3)

    def fourth_script(link, ins, outs, scratch):
        link.keep(ins[0].at[link.c], outs[0].at[link.c])
        exchange_ctx(link, ins[0], lambda s: outs[0].at[s])

    (d_att_all,) = communicate(z, "exchange_back", 6, fourth_script, (d_att,), (sds(d_att.shape),))

    part_out = dot_tn(att_rows, d_mid_low).astype(BF).reshape(dp, ys, 2, rows, d)
    po_got = to_core(dyn(part_out, 1 - ki, 2))
    down_own, down_z = to_outer(part_down, after(down_x, d_att))
    gate_own, gate_z = to_outer(part_gate, after(gate_x, d_att_all))
    out_own, out_came = to_y(after(out_mine, d_att_all), out_got)
    dq, dkv = attend_back_call(z, q, k, v, qdoc, kdoc, att, d_att_all, lse, cos, sin, hc, kvc)

    part_q = dot_tn(flat(normed_a), flat(dq)).astype(BF).reshape(outer, inner, ctx, rows, hc * LANES)
    q_x = to_inner(part_q)
    part_kv = dot_tn(flat(normed_a), flat(dkv)).astype(BF).reshape(outer, inner, ctx, rows, 2 * kvc * LANES)
    kv_x = to_inner(part_kv)
    da = dot_nt(flat(dq), wqkv[:, : hc * LANES]) + dot_nt(flat(dkv), wqkv[:, hc * LANES :])
    da = da.astype(BF).reshape(ys, 2, m, r, d)
    da_own, da_came = to_y(dyn(da, ki, 1), to_core(dyn(da, 1 - ki, 1)))
    up_own, up_z = to_outer(part_up, after(up_x, dq))
    po_own, po_came = to_y(dyn(after(part_out, dq), ki, 2), po_got, 1)
    q_own, q_z = to_outer(part_q, q_x)
    kv_own, kv_z = to_outer(part_kv, kv_x)
    po = close(po_own, po_came).astype(BF).reshape(outer, inner, rows, d)
    po_own, po_z = to_outer(po, to_inner(po))
    outputs = mid + close(out_own, after(out_came, dq))
    grad_down = close(down_own, after(down_z, part_kv))
    gate_mine = close(gate_own, after(gate_z, part_kv)).astype(BF)
    up_mine = close(up_own, after(up_z, da_own)).astype(BF)
    d_normed_a = close(da_own, da_came)
    scale_a = lax.rsqrt(jnp.mean(residual * residual, axis=-1, keepdims=True) + EPS)
    e = d_normed_a * gain_a
    input_grad = d_mid + (
        scale_a * e - residual * (scale_a * scale_a * scale_a) * jnp.mean(e * residual, axis=-1, keepdims=True)
    )
    q_mine = close(q_own, q_z).astype(BF)
    kv_mine = close(kv_own, kv_z).astype(BF)
    grad_out = close(po_own, po_z)

    def seventh_script(link, ins, outs, scratch):
        for src, dst in zip(ins, outs):
            link.keep(src.at[link.c], dst.at[link.c])
            exchange_ctx(link, src, lambda s: dst.at[s])

    last = (gate_mine, up_mine, q_mine, kv_mine)
    gate_all, up_all, q_all, kv_all = communicate(
        z, "reduce_last", 9, seventh_script, last, [sds(a.shape) for a in last]
    )
    spread = lambda a: wide(a).reshape(ctx, rows, dp, frows).transpose(1, 2, 0, 3).reshape(rows, ff)
    grad_gate, grad_up = spread(gate_all), spread(up_all)
    cols = lambda a, heads, split: (
        unpad_heads(wide(a), heads, split).transpose(1, 0, 2).reshape(rows, ctx * heads * HD)
    )
    grad_query = cols(q_all, hc, True)
    grad_key = cols(kv_all[:, :, : kvc * LANES], kvc, True)
    grad_value = cols(kv_all[:, :, kvc * LANES :], kvc, False)

    along = lambda pairs, gain: sum(jnp.sum(wide(w) * g, axis=1) for w, g in pairs) / wide(gain)
    grad_gain_a = along(((w_query, grad_query), (w_key, grad_key), (w_value, grad_value)), gain_attn)
    grad_gain_f = along(((w_gate, grad_gate), (w_up, grad_up)), gain_ffn)
    return (
        outputs,
        input_grad,
        grad_query,
        grad_key,
        grad_value,
        grad_out,
        grad_gate,
        grad_up,
        grad_down,
        grad_gain_a,
        grad_gain_f,
    )


def solution(mesh):
    rows, vec, tok = P(("dp", "ctx"), None), P(("dp", "ctx")), P("dp", "ctx", None)
    return jax.shard_map(
        per_device,
        mesh=mesh,
        in_specs=(tok, P("dp", "ctx"), tok) + (rows,) * 7 + (vec, vec),
        out_specs=(tok, tok) + (rows,) * 7 + (vec, vec),
        check_vma=False,
    )
```

```python
import functools

import jax
import jax.numpy as jnp
from jax import lax
from jax.experimental import pallas as pl
from jax.experimental.pallas import tpu as pltpu
from jax.sharding import PartitionSpec as P

H = 16
KV = 8
HD = 96
HALF = HD // 2
LANES = 128
SPAN = 512

EPS = 1e-05
THETA = 100000.0
MASKED = -1e30

BF = jnp.bfloat16
F32 = jnp.float32
MESH = pl.DeviceIdType.MESH
VMEM_LIMIT = 60 * 1024 * 1024


def sds(shape, dtype=BF):
    return jax.ShapeDtypeStruct(tuple(shape), dtype)


def dot_nn(a, b):
    return lax.dot_general(a, b, (((1,), (0,)), ((), ())), preferred_element_type=F32)


def dot_nt(a, b):
    return lax.dot_general(a, b, (((1,), (1,)), ((), ())), preferred_element_type=F32)


def dot_tn(a, b):
    return lax.dot_general(a, b, (((0,), (0,)), ((), ())), preferred_element_type=F32)


class Sizes:
    def __init__(self, dp, ctx):
        self.dp, self.ctx = dp, ctx
        self.outer = 4 if dp % 4 == 0 else dp
        self.inner = dp // self.outer
        self.ys = ctx // 2


class Link:
    def __init__(self, z, send_sems, recv_sems, local_sems):
        self.z = z
        self.d = lax.axis_index("dp")
        self.c = lax.axis_index("ctx")
        self.o, self.i = lax.div(self.d, z.inner), lax.rem(self.d, z.inner)
        self.y, self.k = lax.div(self.c, 2), lax.rem(self.c, 2)
        self.sems = (send_sems, recv_sems, local_sems)
        self.sent, self.inflight, self.local = 0, [], []

    def ctx_dev(self, y, k):
        return (self.d, y * 2 + k)

    def slot(self, y, rel):
        return y + self.z.ys if rel else y * 2 + self.k

    def slot_across(self, y, rel):
        return y if rel else y * 2 + self.k

    def ctx_peers(self):
        n = self.z.ctx
        return [lax.rem(self.c + j, n) for j in range(1, n)]

    def y_peers(self):
        n = self.z.ys
        return [lax.rem(self.y + j, n) for j in range(1, n)]

    def outer_to(self, j):
        return lax.rem(self.o + j, self.z.outer)

    def outer_from(self, j):
        return lax.rem(self.o + self.z.outer - j, self.z.outer)

    def inner_to(self, j):
        return lax.rem(self.i + j, self.z.inner)

    def dp_dev(self, o, i):
        return (o * self.z.inner + i, self.c)

    def barrier(self, core_only=False):
        devices = [(self.d, c) for c in self.ctx_peers()]
        if core_only:
            devices = [self.ctx_dev(self.y, 1 - self.k)]
            self.signal_all(devices)
            return
        devices += [self.dp_dev(self.outer_to(j), self.i) for j in range(1, self.z.outer)]
        devices += [self.dp_dev(self.o, self.inner_to(j)) for j in range(1, self.z.inner)]
        self.signal_all(devices)

    def signal_all(self, devices):
        barrier = pltpu.get_barrier_semaphore()
        for device in devices:
            pl.semaphore_signal(barrier, inc=1, device_id=device, device_id_type=MESH)
        pl.semaphore_wait(barrier, len(devices))

    def put(self, src, dst, device):
        n = self.sent
        self.sent += 1
        copy = pltpu.make_async_remote_copy(
            src_ref=src,
            dst_ref=dst,
            send_sem=self.sems[0].at[n],
            recv_sem=self.sems[1].at[n],
            device_id=device,
            device_id_type=MESH,
        )
        copy.start()
        self.inflight.append(copy)
        return copy

    def keep(self, src, dst):
        copy = pltpu.make_async_copy(src, dst, self.sems[2].at[len(self.local)])
        copy.start()
        self.local.append(copy)
        return copy

    def arrived(self, copy):
        copy.wait_recv()
        self.inflight = [other for other in self.inflight if other is not copy]
        self.landed.append(copy)

    def finish(self):
        for copy in self.inflight:
            copy.wait_recv()
        for copy in self.landed + self.inflight:
            copy.wait_send()
        for copy in self.local:
            copy.wait()

    landed = None


def communicate(z, name, cid, script, ins, outs, scratch=(), filled=()):
    filled = tuple(filled)
    outs = [sds(a.shape, a.dtype) for a in filled] + list(outs)
    ins = tuple(ins) + filled
    n_in, n_out = len(ins), len(outs)
    aliases = {n_in - len(filled) + n: n for n in range(len(filled))}

    def kernel(*refs):
        in_refs, out_refs = refs[:n_in], refs[n_in : n_in + n_out]
        send, recv, local = refs[n_in + n_out : n_in + n_out + 3]
        link = Link(z, send, recv, local)
        link.landed = []
        link.barrier()
        script(link, in_refs, out_refs, refs[n_in + n_out + 3 :])
        link.finish()

    hbm = pl.BlockSpec(memory_space=pltpu.HBM)
    return pl.pallas_call(
        kernel,
        name=name,
        out_shape=list(outs),
        in_specs=[hbm] * n_in,
        out_specs=[hbm] * n_out,
        input_output_aliases=aliases,
        scratch_shapes=[
            pltpu.SemaphoreType.DMA((64,)),
            pltpu.SemaphoreType.DMA((64,)),
            pltpu.SemaphoreType.DMA((16,)),
        ]
        + list(scratch),
        compiler_params=pltpu.CompilerParams(
            collective_id=cid, has_side_effects=True, vmem_limit_bytes=VMEM_LIMIT
        ),
    )(*ins)


def gather_ctx_start(link, src, buf, rel=False):
    ways = []
    slot = buf.at[link.slot(link.y, rel)]
    for j in range(1, link.z.ys):
        to = lax.rem(link.y + j, link.z.ys)
        frm = lax.rem(link.y + link.z.ys - j, link.z.ys)
        ways.append((frm, link.put(src, slot, link.ctx_dev(to, link.k))))
    link.put(src, buf.at[link.slot_across(link.y, rel)], link.ctx_dev(link.y, 1 - link.k))
    return ways


def gather_ctx_forward(link, buf, ways, rel=False):
    for frm, copy in ways:
        link.arrived(copy)
        link.put(
            buf.at[link.slot(frm, rel)], buf.at[link.slot_across(frm, rel)], link.ctx_dev(link.y, 1 - link.k)
        )


def exchange_ctx(link, pack, slot_of):
    return [link.put(pack.at[c], slot_of(link.c), (link.d, c)) for c in link.ctx_peers()]


def gather_dp_start(link, slot_of):
    own = slot_of(link.d)
    ways = []
    for j in range(1, link.z.outer):
        copy = link.put(own, own, link.dp_dev(link.outer_to(j), link.i))
        ways.append((link.outer_from(j), copy))
    for j in range(1, link.z.inner):
        link.put(own, own, link.dp_dev(link.o, link.inner_to(j)))
    return ways


def gather_dp_forward(link, slot_of, ways):
    for frm, copy in ways:
        link.arrived(copy)
        slot = slot_of(frm * link.z.inner + link.i)
        for j in range(1, link.z.inner):
            link.put(slot, slot, link.dp_dev(link.o, link.inner_to(j)))


def scatter_inner(link, src, dst):
    for j in range(1, link.z.inner):
        to = link.inner_to(j)
        link.put(src.at[:, to], dst.at[j - 1], link.dp_dev(link.o, to))


def scatter_outer(link, src, dst, js):
    for j in js:
        to = link.outer_to(j)
        link.put(src.at[to], dst.at[j - 1], link.dp_dev(to, link.i))


def scatter_core(link, src, dst):
    link.put(src.at[:, 1 - link.k], dst, link.ctx_dev(link.y, 1 - link.k))


def scatter_y(link, src, dst):
    for j in range(1, link.z.ys):
        to = lax.rem(link.y + j, link.z.ys)
        link.put(src.at[to], dst.at[j - 1], link.ctx_dev(to, link.k))


class Cargo(Link):
    def put(self, src, dst, device):
        n = self.sent
        self.sent += 1
        copy = pltpu.make_async_remote_copy(
            src_ref=src,
            dst_ref=dst,
            send_sem=self.sems[0].at[n],
            recv_sem=self.sems[1].at[n],
            device_id=device,
            device_id_type=MESH,
        )
        self.inflight.append(copy)
        return copy


def fused_call(z, name, cid, body, grid, in_specs, out_specs, out_shape, args, script, moved, new=(), filled=(), scratch=()):
    filled, moved = tuple(filled), tuple(moved)
    n_arg, n_moved, n_fill = len(args), len(moved), len(filled)
    n_cargo = n_fill + len(new)
    n_out = n_cargo + len(out_shape)
    steps = 1
    for extent in grid:
        steps *= extent

    def kernel(*refs):
        step = 0
        for axis, extent in enumerate(grid):
            step = step * extent + pl.program_id(axis)
        n_in = n_arg + n_moved + n_fill
        arg_refs, moved_refs = refs[:n_arg], refs[n_arg : n_arg + n_moved]
        cargo_refs, out_refs = refs[n_in : n_in + n_cargo], refs[n_in + n_cargo : n_in + n_out]
        send, recv = refs[n_in + n_out : n_in + n_out + 2]
        cargo = Cargo(z, send, recv, None)
        script(cargo, moved_refs, cargo_refs)

        @pl.when(step == 0)
        def _():
            cargo.barrier()
            for copy in cargo.inflight:
                copy.start()

        body(*arg_refs, *out_refs, *refs[n_in + n_out + 2 :])

        @pl.when(step == steps - 1)
        def _():
            for copy in cargo.inflight:
                copy.wait_recv()
            for copy in cargo.inflight:
                copy.wait_send()

    hbm = pl.BlockSpec(memory_space=pltpu.HBM)
    first = n_arg + n_moved
    return pl.pallas_call(
        kernel,
        name=name,
        grid=grid,
        in_specs=list(in_specs) + [hbm] * (n_moved + n_fill),
        out_specs=[hbm] * n_cargo + list(out_specs),
        out_shape=[sds(a.shape, a.dtype) for a in filled] + list(new) + list(out_shape),
        input_output_aliases={first + n: n for n in range(n_fill)},
        scratch_shapes=[pltpu.SemaphoreType.DMA((32,)), pltpu.SemaphoreType.DMA((32,))] + list(scratch),
        compiler_params=pltpu.CompilerParams(
            collective_id=cid, has_side_effects=True, vmem_limit_bytes=VMEM_LIMIT
        ),
    )(*args, *moved, *filled)


def ring_outer(link, slot_of, step):
    slot = slot_of(link.outer_from(step - 1) * link.z.inner + link.i)
    return link.put(slot, slot, link.dp_dev(link.outer_to(1), link.i))


def pass_inner(link, slot_of, step):
    slot = slot_of(link.outer_from(step) * link.z.inner + link.i)
    for j in range(1, link.z.inner):
        link.put(slot, slot, link.dp_dev(link.o, link.inner_to(j)))


def pass_core(link, buf, parts):
    for j in range(1, link.z.ys):
        at = lax.rem(link.y + link.z.ys - j, link.z.ys)
        for part in parts:
            src, dst = buf.at[link.slot(at, True), part], buf.at[link.slot_across(at, True), part]
            link.put(src, dst, link.ctx_dev(link.y, 1 - link.k))


def own_y(link, src, buf, parts):
    for part in parts:
        slot = buf.at[link.slot(link.y, True), part]
        for j in range(1, link.z.ys):
            to = lax.rem(link.y + j, link.z.ys)
            link.put(src.at[part], slot, link.ctx_dev(to, link.k))
        slot = buf.at[link.slot_across(link.y, True), part]
        link.put(src.at[part], slot, link.ctx_dev(link.y, 1 - link.k))


def rotated(u, cos, sin):
    return u * cos + pltpu.roll(u, LANES // 2, 1) * sin


def qkv_kernel(hc, kvc, x_ref, gain_ref, w_ref, cos_ref, sin_ref, n_ref, q_ref, k_ref, v_ref):
    x = x_ref[0, 0].astype(F32)
    scale = lax.rsqrt(jnp.mean(x * x, axis=-1, keepdims=True) + EPS)
    normed = (x * scale * gain_ref[...]).astype(BF)
    n_ref[0, 0] = normed
    full = dot_nn(normed, w_ref[...])
    cos, sin = cos_ref[0], sin_ref[0]
    for h in range(hc + kvc):
        piece = rotated(full[:, h * LANES : (h + 1) * LANES], cos, sin).astype(BF)
        if h < hc:
            q_ref[0, 0, :, h * LANES : (h + 1) * LANES] = piece
        else:
            k_ref[0, 0, :, (h - hc) * LANES : (h - hc + 1) * LANES] = piece
    v_ref[0, 0] = full[:, (hc + kvc) * LANES :].astype(BF)


def qkv_call(z, x_all, gain, w, cos, sin, hc, kvc, script, moved, new, filled):
    ctx, m, r, d = x_all.shape
    row = lambda s, b: (s, b, 0, 0)
    whole = lambda s, b: (0, 0)
    table = pl.BlockSpec((1, r, LANES), lambda s, b: (s, 0, 0))
    return fused_call(
        z,
        "qkv",
        11,
        functools.partial(qkv_kernel, hc, kvc),
        (ctx, m),
        [
            pl.BlockSpec((1, 1, r, d), row),
            pl.BlockSpec((1, d), whole),
            pl.BlockSpec(w.shape, whole, pipeline_mode=pl.Buffered(1)),
            table,
            table,
        ],
        [
            pl.BlockSpec((1, 1, r, d), row),
            pl.BlockSpec((1, 1, r, hc * LANES), row),
            pl.BlockSpec((1, 1, r, kvc * LANES), row),
            pl.BlockSpec((1, 1, r, kvc * LANES), row),
        ],
        [
            sds((ctx, m, r, d)),
            sds((ctx, m, r, hc * LANES)),
            sds((ctx, m, r, kvc * LANES)),
            sds((ctx, m, r, kvc * LANES)),
        ],
        (x_all, gain, w, cos, sin),
        script,
        moved,
        new,
        filled,
    )


def window_of(s, r, ctx):
    blocks = min(ctx, SPAN // r + 1)
    return jnp.maximum(s - (blocks - 1), 0), blocks


def bias_of(s, first, blocks, r, qdoc_ref, kdoc_ref):
    qdoc = qdoc_ref[0, 0]
    pieces = []
    for b in range(blocks):
        kdoc = kdoc_ref[first + b, 0]
        rows = lax.broadcasted_iota(jnp.int32, (r, r), 0) + s * r
        cols = lax.broadcasted_iota(jnp.int32, (r, r), 1) + (first + b) * r
        pieces.append(jnp.where((qdoc == kdoc) & (cols <= rows), 0.0, MASKED))
    return jnp.concatenate(pieces, axis=1)


def attend_kernel(hc, kvc, ctx, q_ref, k_ref, v_ref, qdoc_ref, kdoc_ref, out_ref, lse_ref):
    s = pl.program_id(1)
    r = q_ref.shape[2]
    first, blocks = window_of(s, r, ctx)
    bias = bias_of(s, first, blocks, r, qdoc_ref, kdoc_ref)
    lane = lax.broadcasted_iota(jnp.int32, (r, LANES), 1)
    lse_all = jnp.zeros((r, LANES), F32)
    outs = []
    for h in range(hc):
        g = h * kvc // hc
        q = q_ref[0, 0, :, h * LANES : (h + 1) * LANES]
        k = k_ref[pl.ds(first, blocks), 0, :, g * LANES : (g + 1) * LANES].reshape(blocks * r, LANES)
        v = v_ref[pl.ds(first, blocks), 0, :, g * LANES : (g + 1) * LANES].reshape(blocks * r, LANES)
        scores = dot_nt(q, k) * HD ** (-0.5) + bias
        top = jnp.max(scores, axis=-1, keepdims=True)
        e = jnp.exp(scores - top)
        total = jnp.sum(e, axis=-1, keepdims=True)
        probs = (e * (1.0 / total)).astype(BF)
        outs.append(dot_nn(probs, v)[:, :HD])
        lse_all = jnp.where(lane == h, top + jnp.log(total), lse_all)
    out_ref[0, 0] = jnp.concatenate(outs, axis=1).astype(BF)
    lse_ref[0, 0] = lse_all


def attend_call(z, q, k, v, qdoc, kdoc, hc, kvc, script, moved, new, filled):
    ctx, m, r, _ = q.shape
    row = lambda b, s: (s, b, 0, 0)
    seq = lambda b, s: (0, b, 0, 0)
    return fused_call(
        z,
        "attend",
        12,
        functools.partial(attend_kernel, hc, kvc, ctx),
        (m, ctx),
        [
            pl.BlockSpec((1, 1, r, hc * LANES), row),
            pl.BlockSpec((ctx, 1, r, kvc * LANES), seq),
            pl.BlockSpec((ctx, 1, r, kvc * LANES), seq),
            pl.BlockSpec((1, 1, r, 1), row),
            pl.BlockSpec((ctx, 1, 1, r), seq),
        ],
        [pl.BlockSpec((1, 1, r, hc * HD), row), pl.BlockSpec((1, 1, r, LANES), row)],
        [sds((ctx, m, r, hc * HD)), sds((ctx, m, r, LANES), F32)],
        (q, k, v, qdoc, kdoc),
        script,
        moved,
        new,
        filled,
    )


def attend_back_kernel(
    hc, kvc, ctx, q_ref, k_ref, v_ref, qdoc_ref, kdoc_ref, o_ref, do_ref, lse_ref, cos_ref, sin_ref,
    dq_ref, dkv_ref, dk_acc, dv_acc,
):
    s = pl.program_id(1)
    r = q_ref.shape[2]
    first, blocks = window_of(s, r, ctx)
    bias = bias_of(s, first, blocks, r, qdoc_ref, kdoc_ref)

    @pl.when(s == 0)
    def _():
        dk_acc[...] = jnp.zeros_like(dk_acc)
        dv_acc[...] = jnp.zeros_like(dv_acc)

    cos, sin = cos_ref[s], sin_ref[s]
    lse_all = lse_ref[0, 0]
    for h in range(hc):
        g = h * kvc // hc
        q = q_ref[0, 0, :, h * LANES : (h + 1) * LANES]
        k = k_ref[pl.ds(first, blocks), 0, :, g * LANES : (g + 1) * LANES].reshape(blocks * r, LANES)
        v = v_ref[pl.ds(first, blocks), 0, :, g * LANES : (g + 1) * LANES].reshape(blocks * r, LANES)
        o = o_ref[0, 0, :, h * HD : (h + 1) * HD].astype(F32)
        do = do_ref[0, 0, :, h * HD : (h + 1) * HD]
        delta = jnp.sum(o * do.astype(F32), axis=-1, keepdims=True)
        do = jnp.concatenate([do, jnp.zeros((r, LANES - HD), BF)], axis=1)
        scores = dot_nt(q, k) * HD ** (-0.5) + bias
        probs = jnp.exp(scores - lse_all[:, h : h + 1])
        d_probs = dot_nt(do, v)
        d_scores = (probs * (d_probs - delta) * HD ** (-0.5)).astype(BF)
        dq = dot_nn(d_scores, k)
        dq_ref[0, 0, :, h * LANES : (h + 1) * LANES] = rotated(dq, cos, -sin).astype(BF)
        dk = dot_tn(d_scores, q).reshape(blocks, r, LANES)
        dv = dot_tn(probs.astype(BF), do).reshape(blocks, r, LANES)
        here = slice(g * LANES, (g + 1) * LANES)
        dk_acc[pl.ds(first, blocks), :, here] += dk
        dv_acc[pl.ds(first, blocks), :, here] += dv

    @pl.when(s == ctx - 1)
    def _():
        for b in range(ctx):
            for g in range(kvc):
                here = slice(g * LANES, (g + 1) * LANES)
                at = g * LANES
                dk = rotated(dk_acc[b, :, here], cos_ref[b], -sin_ref[b])
                dkv_ref[b, 0, :, at : at + LANES] = dk.astype(BF)
                at += kvc * LANES
                dkv_ref[b, 0, :, at : at + LANES] = dv_acc[b, :, here].astype(BF)


def attend_back_call(z, q, k, v, qdoc, kdoc, o, do, lse, cos, sin, hc, kvc, script, moved, new, filled):
    ctx, m, r, _ = q.shape
    row = lambda b, s: (s, b, 0, 0)
    seq = lambda b, s: (0, b, 0, 0)
    table = pl.BlockSpec((ctx, r, LANES), lambda b, s: (0, 0, 0))
    return fused_call(
        z,
        "attend_back",
        14,
        functools.partial(attend_back_kernel, hc, kvc, ctx),
        (m, ctx),
        [
            pl.BlockSpec((1, 1, r, hc * LANES), row),
            pl.BlockSpec((ctx, 1, r, kvc * LANES), seq),
            pl.BlockSpec((ctx, 1, r, kvc * LANES), seq),
            pl.BlockSpec((1, 1, r, 1), row),
            pl.BlockSpec((ctx, 1, 1, r), seq),
            pl.BlockSpec((1, 1, r, hc * HD), row),
            pl.BlockSpec((1, 1, r, hc * HD), row),
            pl.BlockSpec((1, 1, r, LANES), row),
            table,
            table,
        ],
        [
            pl.BlockSpec((1, 1, r, hc * LANES), row),
            pl.BlockSpec((ctx, 1, r, 2 * kvc * LANES), seq),
        ],
        [sds((ctx, m, r, hc * LANES)), sds((ctx, m, r, 2 * kvc * LANES))],
        (q, k, v, qdoc, kdoc, o, do, lse, cos, sin),
        script,
        moved,
        new,
        filled,
        [pltpu.VMEM((ctx, r, kvc * LANES), F32), pltpu.VMEM((ctx, r, kvc * LANES), F32)],
    )


def mix_kernel(ctx, att_ref, x_ref, gain_ref, w_ref, mid_ref, normed_ref, rows_ref):
    rows = jnp.concatenate([att_ref[c, 0] for c in range(ctx)], axis=1)
    rows_ref[0] = rows
    mid = x_ref[0].astype(F32) + dot_nn(rows, w_ref[...])
    mid_ref[0] = mid
    scale = lax.rsqrt(jnp.mean(mid * mid, axis=-1, keepdims=True) + EPS)
    normed_ref[0] = (mid * scale * gain_ref[...]).astype(BF)


def mix_call(z, att, x, gain, w, script, moved, new, filled):
    ctx, m, r, cols = att.shape
    d = x.shape[-1]
    seq = pl.BlockSpec((1, r, d), lambda b: (b, 0, 0))
    whole = lambda b: (0, 0)
    return fused_call(
        z,
        "mix",
        16,
        functools.partial(mix_kernel, ctx),
        (m,),
        [
            pl.BlockSpec((ctx, 1, r, cols), lambda b: (0, b, 0, 0)),
            seq,
            pl.BlockSpec((1, d), whole),
            pl.BlockSpec(w.shape, whole, pipeline_mode=pl.Buffered(1)),
        ],
        [seq, seq, seq],
        [sds((m, r, d), F32), sds((m, r, d)), sds((m, r, d))],
        (att, x, gain, w),
        script,
        moved,
        new,
        filled,
    )


def turn_kernel(z, dn_ref, *refs):
    came_refs = refs[: z.ys - 1]
    mid_ref, cot_ref, gain_ref, w_ref = refs[z.ys - 1 : z.ys + 3]
    d_mid_ref, low_ref, all_ref, hold, send_sems, recv_sems, own_sems = refs[z.ys + 3 :]
    b, last = pl.program_id(0), pl.num_programs(0) - 1
    link = Link(z, send_sems, recv_sems, own_sems)
    cols = hold.shape[-1]

    def copies(n):
        remote = [
            pltpu.make_async_remote_copy(
                src_ref=hold.at[p, n],
                dst_ref=all_ref.at[link.c, n],
                send_sem=send_sems.at[n, j],
                recv_sem=recv_sems.at[n, j],
                device_id=(link.d, p),
                device_id_type=MESH,
            )
            for j, p in enumerate(link.ctx_peers())
        ]
        return remote, pltpu.make_async_copy(hold.at[link.c, n], all_ref.at[link.c, n], own_sems.at[n])

    d_normed = dn_ref[link.y, 0].astype(F32)
    for ref in came_refs:
        d_normed += ref[0].astype(F32)
    mid = mid_ref[0]
    scale = lax.rsqrt(jnp.mean(mid * mid, axis=-1, keepdims=True) + EPS)
    e = d_normed * gain_ref[...]
    d_mid = cot_ref[0].astype(F32) + (
        scale * e - mid * (scale * scale * scale) * jnp.mean(e * mid, axis=-1, keepdims=True)
    )
    d_mid_ref[0] = d_mid
    low = d_mid.astype(BF)
    low_ref[0] = low
    d_att = dot_nt(low, w_ref[...]).astype(BF)
    for c in range(z.ctx):
        hold[c, b] = d_att[:, c * cols : (c + 1) * cols]
    remote, own = copies(b)
    for copy in remote:
        copy.start()
    own.start()

    @pl.when(b == last)
    def _():
        for n in range(hold.shape[1]):
            remote, own = copies(n)
            for copy in remote:
                copy.wait_recv()
            for copy in remote:
                copy.wait_send()
            own.wait()


def turn_call(z, dn, came, mid, cot, gain, w, cols, script, moved, new, filled):
    ys, m, r, d = dn.shape
    seq = pl.BlockSpec((1, r, d), lambda b: (b, 0, 0))
    whole = lambda b: (0, 0)
    return fused_call(
        z,
        "turn",
        6,
        functools.partial(turn_kernel, z),
        (m,),
        [pl.BlockSpec((ys, 1, r, d), lambda b: (0, b, 0, 0))]
        + [seq] * (ys + 1)
        + [pl.BlockSpec((1, d), whole), pl.BlockSpec(w.shape, whole, pipeline_mode=pl.Buffered(1))],
        [seq, seq, pl.BlockSpec(memory_space=pltpu.HBM)],
        [sds((m, r, d), F32), sds((m, r, d)), sds((z.ctx, m, r, cols))],
        (dn, *came, mid, cot, gain, w),
        script,
        moved,
        new,
        filled,
        [
            pltpu.VMEM((z.ctx, m, r, cols), BF),
            pltpu.SemaphoreType.DMA((m, z.ctx)),
            pltpu.SemaphoreType.DMA((m, z.ctx)),
            pltpu.SemaphoreType.DMA((m,)),
        ],
    )


def mlp_kernel(
    z, x_ref, cot_ref, gate_ref, up_ref, down_ref,
    hid_ref, dg_ref, du_ref, dn_ref, out_ref,
    dn_send, dn_got, out_send, out_got, send_sems, recv_sems,
):
    other, y, b = pl.program_id(0) == 0, pl.program_id(1), pl.program_id(2)
    link = Link(z, send_sems, recv_sems, None)
    at = y * pl.num_programs(2) + b

    def copies(n):
        return [
            pltpu.make_async_remote_copy(
                src_ref=src.at[n],
                dst_ref=dst.at[n],
                send_sem=send_sems.at[which, n],
                recv_sem=recv_sems.at[which, n],
                device_id=link.ctx_dev(link.y, 1 - link.k),
                device_id_type=MESH,
            )
            for which, (src, dst) in enumerate(((dn_send, dn_got), (out_send, out_got)))
        ]

    @pl.when(other & (at == 0))
    def _():
        link.barrier(core_only=True)

    x, cot = x_ref[0, 0], cot_ref[0, 0]
    gate, up = dot_nn(x, gate_ref[...]), dot_nn(x, up_ref[...])
    d_hidden = dot_nt(cot, down_ref[...])
    sg = jax.nn.sigmoid(gate)
    act = gate * sg
    hidden = (act * up).astype(BF)
    hid_ref[0, 0] = hidden
    d_gate = (d_hidden * up * sg * (1.0 + gate * (1.0 - sg))).astype(BF)
    d_up = (d_hidden * act).astype(BF)
    dg_ref[0, 0] = d_gate
    du_ref[0, 0] = d_up
    out = dot_nn(hidden, down_ref[...])
    dn = dot_nt(d_gate, gate_ref[...]) + dot_nt(d_up, up_ref[...])

    @pl.when(other)
    def _():
        dn_send[at] = dn.astype(BF)
        out_send[at] = out.astype(BF)
        for copy in copies(at):
            copy.start()

    @pl.when(jnp.logical_not(other))
    def _():
        for copy in copies(at):
            copy.wait_recv()
        dn_ref[0, 0] = (dn + dn_got[at].astype(F32)).astype(BF)
        out_ref[0, 0] = (out + out_got[at].astype(F32)).astype(BF)
        for copy in copies(at):
            copy.wait_send()


def mlp_call(z, x, cot, gate, up, down):
    ctx, m, r, d = x.shape
    f = down.shape[0]
    row = lambda a, y, b: (a * z.ys + y, b, 0, 0)
    whole = lambda a, y, b: (0, 0)
    mine = lambda a, y, b: (a * y, a * b, 0, 0)
    block = lambda width, at: pl.BlockSpec((1, 1, r, width), at)
    resident = lambda w: pl.BlockSpec(w.shape, whole, pipeline_mode=pl.Buffered(1))
    held = pltpu.VMEM((z.ys * m, r, d), BF)
    return pl.pallas_call(
        functools.partial(mlp_kernel, z),
        name="mlp",
        grid=(2, z.ys, m),
        in_specs=[block(d, row), block(d, row), resident(gate), resident(up), resident(down)],
        out_specs=[block(f, row), block(f, row), block(f, row), block(d, mine), block(d, mine)],
        scratch_shapes=[held] * 4
        + [pltpu.SemaphoreType.DMA((2, z.ys * m)), pltpu.SemaphoreType.DMA((2, z.ys * m))],
        out_shape=[sds((ctx, m, r, f))] * 3 + [sds((z.ys, m, r, d))] * 2,
        compiler_params=pltpu.CompilerParams(
            collective_id=13, has_side_effects=True, vmem_limit_bytes=VMEM_LIMIT
        ),
    )(x, cot, gate, up, down)


def tail_kernel(
    z, da_ref, q_ref, kv_ref, po_ref, up_ref, gate_ref,
    da_out, q_out, kv_out, po_out, gate_out, up_out,
    da_mine, da_got, da_send, da_came, q_x, q_col, q_z, kv_x, kv_col, kv_z, po_x, po_col, po_z,
    up_mine, up_z, mine_q, mine_kv, mine_up, send_sems, recv_sems, local_sems,
):
    link = Link(z, send_sems, recv_sems, local_sems)
    link.landed = []
    link.barrier()
    peer = link.ctx_dev(link.y, 1 - link.k)
    far = list(range(1, z.outer))
    order = [j for j in far if j in (1, z.outer - 1)] + [j for j in far if j not in (1, z.outer - 1)]
    wide = lambda a: a.astype(F32)

    core = link.put(da_ref.at[:, 1 - link.k], da_got, peer)
    scatter = lambda src, dst: [
        link.put(src.at[:, link.inner_to(j)], dst.at[j - 1], link.dp_dev(link.o, link.inner_to(j)))
        for j in range(1, z.inner)
    ]
    x_ways = [(q_ref, q_x, q_col, q_z, scatter(q_ref, q_x)), (kv_ref, kv_x, kv_col, kv_z, scatter(kv_ref, kv_x))]
    po_way = (po_ref, po_x, po_col, po_z, scatter(po_ref, po_x))
    up_ways = []
    near = [j for j in order if j in (1, z.outer - 1)]
    rest = [j for j in order if j not in near]

    def outer_put(src, dst, j):
        to = link.outer_to(j)
        return link.put(src.at[to], dst.at[j - 1], link.dp_dev(to, link.i))

    up_ways += [outer_put(up_ref, up_z, j) for j in near]
    load = link.keep(da_ref.at[:, link.k], da_mine)
    load_up = link.keep(up_ref.at[link.o], up_mine)
    link.keep(gate_ref.at[link.c], gate_out.at[link.c])
    exchange_ctx(link, gate_ref, lambda s: gate_out.at[s])

    link.arrived(core)
    load.wait()
    load_up.wait()
    link.local = [copy for copy in link.local if copy is not load and copy is not load_up]
    rows = 32 if da_mine.shape[2] % 32 == 0 else da_mine.shape[2]
    count = da_mine.shape[2] // rows
    seqs = da_mine.shape[1]

    def add_core(step, _):
        b, at = lax.div(step, count), pl.ds(pl.multiple_of(lax.rem(step, count) * rows, rows), rows)
        for j in range(z.ys):
            y = lax.rem(link.y + j, z.ys)
            total = wide(da_mine[y, b, at]) + wide(da_got[y, b, at])
            if j == 0:
                da_out[b, at] = total
            else:
                da_send[j - 1, b, at] = total.astype(BF)
        return 0

    lax.fori_loop(0, seqs * count, add_core, 0)
    y_ways = []
    for j in range(1, z.ys):
        to = lax.rem(link.y + j, z.ys)
        y_ways.append(link.put(da_send.at[j - 1], da_came.at[j - 1], link.ctx_dev(to, link.k)))

    def columns(way):
        part, came, col, got, copies = way
        for copy in copies:
            link.arrived(copy)
        for o in range(z.outer):
            total = wide(part[o, link.i])
            for j in range(z.inner - 1):
                total += wide(came[j, o])
            col[o] = total.astype(BF)
        return [outer_put(col, got, j) for j in order]

    z_ways = [columns(way) for way in x_ways]
    z_ways.append(columns(po_way))
    up_ways += [outer_put(up_ref, up_z, j) for j in rest]

    def close(col, got, copies):
        for copy in copies:
            link.arrived(copy)
        total = wide(col)
        for j in range(z.outer - 1):
            total += wide(got[j])
        return total

    for way, copies, mine, out in zip(x_ways, z_ways, (mine_q, mine_kv), (q_out, kv_out)):
        mine[...] = close(way[2][link.o], way[3], copies).astype(BF)
        exchange_ctx(link, mine, lambda s: out.at[s])
        link.keep(mine.at[link.c], out.at[link.c])
    for copy in y_ways:
        link.arrived(copy)

    def add_y(step, _):
        b, at = lax.div(step, count), pl.ds(pl.multiple_of(lax.rem(step, count) * rows, rows), rows)
        total = da_out[b, at]
        for j in range(z.ys - 1):
            total += wide(da_came[j, b, at])
        da_out[b, at] = total
        return 0

    lax.fori_loop(0, seqs * count, add_y, 0)
    po_out[...] = close(po_col[link.o], po_z, z_ways[2])
    mine_up[...] = close(up_mine[...], up_z, up_ways).astype(BF)
    exchange_ctx(link, mine_up, lambda s: up_out.at[s])
    link.keep(mine_up.at[link.c], up_out.at[link.c])
    link.finish()


def tail_call(z, da, part_q, part_kv, po, up_col, gate_mine):
    ys, _, m, r, d = da.shape
    one = lambda a: a.shape[2:]
    grown = lambda n, a: (n,) + tuple(a)
    q1, kv1, po1, up1 = one(part_q), one(part_kv), one(po), up_col.shape[1:]
    vm = lambda shape: pltpu.VMEM(tuple(shape), BF)
    hbm, vmem = pl.BlockSpec(memory_space=pltpu.HBM), pl.BlockSpec(memory_space=pltpu.VMEM)
    scratch = [vm((ys, m, r, d)), vm((ys, m, r, d)), vm((ys - 1, m, r, d)), vm((ys - 1, m, r, d))]
    for shape in (q1, kv1, po1):
        scratch += [vm((z.inner - 1, z.outer) + shape), vm((z.outer,) + shape), vm((z.outer - 1,) + shape)]
    scratch += [vm(up1), vm((z.outer - 1,) + up1), vm(q1), vm(kv1), vm(up1)]
    scratch += [
        pltpu.SemaphoreType.DMA((64,)),
        pltpu.SemaphoreType.DMA((64,)),
        pltpu.SemaphoreType.DMA((16,)),
    ]

    def body(da, q, kv, po, up, gate, *rest):
        tail_kernel(z, da, q, kv, po, up, gate, *rest)

    return pl.pallas_call(
        body,
        name="tail",
        in_specs=[hbm, vmem, vmem, vmem, hbm, hbm],
        out_specs=[vmem, hbm, hbm, vmem, hbm, hbm],
        out_shape=[sds((m, r, d), F32), sds(q1), sds(kv1), sds(po1, F32), sds(gate_mine.shape), sds(up1)],
        scratch_shapes=scratch,
        compiler_params=pltpu.CompilerParams(
            collective_id=15, has_side_effects=True, vmem_limit_bytes=VMEM_LIMIT
        ),
    )(da, part_q, part_kv, po, up_col, gate_mine)


def pad_heads(w, heads, split):
    rows = w.shape[0]
    if split:
        w = jnp.pad(w.reshape(rows, heads, 2, HALF), ((0, 0), (0, 0), (0, 0), (0, LANES // 2 - HALF)))
    else:
        w = jnp.pad(w.reshape(rows, heads, HD), ((0, 0), (0, 0), (0, LANES - HD)))
    return w.reshape(rows, heads * LANES)


def unpad_heads(w, heads, split):
    if split:
        w = w.reshape(w.shape[:-1] + (heads, 2, LANES // 2))[..., :HALF]
    else:
        w = w.reshape(w.shape[:-1] + (heads, LANES))[..., :HD]
    return w.reshape(w.shape[: w.ndim - (3 if split else 2)] + (heads * HD,))


def rope_tables(ctx, r):
    frequency = THETA ** (-(jnp.arange(HALF, dtype=F32) * (2.0 / HD)))
    angles = jnp.arange(ctx * r, dtype=jnp.int32).astype(F32)[:, None] * frequency[None, :]
    pad = ((0, 0), (0, LANES // 2 - HALF))
    cos, sin = jnp.pad(jnp.cos(angles), pad), jnp.pad(jnp.sin(angles), pad)
    cos = jnp.concatenate([cos, cos], axis=1).reshape(ctx, r, LANES)
    sin = jnp.concatenate([-sin, sin], axis=1).reshape(ctx, r, LANES)
    return cos, sin


def per_device(
    inputs, segments, cotangent, w_query, w_key, w_value, w_out, w_gate, w_up, w_down, gain_attn, gain_ffn
):
    z = Sizes(lax.axis_size("dp"), lax.axis_size("ctx"))
    dp, ctx, outer, inner, ys = z.dp, z.ctx, z.outer, z.inner, z.ys
    m, r, d = inputs.shape
    rows = w_query.shape[0]
    frows, ff = w_down.shape[0], w_gate.shape[1]
    f = ff // ctx
    hc, kvc = H // ctx, KV // ctx
    width = (hc + 2 * kvc) * LANES
    c = lax.axis_index("ctx")
    di = lax.axis_index("dp")
    oi, ii = di // inner, di % inner
    yi, ki = c // 2, c % 2
    dyn = lambda a, at, axis: lax.dynamic_index_in_dim(a, at, axis, keepdims=False)

    pack_qkv = jnp.concatenate(
        [
            pad_heads(w_query, H, True).reshape(rows, ctx, hc * LANES),
            pad_heads(w_key, KV, True).reshape(rows, ctx, kvc * LANES),
            pad_heads(w_value, KV, False).reshape(rows, ctx, kvc * LANES),
        ],
        axis=2,
    ).transpose(1, 0, 2)
    by_rank = lambda w: w.reshape(rows, dp, ctx, frows).transpose(2, 0, 1, 3).reshape(ctx, rows, f)
    pack_gate, pack_up = by_rank(w_gate), by_rank(w_up)
    gains = jnp.stack([gain_attn, gain_ffn]).astype(F32)
    gains = jnp.pad(gains, ((0, 6), (0, LANES - rows)))

    steps = list(range(1, outer))
    by_owner = lambda buf: lambda s: buf.at[s]
    out_slot = lambda link, buf: lambda s: buf.at[s, :, link.k]

    def first_script(link, ins, outs, scratch):
        x, seg, qkv, gain, wo, pg, pu, wd = ins
        x_all, seg_all, g_qkv, g_gain, g_out, g_gate, g_up, g_down = outs
        (hold,) = scratch
        load = pltpu.make_async_copy(x, hold, link.sems[2].at[15])
        load.start()
        mine = [
            link.keep(qkv.at[link.c], g_qkv.at[link.d, link.c]),
            link.keep(gain, g_gain.at[link.d, link.c]),
            link.keep(wo, g_out.at[link.d, link.y, link.k]),
            link.keep(seg, seg_all.at[link.c]),
        ]
        a2a = exchange_ctx(link, qkv, lambda s: g_qkv.at[link.d, s])
        a2a += [link.put(gain, g_gain.at[link.d, link.c], (link.d, p)) for p in link.ctx_peers()]
        for p in link.ctx_peers():
            link.put(seg, seg_all.at[link.c], (link.d, p))
        over_y = [
            link.put(wo, g_out.at[link.d, link.y, link.k], link.ctx_dev(p, link.k)) for p in link.y_peers()
        ]
        ways_x = gather_ctx_start(link, x, x_all)
        exchange_ctx(link, pg, lambda s: g_gate.at[link.d, s])
        for copy in a2a:
            link.arrived(copy)
        for copy in mine:
            copy.wait()
        link.local = []
        small = [by_owner(g_qkv), by_owner(g_gain)]
        ways = [ring_outer(link, slot, 1) for slot in small]
        for slot in small:
            pass_inner(link, slot, 0)
        link.keep(pg.at[link.c], g_gate.at[link.d, link.c])
        link.keep(pu.at[link.c], g_up.at[link.d, link.c])
        link.keep(wd, g_down.at[link.d])
        load.wait()
        store = pltpu.make_async_copy(hold, x_all.at[link.c], link.sems[2].at[14])
        store.start()
        for step in steps:
            came, ways = ways, []
            for copy, slot in zip(came, small):
                link.arrived(copy)
                if step < steps[-1]:
                    ways.append(ring_outer(link, slot, step + 1))
                pass_inner(link, slot, step)
        for copy in over_y:
            link.arrived(copy)
        ring_outer(link, out_slot(link, g_out), 1)
        pass_inner(link, out_slot(link, g_out), 0)
        gather_ctx_forward(link, x_all, ways_x)
        store.wait()

    x_all, seg_all, g_qkv, g_gain, g_out, g_gate, g_up, g_down = communicate(
        z,
        "gather_first",
        1,
        first_script,
        (inputs, segments, pack_qkv, gains, w_out, pack_gate, pack_up, w_down),
        (
            sds((ctx, m, r, d)),
            sds((ctx, m, r), jnp.int32),
            sds((dp, ctx, rows, width)),
            sds((dp, ctx, 8, LANES), F32),
            sds((dp, ys, 2, rows, d)),
            sds((dp, ctx, rows, f)),
            sds((dp, ctx, rows, f)),
            sds((dp, frows, d)),
        ),
        [pltpu.VMEM((m, r, d), BF)],
    )
    gain_a = g_gain[:, :, 0, :rows].reshape(1, d)
    gain_f = g_gain[:, :, 1, :rows].reshape(1, d)
    wqkv = g_qkv.reshape(d, width)
    cos, sin = rope_tables(ctx, r)
    qdoc = seg_all.reshape(ctx, m, r, 1)
    kdoc = seg_all.reshape(ctx, m, 1, r)
    early, late = range(m // 2), range(m // 2, m)

    def qkv_cargo(cargo, moved, bufs):
        (cot, pu), (g_out, g_gate, g_up, cot_all) = moved, bufs
        exchange_ctx(cargo, pu, lambda s: g_up.at[cargo.d, s])
        own_y(cargo, cot, cot_all, early)
        for slot, step in ((out_slot(cargo, g_out), 2), (by_owner(g_gate), 1)):
            ring_outer(cargo, slot, step)
            pass_inner(cargo, slot, step - 1)

    g_out, g_gate, g_up, cot_all, normed_a, q, k, v = qkv_call(
        z, x_all, gain_a, wqkv, cos, sin, hc, kvc,
        qkv_cargo, (cotangent, pack_up), (sds((ctx, m, r, d)),), (g_out, g_gate, g_up),
    )

    def attend_cargo(cargo, moved, bufs):
        (cot,), (g_out, g_gate, g_up, cot_all) = moved, bufs
        own_y(cargo, cot, cot_all, late)
        pass_core(cargo, cot_all, early)
        for slot, step in ((out_slot(cargo, g_out), 3), (by_owner(g_gate), 2), (by_owner(g_up), 1)):
            ring_outer(cargo, slot, step)
            pass_inner(cargo, slot, step - 1)

    g_out, g_gate, g_up, cot_all, att, lse = attend_call(
        z, q, k, v, qdoc, kdoc, hc, kvc, attend_cargo, (cotangent,), (), (g_out, g_gate, g_up, cot_all)
    )

    def second_script(link, ins, outs, scratch):
        att, cot = ins[:2]
        g_out, g_gate, g_up, cot_all, att_all = outs
        (hold,) = scratch
        load = pltpu.make_async_copy(cot, hold, link.sems[2].at[15])
        load.start()
        link.keep(att.at[link.c], att_all.at[link.c])
        first = len(link.inflight)
        pass_inner(link, out_slot(link, g_out), 3)
        last_out = link.inflight[first:]
        exchange_ctx(link, att, lambda s: att_all.at[s])
        for slot, step in ((by_owner(g_gate), 3), (by_owner(g_up), 2)):
            ring_outer(link, slot, step)
        pass_inner(link, by_owner(g_gate), 2)
        pass_core(link, cot_all, late)
        load.wait()
        store = pltpu.make_async_copy(hold, cot_all.at[link.slot(link.y, True)], link.sems[2].at[14])
        store.start()
        for copy in last_out:
            link.arrived(copy)
        both = g_out.at[:, :, link.k]
        link.put(both, both, link.ctx_dev(link.y, 1 - link.k))
        store.wait()

    g_out, g_gate, g_up, cot_all, att_all = communicate(
        z,
        "exchange_heads",
        2,
        second_script,
        (att, cotangent),
        (sds(att.shape),),
        [pltpu.VMEM((m, r, d), BF)],
        (g_out, g_gate, g_up, cot_all),
    )
    wo = g_out.reshape(d, d)

    def mix_cargo(cargo, moved, bufs):
        g_gate, g_up, g_down = bufs
        ring_outer(cargo, by_owner(g_up), 3)
        ring_outer(cargo, by_owner(g_down), 1)
        pass_inner(cargo, by_owner(g_gate), 3)
        pass_inner(cargo, by_owner(g_up), 1)

    g_gate, g_up, g_down, mid, normed, att_rows = mix_call(
        z, att_all, inputs, gain_f, wo, mix_cargo, (), (), (g_gate, g_up, g_down)
    )
    att_rows = att_rows.reshape(m * r, H * HD)
    residual = inputs.astype(F32)

    def third_script(link, ins, outs, scratch):
        x, (g_up, g_down, x_all), (hold,) = ins[0], outs, scratch
        load = pltpu.make_async_copy(x, hold, link.sems[2].at[15])
        load.start()
        ways = gather_ctx_start(link, x, x_all, True)
        way = ring_outer(link, by_owner(g_down), 2)
        pass_inner(link, by_owner(g_down), 1)
        pass_inner(link, by_owner(g_up), 2)
        load.wait()
        store = pltpu.make_async_copy(hold, x_all.at[link.slot(link.y, True)], link.sems[2].at[14])
        store.start()
        link.arrived(way)
        way = ring_outer(link, by_owner(g_down), 3)
        pass_inner(link, by_owner(g_down), 0)
        pass_inner(link, by_owner(g_up), 3)
        pass_inner(link, by_owner(g_down), 2)
        link.arrived(way)
        pass_inner(link, by_owner(g_down), 3)
        gather_ctx_forward(link, x_all, ways, True)
        store.wait()

    g_up, g_down, normed_all = communicate(
        z,
        "gather_third",
        3,
        third_script,
        (normed,),
        (sds((ctx, m, r, d)),),
        [pltpu.VMEM((m, r, d), BF)],
        (g_up, g_down),
    )
    w_gate_c, w_up_c, w_down_c = g_gate.reshape(d, f), g_up.reshape(d, f), g_down.reshape(f, d)

    hidden, d_gate, d_up, dn_pair, out_pair = mlp_call(z, normed_all, cot_all, w_gate_c, w_up_c, w_down_c)

    dp_perm = lambda fn: [(o * inner + i, fn(o, i)) for o in range(outer) for i in range(inner)]
    ctx_perm = lambda fn: [(y * 2 + k, fn(y, k)) for y in range(ys) for k in range(2)]
    wide = lambda a: a.astype(F32)
    flat = lambda a: a.reshape(ctx * m * r, a.shape[-1])

    def after(a, dep):
        return lax.optimization_barrier((a, dep))[0]

    def to_core(a):
        return lax.ppermute(a, "ctx", ctx_perm(lambda y, k: y * 2 + 1 - k))

    def to_y(pair):
        return [
            lax.ppermute(
                dyn(pair, (yi + j) % ys, 0), "ctx", ctx_perm(lambda y, k: (y + j) % ys * 2 + k)
            )
            for j in range(1, ys)
        ]

    def to_inner(part):
        return [
            lax.ppermute(
                dyn(part, (ii + j) % inner, 1), "dp", dp_perm(lambda o, i: o * inner + (i + j) % inner)
            )
            for j in range(1, inner)
        ]

    column = lambda part, came: (wide(dyn(part, ii, 1)) + sum(wide(a) for a in came)).astype(BF)
    close = lambda own, came: wide(own) + sum(wide(a) for a in came)

    dn_came = to_y(dn_pair)
    part_down = dot_tn(flat(hidden), flat(cot_all)).astype(BF).reshape(outer, inner, frows, d)
    down_x = to_inner(part_down)
    shape_g = (outer, inner, ctx, rows, f)
    part_gate = dot_tn(flat(normed_all), flat(d_gate)).astype(BF).reshape(shape_g)
    gate_x = to_inner(part_gate)
    part_up = dot_tn(flat(normed_all), flat(after(d_up, part_gate))).astype(BF).reshape(shape_g)
    near = [j for j in steps if j in (1, outer - 1)]
    mid_way = [j for j in steps if j not in near]
    down_col = column(part_down, after(down_x, part_up))

    def turn_cargo(cargo, moved, bufs):
        scatter_outer(cargo, moved[0], bufs[0], near)

    down_z, d_mid, d_mid_low, d_att_all = turn_call(
        z, dn_pair, dn_came, mid, cotangent, gain_f, wo, hc * HD,
        turn_cargo, (down_col,), (sds((outer - 1, frows, d)),), (),
    )

    part_out = dot_tn(att_rows, d_mid_low.reshape(m * r, d)).astype(BF).reshape(dp, ys, 2, rows, d)
    gate_col = column(part_gate, after(gate_x, d_att_all))

    def back_cargo(cargo, moved, bufs):
        (down_col, gate_col, part_up, part_out), (down_z, gate_z, up_x, po_in) = moved, bufs
        scatter_inner(cargo, part_up, up_x)
        scatter_outer(cargo, down_col, down_z, mid_way)
        scatter_outer(cargo, gate_col, gate_z, near)
        cargo.put(part_out.at[:, :, 1 - cargo.k], po_in, cargo.ctx_dev(cargo.y, 1 - cargo.k))

    down_z, gate_z, up_x, po_in, dq, dkv = attend_back_call(
        z, q, k, v, qdoc, kdoc, att, d_att_all, lse, cos, sin, hc, kvc,
        back_cargo,
        (down_col, gate_col, part_up, part_out),
        (
            sds((outer - 1,) + gate_col.shape[1:]),
            sds((inner - 1, outer) + gate_col.shape[1:]),
            sds((dp, ys, rows, d)),
        ),
        (down_z,),
    )
    po_both = lambda at: wide(dyn(dyn(part_out, ki, 2), at, 1)) + wide(dyn(po_in, at, 1))
    po_came = [
        lax.ppermute(
            po_both((yi + j) % ys).astype(BF), "ctx", ctx_perm(lambda y, k: (y + j) % ys * 2 + k)
        )
        for j in range(1, ys)
    ]
    gate_far = [
        lax.ppermute(
            dyn(after(gate_col, dq), (oi + j) % outer, 0), "dp", dp_perm(lambda o, i: (o + j) % outer * inner + i)
        )
        for j in mid_way
    ]
    out_came = to_y(after(out_pair, po_came))
    da = dot_nt(flat(dq), wqkv[:, : hc * LANES]) + dot_nt(flat(dkv), wqkv[:, hc * LANES :])
    da = da.astype(BF).reshape(ys, 2, m, r, d)
    part_q = dot_tn(flat(normed_a), flat(dq)).astype(BF).reshape(outer, inner, ctx, rows, hc * LANES)
    part_kv = dot_tn(flat(normed_a), flat(dkv)).astype(BF).reshape(outer, inner, ctx, rows, 2 * kvc * LANES)
    up_col = column(part_up, [up_x[j] for j in range(inner - 1)])
    po = close(po_both(yi), after(po_came, part_kv)).astype(BF).reshape(outer, inner, rows, d)
    gate_near = [gate_z[j - 1] for j in near]
    gate_mine = close(dyn(gate_col, oi, 0), gate_near + gate_far).astype(BF)

    d_normed_a, q_all, kv_all, grad_out, gate_all, up_all = tail_call(z, da, part_q, part_kv, po, up_col, gate_mine)
    grad_down = close(dyn(down_col, oi, 0), [down_z[j - 1] for j in steps])
    outputs = mid + close(dyn(out_pair, yi, 0), out_came)
    scale_a = lax.rsqrt(jnp.mean(residual * residual, axis=-1, keepdims=True) + EPS)
    e = d_normed_a * gain_a
    input_grad = d_mid + (
        scale_a * e - residual * (scale_a * scale_a * scale_a) * jnp.mean(e * residual, axis=-1, keepdims=True)
    )
    spread = lambda a: wide(a).reshape(ctx, rows, dp, frows).transpose(1, 2, 0, 3).reshape(rows, ff)
    grad_gate, grad_up = spread(gate_all), spread(up_all)
    cols = lambda a, heads, split: (
        unpad_heads(wide(a), heads, split).transpose(1, 0, 2).reshape(rows, ctx * heads * HD)
    )
    grad_query = cols(q_all, hc, True)
    grad_key = cols(kv_all[:, :, : kvc * LANES], kvc, True)
    grad_value = cols(kv_all[:, :, kvc * LANES :], kvc, False)

    along = lambda pairs, gain: sum(jnp.sum(wide(w) * g, axis=1) for w, g in pairs) / wide(gain)
    grad_gain_a = along(((w_query, grad_query), (w_key, grad_key), (w_value, grad_value)), gain_attn)
    grad_gain_f = along(((w_gate, grad_gate), (w_up, grad_up)), gain_ffn)
    return (
        outputs,
        input_grad,
        grad_query,
        grad_key,
        grad_value,
        grad_out,
        grad_gate,
        grad_up,
        grad_down,
        grad_gain_a,
        grad_gain_f,
    )


def solution(mesh):
    rows, vec, tok = P(("dp", "ctx"), None), P(("dp", "ctx")), P("dp", "ctx", None)
    return jax.shard_map(
        per_device,
        mesh=mesh,
        in_specs=(tok, P("dp", "ctx"), tok) + (rows,) * 7 + (vec, vec),
        out_specs=(tok, tok) + (rows,) * 7 + (vec, vec),
        check_vma=False,
    )
```

```python
import functools

import jax
import jax.numpy as jnp
from jax import lax
from jax.experimental import pallas as pl
from jax.experimental.pallas import tpu as pltpu
from jax.sharding import PartitionSpec as P

H = 16
KV = 8
HD = 96
HALF = HD // 2
LANES = 128
SPAN = 512

EPS = 1e-05
THETA = 100000.0
MASKED = -1e30

BF = jnp.bfloat16
F32 = jnp.float32
MESH = pl.DeviceIdType.MESH
VMEM_LIMIT = 60 * 1024 * 1024


def sds(shape, dtype=BF):
    return jax.ShapeDtypeStruct(tuple(shape), dtype)


def dot_nn(a, b):
    return lax.dot_general(a, b, (((1,), (0,)), ((), ())), preferred_element_type=F32)


def dot_nt(a, b):
    return lax.dot_general(a, b, (((1,), (1,)), ((), ())), preferred_element_type=F32)


def dot_tn(a, b):
    return lax.dot_general(a, b, (((0,), (0,)), ((), ())), preferred_element_type=F32)


class Sizes:
    def __init__(self, dp, ctx):
        self.dp, self.ctx = dp, ctx
        self.outer = 4 if dp % 4 == 0 else dp
        self.inner = dp // self.outer
        self.ys = ctx // 2


class Link:
    def __init__(self, z, send_sems, recv_sems, local_sems):
        self.z = z
        self.d = lax.axis_index("dp")
        self.c = lax.axis_index("ctx")
        self.o, self.i = lax.div(self.d, z.inner), lax.rem(self.d, z.inner)
        self.y, self.k = lax.div(self.c, 2), lax.rem(self.c, 2)
        self.sems = (send_sems, recv_sems, local_sems)
        self.sent, self.inflight, self.local = 0, [], []

    def ctx_dev(self, y, k):
        return (self.d, y * 2 + k)

    def slot(self, y, rel):
        return y + self.z.ys if rel else y * 2 + self.k

    def slot_across(self, y, rel):
        return y if rel else y * 2 + self.k

    def ctx_peers(self):
        n = self.z.ctx
        return [lax.rem(self.c + j, n) for j in range(1, n)]

    def y_peers(self):
        n = self.z.ys
        return [lax.rem(self.y + j, n) for j in range(1, n)]

    def outer_to(self, j):
        return lax.rem(self.o + j, self.z.outer)

    def outer_from(self, j):
        return lax.rem(self.o + self.z.outer - j, self.z.outer)

    def inner_to(self, j):
        return lax.rem(self.i + j, self.z.inner)

    def dp_dev(self, o, i):
        return (o * self.z.inner + i, self.c)

    def barrier(self, core_only=False):
        devices = [(self.d, c) for c in self.ctx_peers()]
        if core_only:
            devices = [self.ctx_dev(self.y, 1 - self.k)]
            self.signal_all(devices)
            return
        devices += [self.dp_dev(self.outer_to(j), self.i) for j in range(1, self.z.outer)]
        devices += [self.dp_dev(self.o, self.inner_to(j)) for j in range(1, self.z.inner)]
        self.signal_all(devices)

    def signal_all(self, devices):
        barrier = pltpu.get_barrier_semaphore()
        for device in devices:
            pl.semaphore_signal(barrier, inc=1, device_id=device, device_id_type=MESH)
        pl.semaphore_wait(barrier, len(devices))

    def put(self, src, dst, device):
        n = self.sent
        self.sent += 1
        copy = pltpu.make_async_remote_copy(
            src_ref=src,
            dst_ref=dst,
            send_sem=self.sems[0].at[n],
            recv_sem=self.sems[1].at[n],
            device_id=device,
            device_id_type=MESH,
        )
        copy.start()
        self.inflight.append(copy)
        return copy

    def keep(self, src, dst):
        copy = pltpu.make_async_copy(src, dst, self.sems[2].at[len(self.local)])
        copy.start()
        self.local.append(copy)
        return copy

    def arrived(self, copy):
        copy.wait_recv()
        self.inflight = [other for other in self.inflight if other is not copy]
        self.landed.append(copy)

    def finish(self):
        for copy in self.inflight:
            copy.wait_recv()
        for copy in self.landed + self.inflight:
            copy.wait_send()
        for copy in self.local:
            copy.wait()

    landed = None


def communicate(z, name, cid, script, ins, outs, scratch=(), filled=()):
    filled = tuple(filled)
    outs = [sds(a.shape, a.dtype) for a in filled] + list(outs)
    ins = tuple(ins) + filled
    n_in, n_out = len(ins), len(outs)
    aliases = {n_in - len(filled) + n: n for n in range(len(filled))}

    def kernel(*refs):
        in_refs, out_refs = refs[:n_in], refs[n_in : n_in + n_out]
        send, recv, local = refs[n_in + n_out : n_in + n_out + 3]
        link = Link(z, send, recv, local)
        link.landed = []
        link.barrier()
        script(link, in_refs, out_refs, refs[n_in + n_out + 3 :])
        link.finish()

    hbm = pl.BlockSpec(memory_space=pltpu.HBM)
    return pl.pallas_call(
        kernel,
        name=name,
        out_shape=list(outs),
        in_specs=[hbm] * n_in,
        out_specs=[hbm] * n_out,
        input_output_aliases=aliases,
        scratch_shapes=[
            pltpu.SemaphoreType.DMA((64,)),
            pltpu.SemaphoreType.DMA((64,)),
            pltpu.SemaphoreType.DMA((16,)),
        ]
        + list(scratch),
        compiler_params=pltpu.CompilerParams(
            collective_id=cid, has_side_effects=True, vmem_limit_bytes=VMEM_LIMIT
        ),
    )(*ins)


def gather_ctx_start(link, src, buf, rel=False):
    ways = []
    slot = buf.at[link.slot(link.y, rel)]
    for j in range(1, link.z.ys):
        to = lax.rem(link.y + j, link.z.ys)
        frm = lax.rem(link.y + link.z.ys - j, link.z.ys)
        ways.append((frm, link.put(src, slot, link.ctx_dev(to, link.k))))
    link.put(src, buf.at[link.slot_across(link.y, rel)], link.ctx_dev(link.y, 1 - link.k))
    return ways


def gather_ctx_forward(link, buf, ways, rel=False):
    for frm, copy in ways:
        link.arrived(copy)
        link.put(
            buf.at[link.slot(frm, rel)], buf.at[link.slot_across(frm, rel)], link.ctx_dev(link.y, 1 - link.k)
        )


def exchange_ctx(link, pack, slot_of):
    return [link.put(pack.at[c], slot_of(link.c), (link.d, c)) for c in link.ctx_peers()]


def gather_dp_start(link, slot_of):
    own = slot_of(link.d)
    ways = []
    for j in range(1, link.z.outer):
        copy = link.put(own, own, link.dp_dev(link.outer_to(j), link.i))
        ways.append((link.outer_from(j), copy))
    for j in range(1, link.z.inner):
        link.put(own, own, link.dp_dev(link.o, link.inner_to(j)))
    return ways


def gather_dp_forward(link, slot_of, ways):
    for frm, copy in ways:
        link.arrived(copy)
        slot = slot_of(frm * link.z.inner + link.i)
        for j in range(1, link.z.inner):
            link.put(slot, slot, link.dp_dev(link.o, link.inner_to(j)))


def scatter_inner(link, src, dst):
    for j in range(1, link.z.inner):
        to = link.inner_to(j)
        link.put(src.at[:, to], dst.at[j - 1], link.dp_dev(link.o, to))


def scatter_outer(link, src, dst, js):
    for j in js:
        to = link.outer_to(j)
        link.put(src.at[to], dst.at[j - 1], link.dp_dev(to, link.i))


def scatter_core(link, src, dst):
    link.put(src.at[:, 1 - link.k], dst, link.ctx_dev(link.y, 1 - link.k))


def scatter_y(link, src, dst):
    for j in range(1, link.z.ys):
        to = lax.rem(link.y + j, link.z.ys)
        link.put(src.at[to], dst.at[j - 1], link.ctx_dev(to, link.k))


class Cargo(Link):
    def put(self, src, dst, device):
        n = self.sent
        self.sent += 1
        copy = pltpu.make_async_remote_copy(
            src_ref=src,
            dst_ref=dst,
            send_sem=self.sems[0].at[n],
            recv_sem=self.sems[1].at[n],
            device_id=device,
            device_id_type=MESH,
        )
        self.inflight.append(copy)
        return copy


def fused_call(z, name, cid, body, grid, in_specs, out_specs, out_shape, args, script, moved, new=(), filled=(), scratch=()):
    filled, moved = tuple(filled), tuple(moved)
    n_arg, n_moved, n_fill = len(args), len(moved), len(filled)
    n_cargo = n_fill + len(new)
    n_out = n_cargo + len(out_shape)
    steps = 1
    for extent in grid:
        steps *= extent

    def kernel(*refs):
        step = 0
        for axis, extent in enumerate(grid):
            step = step * extent + pl.program_id(axis)
        n_in = n_arg + n_moved + n_fill
        arg_refs, moved_refs = refs[:n_arg], refs[n_arg : n_arg + n_moved]
        cargo_refs, out_refs = refs[n_in : n_in + n_cargo], refs[n_in + n_cargo : n_in + n_out]
        send, recv = refs[n_in + n_out : n_in + n_out + 2]
        cargo = Cargo(z, send, recv, None)
        script(cargo, moved_refs, cargo_refs)

        @pl.when(step == 0)
        def _():
            cargo.barrier()
            for copy in cargo.inflight:
                copy.start()

        body(*arg_refs, *out_refs, *refs[n_in + n_out + 2 :])

        @pl.when(step == steps - 1)
        def _():
            for copy in cargo.inflight:
                copy.wait_recv()
            for copy in cargo.inflight:
                copy.wait_send()

    hbm = pl.BlockSpec(memory_space=pltpu.HBM)
    first = n_arg + n_moved
    return pl.pallas_call(
        kernel,
        name=name,
        grid=grid,
        in_specs=list(in_specs) + [hbm] * (n_moved + n_fill),
        out_specs=[hbm] * n_cargo + list(out_specs),
        out_shape=[sds(a.shape, a.dtype) for a in filled] + list(new) + list(out_shape),
        input_output_aliases={first + n: n for n in range(n_fill)},
        scratch_shapes=[pltpu.SemaphoreType.DMA((32,)), pltpu.SemaphoreType.DMA((32,))] + list(scratch),
        compiler_params=pltpu.CompilerParams(
            collective_id=cid, has_side_effects=True, vmem_limit_bytes=VMEM_LIMIT
        ),
    )(*args, *moved, *filled)


def ring_outer(link, slot_of, step):
    slot = slot_of(link.outer_from(step - 1) * link.z.inner + link.i)
    return link.put(slot, slot, link.dp_dev(link.outer_to(1), link.i))


def ring_columns(link, buf, step):
    slot = buf.at[pl.ds(link.outer_from(step - 1) * link.z.inner, link.z.inner)]
    return link.put(slot, slot, link.dp_dev(link.outer_to(1), link.i))


def pass_inner(link, slot_of, step):
    slot = slot_of(link.outer_from(step) * link.z.inner + link.i)
    for j in range(1, link.z.inner):
        link.put(slot, slot, link.dp_dev(link.o, link.inner_to(j)))


def pass_core(link, buf, parts):
    for j in range(1, link.z.ys):
        at = lax.rem(link.y + link.z.ys - j, link.z.ys)
        for part in parts:
            src, dst = buf.at[link.slot(at, True), part], buf.at[link.slot_across(at, True), part]
            link.put(src, dst, link.ctx_dev(link.y, 1 - link.k))


def own_y(link, src, buf, parts):
    for part in parts:
        slot = buf.at[link.slot(link.y, True), part]
        for j in range(1, link.z.ys):
            to = lax.rem(link.y + j, link.z.ys)
            link.put(src.at[part], slot, link.ctx_dev(to, link.k))
        slot = buf.at[link.slot_across(link.y, True), part]
        link.put(src.at[part], slot, link.ctx_dev(link.y, 1 - link.k))


def rotated(u, cos, sin):
    return u * cos + pltpu.roll(u, LANES // 2, 1) * sin


def qkv_kernel(hc, kvc, x_ref, gain_ref, w_ref, cos_ref, sin_ref, n_ref, q_ref, k_ref, v_ref):
    x = x_ref[0, 0].astype(F32)
    scale = lax.rsqrt(jnp.mean(x * x, axis=-1, keepdims=True) + EPS)
    normed = (x * scale * gain_ref[...]).astype(BF)
    n_ref[0, 0] = normed
    full = dot_nn(normed, w_ref[...])
    cos, sin = cos_ref[0], sin_ref[0]
    for h in range(hc + kvc):
        piece = rotated(full[:, h * LANES : (h + 1) * LANES], cos, sin).astype(BF)
        if h < hc:
            q_ref[0, 0, :, h * LANES : (h + 1) * LANES] = piece
        else:
            k_ref[0, 0, :, (h - hc) * LANES : (h - hc + 1) * LANES] = piece
    v_ref[0, 0] = full[:, (hc + kvc) * LANES :].astype(BF)


def qkv_call(z, x_all, gain, w, cos, sin, hc, kvc, script, moved, new, filled):
    ctx, m, r, d = x_all.shape
    row = lambda s, b: (s, b, 0, 0)
    whole = lambda s, b: (0, 0)
    table = pl.BlockSpec((1, r, LANES), lambda s, b: (s, 0, 0))
    return fused_call(
        z,
        "qkv",
        11,
        functools.partial(qkv_kernel, hc, kvc),
        (ctx, m),
        [
            pl.BlockSpec((1, 1, r, d), row),
            pl.BlockSpec((1, d), whole),
            pl.BlockSpec(w.shape, whole, pipeline_mode=pl.Buffered(1)),
            table,
            table,
        ],
        [
            pl.BlockSpec((1, 1, r, d), row),
            pl.BlockSpec((1, 1, r, hc * LANES), row),
            pl.BlockSpec((1, 1, r, kvc * LANES), row),
            pl.BlockSpec((1, 1, r, kvc * LANES), row),
        ],
        [
            sds((ctx, m, r, d)),
            sds((ctx, m, r, hc * LANES)),
            sds((ctx, m, r, kvc * LANES)),
            sds((ctx, m, r, kvc * LANES)),
        ],
        (x_all, gain, w, cos, sin),
        script,
        moved,
        new,
        filled,
    )


def window_of(s, r, ctx):
    blocks = min(ctx, SPAN // r + 1)
    return jnp.maximum(s - (blocks - 1), 0), blocks


def bias_of(s, first, blocks, r, qdoc_ref, kdoc_ref):
    qdoc = qdoc_ref[0, 0]
    pieces = []
    for b in range(blocks):
        kdoc = kdoc_ref[first + b, 0]
        rows = lax.broadcasted_iota(jnp.int32, (r, r), 0) + s * r
        cols = lax.broadcasted_iota(jnp.int32, (r, r), 1) + (first + b) * r
        pieces.append(jnp.where((qdoc == kdoc) & (cols <= rows), 0.0, MASKED))
    return jnp.concatenate(pieces, axis=1)


def attend_kernel(hc, kvc, ctx, q_ref, k_ref, v_ref, qdoc_ref, kdoc_ref, out_ref, lse_ref):
    s = pl.program_id(1)
    r = q_ref.shape[2]
    first, blocks = window_of(s, r, ctx)
    bias = bias_of(s, first, blocks, r, qdoc_ref, kdoc_ref)
    lane = lax.broadcasted_iota(jnp.int32, (r, LANES), 1)
    lse_all = jnp.zeros((r, LANES), F32)
    outs = []
    for h in range(hc):
        g = h * kvc // hc
        q = q_ref[0, 0, :, h * LANES : (h + 1) * LANES]
        k = k_ref[pl.ds(first, blocks), 0, :, g * LANES : (g + 1) * LANES].reshape(blocks * r, LANES)
        v = v_ref[pl.ds(first, blocks), 0, :, g * LANES : (g + 1) * LANES].reshape(blocks * r, LANES)
        scores = dot_nt(q, k) * HD ** (-0.5) + bias
        top = jnp.max(scores, axis=-1, keepdims=True)
        e = jnp.exp(scores - top)
        total = jnp.sum(e, axis=-1, keepdims=True)
        probs = (e * (1.0 / total)).astype(BF)
        outs.append(dot_nn(probs, v)[:, :HD])
        lse_all = jnp.where(lane == h, top + jnp.log(total), lse_all)
    out_ref[0, 0] = jnp.concatenate(outs, axis=1).astype(BF)
    lse_ref[0, 0] = lse_all


def attend_call(z, q, k, v, qdoc, kdoc, hc, kvc, script, moved, new, filled):
    ctx, m, r, _ = q.shape
    row = lambda b, s: (s, b, 0, 0)
    seq = lambda b, s: (0, b, 0, 0)
    return fused_call(
        z,
        "attend",
        12,
        functools.partial(attend_kernel, hc, kvc, ctx),
        (m, ctx),
        [
            pl.BlockSpec((1, 1, r, hc * LANES), row),
            pl.BlockSpec((ctx, 1, r, kvc * LANES), seq),
            pl.BlockSpec((ctx, 1, r, kvc * LANES), seq),
            pl.BlockSpec((1, 1, r, 1), row),
            pl.BlockSpec((ctx, 1, 1, r), seq),
        ],
        [pl.BlockSpec((1, 1, r, hc * HD), row), pl.BlockSpec((1, 1, r, LANES), row)],
        [sds((ctx, m, r, hc * HD)), sds((ctx, m, r, LANES), F32)],
        (q, k, v, qdoc, kdoc),
        script,
        moved,
        new,
        filled,
    )


def attend_back_kernel(
    hc, kvc, ctx, q_ref, k_ref, v_ref, qdoc_ref, kdoc_ref, o_ref, do_ref, lse_ref, cos_ref, sin_ref,
    dq_ref, dkv_ref, dk_acc, dv_acc,
):
    s = pl.program_id(1)
    r = q_ref.shape[2]
    first, blocks = window_of(s, r, ctx)
    bias = bias_of(s, first, blocks, r, qdoc_ref, kdoc_ref)

    @pl.when(s == 0)
    def _():
        dk_acc[...] = jnp.zeros_like(dk_acc)
        dv_acc[...] = jnp.zeros_like(dv_acc)

    cos, sin = cos_ref[s], sin_ref[s]
    lse_all = lse_ref[0, 0]
    for h in range(hc):
        g = h * kvc // hc
        q = q_ref[0, 0, :, h * LANES : (h + 1) * LANES]
        k = k_ref[pl.ds(first, blocks), 0, :, g * LANES : (g + 1) * LANES].reshape(blocks * r, LANES)
        v = v_ref[pl.ds(first, blocks), 0, :, g * LANES : (g + 1) * LANES].reshape(blocks * r, LANES)
        o = o_ref[0, 0, :, h * HD : (h + 1) * HD].astype(F32)
        do = do_ref[0, 0, :, h * HD : (h + 1) * HD]
        delta = jnp.sum(o * do.astype(F32), axis=-1, keepdims=True)
        do = jnp.concatenate([do, jnp.zeros((r, LANES - HD), BF)], axis=1)
        scores = dot_nt(q, k) * HD ** (-0.5) + bias
        probs = jnp.exp(scores - lse_all[:, h : h + 1])
        d_probs = dot_nt(do, v)
        d_scores = (probs * (d_probs - delta) * HD ** (-0.5)).astype(BF)
        dq = dot_nn(d_scores, k)
        dq_ref[0, 0, :, h * LANES : (h + 1) * LANES] = rotated(dq, cos, -sin).astype(BF)
        dk = dot_tn(d_scores, q).reshape(blocks, r, LANES)
        dv = dot_tn(probs.astype(BF), do).reshape(blocks, r, LANES)
        here = slice(g * LANES, (g + 1) * LANES)
        dk_acc[pl.ds(first, blocks), :, here] += dk
        dv_acc[pl.ds(first, blocks), :, here] += dv

    @pl.when(s == ctx - 1)
    def _():
        for b in range(ctx):
            for g in range(kvc):
                here = slice(g * LANES, (g + 1) * LANES)
                at = g * LANES
                dk = rotated(dk_acc[b, :, here], cos_ref[b], -sin_ref[b])
                dkv_ref[b, 0, :, at : at + LANES] = dk.astype(BF)
                at += kvc * LANES
                dkv_ref[b, 0, :, at : at + LANES] = dv_acc[b, :, here].astype(BF)


def attend_back_call(z, q, k, v, qdoc, kdoc, o, do, lse, cos, sin, hc, kvc, script, moved, new, filled):
    ctx, m, r, _ = q.shape
    row = lambda b, s: (s, b, 0, 0)
    seq = lambda b, s: (0, b, 0, 0)
    table = pl.BlockSpec((ctx, r, LANES), lambda b, s: (0, 0, 0))
    return fused_call(
        z,
        "attend_back",
        14,
        functools.partial(attend_back_kernel, hc, kvc, ctx),
        (m, ctx),
        [
            pl.BlockSpec((1, 1, r, hc * LANES), row),
            pl.BlockSpec((ctx, 1, r, kvc * LANES), seq),
            pl.BlockSpec((ctx, 1, r, kvc * LANES), seq),
            pl.BlockSpec((1, 1, r, 1), row),
            pl.BlockSpec((ctx, 1, 1, r), seq),
            pl.BlockSpec((1, 1, r, hc * HD), row),
            pl.BlockSpec((1, 1, r, hc * HD), row),
            pl.BlockSpec((1, 1, r, LANES), row),
            table,
            table,
        ],
        [
            pl.BlockSpec((1, 1, r, hc * LANES), row),
            pl.BlockSpec((ctx, 1, r, 2 * kvc * LANES), seq),
        ],
        [sds((ctx, m, r, hc * LANES)), sds((ctx, m, r, 2 * kvc * LANES))],
        (q, k, v, qdoc, kdoc, o, do, lse, cos, sin),
        script,
        moved,
        new,
        filled,
        [pltpu.VMEM((ctx, r, kvc * LANES), F32), pltpu.VMEM((ctx, r, kvc * LANES), F32)],
    )


def mix_kernel(ctx, att_ref, x_ref, gain_ref, w_ref, mid_ref, normed_ref, rows_ref):
    rows = jnp.concatenate([att_ref[c, 0] for c in range(ctx)], axis=1)
    rows_ref[0] = rows
    mid = x_ref[0].astype(F32) + dot_nn(rows, w_ref[...])
    mid_ref[0] = mid
    scale = lax.rsqrt(jnp.mean(mid * mid, axis=-1, keepdims=True) + EPS)
    normed_ref[0] = (mid * scale * gain_ref[...]).astype(BF)


def mix_call(z, att, x, gain, w, script, moved, new, filled):
    ctx, m, r, cols = att.shape
    d = x.shape[-1]
    seq = pl.BlockSpec((1, r, d), lambda b: (b, 0, 0))
    whole = lambda b: (0, 0)
    return fused_call(
        z,
        "mix",
        16,
        functools.partial(mix_kernel, ctx),
        (m,),
        [
            pl.BlockSpec((ctx, 1, r, cols), lambda b: (0, b, 0, 0)),
            seq,
            pl.BlockSpec((1, d), whole),
            pl.BlockSpec(w.shape, whole, pipeline_mode=pl.Buffered(1)),
        ],
        [seq, seq, seq],
        [sds((m, r, d), F32), sds((m, r, d)), sds((m, r, d))],
        (att, x, gain, w),
        script,
        moved,
        new,
        filled,
    )


def turn_kernel(z, dn_ref, *refs):
    came_refs = refs[: z.ys - 1]
    mid_ref, cot_ref, gain_ref, w_ref = refs[z.ys - 1 : z.ys + 3]
    d_mid_ref, low_ref, all_ref, hold, send_sems, recv_sems, own_sems = refs[z.ys + 3 :]
    b, last = pl.program_id(0), pl.num_programs(0) - 1
    link = Link(z, send_sems, recv_sems, own_sems)
    cols = hold.shape[-1]

    def copies(n):
        remote = [
            pltpu.make_async_remote_copy(
                src_ref=hold.at[p, n],
                dst_ref=all_ref.at[link.c, n],
                send_sem=send_sems.at[n, j],
                recv_sem=recv_sems.at[n, j],
                device_id=(link.d, p),
                device_id_type=MESH,
            )
            for j, p in enumerate(link.ctx_peers())
        ]
        return remote, pltpu.make_async_copy(hold.at[link.c, n], all_ref.at[link.c, n], own_sems.at[n])

    d_normed = dn_ref[link.y, 0].astype(F32)
    for ref in came_refs:
        d_normed += ref[0].astype(F32)
    mid = mid_ref[0]
    scale = lax.rsqrt(jnp.mean(mid * mid, axis=-1, keepdims=True) + EPS)
    e = d_normed * gain_ref[...]
    d_mid = cot_ref[0].astype(F32) + (
        scale * e - mid * (scale * scale * scale) * jnp.mean(e * mid, axis=-1, keepdims=True)
    )
    d_mid_ref[0] = d_mid
    low = d_mid.astype(BF)
    low_ref[0] = low
    d_att = dot_nt(low, w_ref[...]).astype(BF)
    for c in range(z.ctx):
        hold[c, b] = d_att[:, c * cols : (c + 1) * cols]
    remote, own = copies(b)
    for copy in remote:
        copy.start()
    own.start()

    @pl.when(b == last)
    def _():
        for n in range(hold.shape[1]):
            remote, own = copies(n)
            for copy in remote:
                copy.wait_recv()
            for copy in remote:
                copy.wait_send()
            own.wait()


def turn_call(z, dn, came, mid, cot, gain, w, cols, script, moved, new, filled):
    ys, m, r, d = dn.shape
    seq = pl.BlockSpec((1, r, d), lambda b: (b, 0, 0))
    whole = lambda b: (0, 0)
    return fused_call(
        z,
        "turn",
        6,
        functools.partial(turn_kernel, z),
        (m,),
        [pl.BlockSpec((ys, 1, r, d), lambda b: (0, b, 0, 0))]
        + [seq] * (ys + 1)
        + [pl.BlockSpec((1, d), whole), pl.BlockSpec(w.shape, whole, pipeline_mode=pl.Buffered(1))],
        [seq, seq, pl.BlockSpec(memory_space=pltpu.HBM)],
        [sds((m, r, d), F32), sds((m, r, d)), sds((z.ctx, m, r, cols))],
        (dn, *came, mid, cot, gain, w),
        script,
        moved,
        new,
        filled,
        [
            pltpu.VMEM((z.ctx, m, r, cols), BF),
            pltpu.SemaphoreType.DMA((m, z.ctx)),
            pltpu.SemaphoreType.DMA((m, z.ctx)),
            pltpu.SemaphoreType.DMA((m,)),
        ],
    )


def mlp_kernel(
    z, x_ref, cot_ref, gate_ref, up_ref, down_ref,
    hid_ref, dg_ref, du_ref, dn_ref, out_ref,
    dn_send, dn_got, out_send, out_got, send_sems, recv_sems,
):
    other, y, b = pl.program_id(0) == 0, pl.program_id(1), pl.program_id(2)
    link = Link(z, send_sems, recv_sems, None)
    at = y * pl.num_programs(2) + b

    def copies(n):
        return [
            pltpu.make_async_remote_copy(
                src_ref=src.at[n],
                dst_ref=dst.at[n],
                send_sem=send_sems.at[which, n],
                recv_sem=recv_sems.at[which, n],
                device_id=link.ctx_dev(link.y, 1 - link.k),
                device_id_type=MESH,
            )
            for which, (src, dst) in enumerate(((dn_send, dn_got), (out_send, out_got)))
        ]

    @pl.when(other & (at == 0))
    def _():
        link.barrier(core_only=True)

    x, cot = x_ref[0, 0], cot_ref[0, 0]
    gate, up = dot_nn(x, gate_ref[...]), dot_nn(x, up_ref[...])
    d_hidden = dot_nt(cot, down_ref[...])
    sg = jax.nn.sigmoid(gate)
    act = gate * sg
    hidden = (act * up).astype(BF)
    hid_ref[0, 0] = hidden
    d_gate = (d_hidden * up * sg * (1.0 + gate * (1.0 - sg))).astype(BF)
    d_up = (d_hidden * act).astype(BF)
    dg_ref[0, 0] = d_gate
    du_ref[0, 0] = d_up
    out = dot_nn(hidden, down_ref[...])
    dn = dot_nt(d_gate, gate_ref[...]) + dot_nt(d_up, up_ref[...])

    @pl.when(other)
    def _():
        dn_send[at] = dn.astype(BF)
        out_send[at] = out.astype(BF)
        for copy in copies(at):
            copy.start()

    @pl.when(jnp.logical_not(other))
    def _():
        for copy in copies(at):
            copy.wait_recv()
        dn_ref[0, 0] = (dn + dn_got[at].astype(F32)).astype(BF)
        out_ref[0, 0] = (out + out_got[at].astype(F32)).astype(BF)
        for copy in copies(at):
            copy.wait_send()


def mlp_call(z, x, cot, gate, up, down):
    ctx, m, r, d = x.shape
    f = down.shape[0]
    row = lambda a, y, b: (a * z.ys + y, b, 0, 0)
    whole = lambda a, y, b: (0, 0)
    mine = lambda a, y, b: (a * y, a * b, 0, 0)
    block = lambda width, at: pl.BlockSpec((1, 1, r, width), at)
    resident = lambda w: pl.BlockSpec(w.shape, whole, pipeline_mode=pl.Buffered(1))
    held = pltpu.VMEM((z.ys * m, r, d), BF)
    return pl.pallas_call(
        functools.partial(mlp_kernel, z),
        name="mlp",
        grid=(2, z.ys, m),
        in_specs=[block(d, row), block(d, row), resident(gate), resident(up), resident(down)],
        out_specs=[block(f, row), block(f, row), block(f, row), block(d, mine), block(d, mine)],
        scratch_shapes=[held] * 4
        + [pltpu.SemaphoreType.DMA((2, z.ys * m)), pltpu.SemaphoreType.DMA((2, z.ys * m))],
        out_shape=[sds((ctx, m, r, f))] * 3 + [sds((z.ys, m, r, d))] * 2,
        compiler_params=pltpu.CompilerParams(
            collective_id=13, has_side_effects=True, vmem_limit_bytes=VMEM_LIMIT
        ),
    )(x, cot, gate, up, down)


def tail_kernel(
    z, hc, dq_hbm, dkv_hbm, w_ref, q_ref, kv_ref, po_own, po_send, up_ref, gain_ref, gate_hbm,
    x_hbm, d_mid_hbm, mid_hbm, out_hbm, came_hbm,
    outputs_ref, grad_ref, po_out, q_out, kv_out, gate_out, up_out,
    dq, dkv, x, d_mid, mid, out_own, out_came, da_core, da_got, da_send, da_came,
    po_came, po_ref, q_x, q_col, q_z, kv_x, kv_col, kv_z, po_x, po_col, po_z, up_z, mine_q, mine_kv, mine_up,
    send_sems, recv_sems, local_sems,
):
    link = Link(z, send_sems, recv_sems, local_sems)
    link.landed = []
    wide = lambda a: a.astype(F32)
    ys, seqs, r = z.ys, x.shape[0], x.shape[1]
    half = dq.shape[-1]
    loads = [link.keep(dq_hbm, dq), link.keep(dkv_hbm, dkv)]
    later = [
        link.keep(x_hbm, x),
        link.keep(d_mid_hbm, d_mid),
        link.keep(mid_hbm, mid),
        link.keep(out_hbm.at[link.y], out_own),
        link.keep(came_hbm, out_came),
    ]
    link.barrier()

    def inner_puts(src, dst):
        return [
            link.put(src.at[:, link.inner_to(j)], dst.at[j - 1], link.dp_dev(link.o, link.inner_to(j)))
            for j in range(1, z.inner)
        ]

    def ring(col, got, step, copies):
        if copies:
            link.arrived(copies[-1])
            total = wide(got[step - 2]) + wide(col[link.outer_from(step)])
            if step == z.outer:
                return total
            got[step - 2] = total.astype(BF)
            src = got.at[step - 2]
        else:
            src = col.at[link.outer_from(1)]
        copies.append(link.put(src, got.at[step - 1], link.dp_dev(link.outer_to(1), link.i)))

    def columns(part, came, col, copies):
        for copy in copies:
            link.arrived(copy)
        for o in range(z.outer):
            total = wide(part[o, link.i])
            for j in range(z.inner - 1):
                total += wide(came[j, o])
            col[o] = total.astype(BF)

    up_way, q_way, kv_way, po_way = [], [], [], []
    ring(up_ref, up_z, 1, up_way)
    q_in = inner_puts(q_ref, q_x)
    po_y = []
    for j in range(1, ys):
        to = lax.rem(link.y + j, ys)
        po_y.append(link.put(po_send.at[j - 1], po_came.at[j - 1], link.ctx_dev(to, link.k)))
    exchange_ctx(link, gate_hbm, lambda s: gate_out.at[s])
    link.keep(gate_hbm.at[link.c], gate_out.at[link.c])
    for copy in loads:
        copy.wait()

    def da_of(place, b):
        left = dot_nt(dq[place, b], w_ref[:, :half])
        return left + dot_nt(dkv[place, b], w_ref[:, half:])

    core = []
    for y in range(ys):
        for b in range(seqs):
            da_core[y, b] = da_of(y * 2 + 1 - link.k, b).astype(BF)
            core.append(link.put(da_core.at[y, b], da_got.at[y, b], link.ctx_dev(link.y, 1 - link.k)))
    kv_in = inner_puts(kv_ref, kv_x)
    for copy in core:
        link.arrived(copy)
    y_ways = []
    for j in list(range(1, ys)) + [0]:
        y = lax.rem(link.y + j, ys)
        for b in range(seqs):
            total = da_of(y * 2 + link.k, b) + wide(da_got[y, b])
            if j == 0:
                grad_ref[b] = total
            else:
                da_send[j - 1, b] = total.astype(BF)
        if j > 0:
            y_ways.append(link.put(da_send.at[j - 1], da_came.at[j - 1], link.ctx_dev(y, link.k)))
    ring(up_ref, up_z, 2, up_way)
    columns(q_ref, q_x, q_col, q_in)
    ring(q_col, q_z, 1, q_way)
    for copy in po_y:
        link.arrived(copy)
    for o in range(z.outer):
        total = wide(po_own[o])
        for j in range(ys - 1):
            total += wide(po_came[j, o])
        po_ref[o] = total.astype(BF)
    po_in = inner_puts(po_ref, po_x)
    for copy in later:
        copy.wait()
    link.local = link.local[len(loads) + len(later) :]

    rows = 32 if r % 32 == 0 else r
    count = r // rows
    at_of = lambda step: (lax.div(step, count), pl.ds(pl.multiple_of(lax.rem(step, count) * rows, rows), rows))

    def finish_outputs(step, _):
        b, at = at_of(step)
        total = mid[b, at] + wide(out_own[b, at])
        for j in range(ys - 1):
            total += wide(out_came[j, b, at])
        outputs_ref[b, at] = total
        return 0

    lax.fori_loop(0, seqs * count, finish_outputs, 0)
    for step in range(3, z.outer):
        ring(up_ref, up_z, step, up_way)
    columns(kv_ref, kv_x, kv_col, kv_in)
    ring(kv_col, kv_z, 1, kv_way)
    ring(q_col, q_z, 2, q_way)
    mine_up[...] = ring(up_ref, up_z, z.outer, up_way).astype(BF)
    exchange_ctx(link, mine_up, lambda s: up_out.at[s])
    link.keep(mine_up.at[link.c], up_out.at[link.c])
    columns(po_ref, po_x, po_col, po_in)
    ring(po_col, po_z, 1, po_way)
    for step in range(3, z.outer + 1):
        ring(kv_col, kv_z, step - 1, kv_way)
        if step < z.outer:
            ring(q_col, q_z, step, q_way)
        ring(po_col, po_z, step - 1, po_way)
    for copy in y_ways:
        link.arrived(copy)
    gain = gain_ref[...]

    def finish_grad(step, _):
        b, at = at_of(step)
        total = grad_ref[b, at]
        for j in range(ys - 1):
            total += wide(da_came[j, b, at])
        value = wide(x[b, at])
        scale = lax.rsqrt(jnp.mean(value * value, axis=-1, keepdims=True) + EPS)
        e = total * gain
        grad_ref[b, at] = d_mid[b, at] + (
            scale * e - value * (scale * scale * scale) * jnp.mean(e * value, axis=-1, keepdims=True)
        )
        return 0

    lax.fori_loop(0, seqs * count, finish_grad, 0)
    mine_q[...] = ring(q_col, q_z, z.outer, q_way).astype(BF)
    exchange_ctx(link, mine_q, lambda s: q_out.at[s])
    link.keep(mine_q.at[link.c], q_out.at[link.c])
    mine_kv[...] = ring(kv_col, kv_z, z.outer, kv_way).astype(BF)
    exchange_ctx(link, mine_kv, lambda s: kv_out.at[s])
    link.keep(mine_kv.at[link.c], kv_out.at[link.c])
    po_out[...] = ring(po_col, po_z, z.outer, po_way)
    link.finish()


def tail_call(z, hc, dq, dkv, w, part_q, part_kv, po, po_send, up_col, gain, gate_mine, x, d_mid, mid, out_pair, out_came):
    m, r, d = x.shape
    one = lambda a: a.shape[2:]
    q1, kv1, po1, up1 = one(part_q), one(part_kv), one(po), up_col.shape[1:]
    vm = lambda shape, dtype=BF: pltpu.VMEM(tuple(shape), dtype)
    hbm, vmem = pl.BlockSpec(memory_space=pltpu.HBM), pl.BlockSpec(memory_space=pltpu.VMEM)
    scratch = [vm(dq.shape), vm(dkv.shape), vm(x.shape), vm(x.shape, F32), vm(x.shape, F32), vm(x.shape)]
    scratch += [vm((z.ys - 1,) + x.shape), vm((z.ys,) + x.shape), vm((z.ys,) + x.shape)]
    scratch += [vm((z.ys - 1,) + x.shape), vm((z.ys - 1,) + x.shape)]
    scratch += [vm(po_send.shape), vm(po.shape)]
    for shape in (q1, kv1, po1):
        scratch += [vm((z.inner - 1, z.outer) + shape), vm((z.outer,) + shape), vm((z.outer - 1,) + shape)]
    scratch += [vm((z.outer - 1,) + up1), vm(q1), vm(kv1), vm(up1)]
    scratch += [
        pltpu.SemaphoreType.DMA((64,)),
        pltpu.SemaphoreType.DMA((64,)),
        pltpu.SemaphoreType.DMA((16,)),
    ]
    return pl.pallas_call(
        functools.partial(tail_kernel, z, hc),
        name="tail",
        in_specs=[hbm, hbm] + [vmem] * 7 + [hbm] * 6,
        out_specs=[vmem, vmem, vmem, hbm, hbm, hbm, hbm],
        out_shape=[
            sds(x.shape, F32),
            sds(x.shape, F32),
            sds(po1, F32),
            sds(q1),
            sds(kv1),
            sds(gate_mine.shape),
            sds(up1),
        ],
        scratch_shapes=scratch,
        compiler_params=pltpu.CompilerParams(
            collective_id=15, has_side_effects=True, vmem_limit_bytes=VMEM_LIMIT
        ),
    )(dq, dkv, w, part_q, part_kv, po, po_send, up_col, gain, gate_mine, x, d_mid, mid, out_pair, out_came)


def pad_heads(w, heads, split):
    rows = w.shape[0]
    if split:
        w = jnp.pad(w.reshape(rows, heads, 2, HALF), ((0, 0), (0, 0), (0, 0), (0, LANES // 2 - HALF)))
    else:
        w = jnp.pad(w.reshape(rows, heads, HD), ((0, 0), (0, 0), (0, LANES - HD)))
    return w.reshape(rows, heads * LANES)


def unpad_heads(w, heads, split):
    if split:
        w = w.reshape(w.shape[:-1] + (heads, 2, LANES // 2))[..., :HALF]
    else:
        w = w.reshape(w.shape[:-1] + (heads, LANES))[..., :HD]
    return w.reshape(w.shape[: w.ndim - (3 if split else 2)] + (heads * HD,))


def rope_tables(ctx, r):
    frequency = THETA ** (-(jnp.arange(HALF, dtype=F32) * (2.0 / HD)))
    angles = jnp.arange(ctx * r, dtype=jnp.int32).astype(F32)[:, None] * frequency[None, :]
    pad = ((0, 0), (0, LANES // 2 - HALF))
    cos, sin = jnp.pad(jnp.cos(angles), pad), jnp.pad(jnp.sin(angles), pad)
    cos = jnp.concatenate([cos, cos], axis=1).reshape(ctx, r, LANES)
    sin = jnp.concatenate([-sin, sin], axis=1).reshape(ctx, r, LANES)
    return cos, sin


def per_device(
    inputs, segments, cotangent, w_query, w_key, w_value, w_out, w_gate, w_up, w_down, gain_attn, gain_ffn
):
    z = Sizes(lax.axis_size("dp"), lax.axis_size("ctx"))
    dp, ctx, outer, inner, ys = z.dp, z.ctx, z.outer, z.inner, z.ys
    m, r, d = inputs.shape
    rows = w_query.shape[0]
    frows, ff = w_down.shape[0], w_gate.shape[1]
    f = ff // ctx
    hc, kvc = H // ctx, KV // ctx
    width = (hc + 2 * kvc) * LANES
    c = lax.axis_index("ctx")
    di = lax.axis_index("dp")
    oi, ii = di // inner, di % inner
    yi, ki = c // 2, c % 2
    dyn = lambda a, at, axis: lax.dynamic_index_in_dim(a, at, axis, keepdims=False)

    pack_qkv = jnp.concatenate(
        [
            pad_heads(w_query, H, True).reshape(rows, ctx, hc * LANES),
            pad_heads(w_key, KV, True).reshape(rows, ctx, kvc * LANES),
            pad_heads(w_value, KV, False).reshape(rows, ctx, kvc * LANES),
        ],
        axis=2,
    ).transpose(1, 0, 2)
    by_rank = lambda w: w.reshape(rows, dp, ctx, frows).transpose(2, 0, 1, 3).reshape(ctx, rows, f)
    pack_gate, pack_up = by_rank(w_gate), by_rank(w_up)
    gains = jnp.stack([gain_attn, gain_ffn]).astype(F32)
    gains = jnp.pad(gains, ((0, 6), (0, LANES - rows)))

    steps = list(range(1, outer))
    by_owner = lambda buf: lambda s: buf.at[s]
    out_slot = lambda link, buf: lambda s: buf.at[s, :, link.k]

    def first_script(link, ins, outs, scratch):
        x, seg, qkv, gain, wo, pg, pu, wd = ins
        x_all, seg_all, g_qkv, g_gain, g_out, g_gate, g_up, g_down = outs
        (hold,) = scratch
        load = pltpu.make_async_copy(x, hold, link.sems[2].at[15])
        load.start()
        mine = [
            link.keep(qkv.at[link.c], g_qkv.at[link.d, link.c]),
            link.keep(gain, g_gain.at[link.d, link.c]),
            link.keep(wo, g_out.at[link.d, link.y, link.k]),
            link.keep(seg, seg_all.at[link.c]),
        ]
        a2a = exchange_ctx(link, qkv, lambda s: g_qkv.at[link.d, s])
        a2a += [link.put(gain, g_gain.at[link.d, link.c], (link.d, p)) for p in link.ctx_peers()]
        for p in link.ctx_peers():
            link.put(seg, seg_all.at[link.c], (link.d, p))
        over_y = [
            link.put(wo, g_out.at[link.d, link.y, link.k], link.ctx_dev(p, link.k)) for p in link.y_peers()
        ]
        ways_x = gather_ctx_start(link, x, x_all)
        exchange_ctx(link, pg, lambda s: g_gate.at[link.d, s])
        for copy in a2a:
            link.arrived(copy)
        for copy in mine:
            copy.wait()
        link.local = []
        split = ctx // 2
        small = [lambda s: g_qkv.at[s, :split], lambda s: g_qkv.at[s, split:], by_owner(g_gain)]
        ways = [ring_outer(link, slot, 1) for slot in small]
        for slot in small:
            pass_inner(link, slot, 0)
        link.keep(pg.at[link.c], g_gate.at[link.d, link.c])
        link.keep(pu.at[link.c], g_up.at[link.d, link.c])
        link.keep(wd, g_down.at[link.d])
        load.wait()
        store = pltpu.make_async_copy(hold, x_all.at[link.c], link.sems[2].at[14])
        store.start()
        for step in steps:
            came, ways = ways, []
            for copy, slot in zip(came, small):
                link.arrived(copy)
                if step < steps[-1]:
                    ways.append(ring_outer(link, slot, step + 1))
                pass_inner(link, slot, step)
        for copy in over_y:
            link.arrived(copy)
        ring_outer(link, out_slot(link, g_out), 1)
        pass_inner(link, out_slot(link, g_out), 0)
        gather_ctx_forward(link, x_all, ways_x)
        store.wait()

    x_all, seg_all, g_qkv, g_gain, g_out, g_gate, g_up, g_down = communicate(
        z,
        "gather_first",
        1,
        first_script,
        (inputs, segments, pack_qkv, gains, w_out, pack_gate, pack_up, w_down),
        (
            sds((ctx, m, r, d)),
            sds((ctx, m, r), jnp.int32),
            sds((dp, ctx, rows, width)),
            sds((dp, ctx, 8, LANES), F32),
            sds((dp, ys, 2, rows, d)),
            sds((dp, ctx, rows, f)),
            sds((dp, ctx, rows, f)),
            sds((dp, frows, d)),
        ),
        [pltpu.VMEM((m, r, d), BF)],
    )
    gain_a = g_gain[:, :, 0, :rows].reshape(1, d)
    gain_f = g_gain[:, :, 1, :rows].reshape(1, d)
    wqkv = g_qkv.reshape(d, width)
    cos, sin = rope_tables(ctx, r)
    qdoc = seg_all.reshape(ctx, m, r, 1)
    kdoc = seg_all.reshape(ctx, m, 1, r)
    early, late = range(m // 2), range(m // 2, m)

    def qkv_cargo(cargo, moved, bufs):
        (pu,), (g_out, g_gate, g_up) = moved, bufs
        exchange_ctx(cargo, pu, lambda s: g_up.at[cargo.d, s])
        for slot, step in ((out_slot(cargo, g_out), 2), (by_owner(g_gate), 1)):
            ring_outer(cargo, slot, step)
            pass_inner(cargo, slot, step - 1)

    g_out, g_gate, g_up, normed_a, q, k, v = qkv_call(
        z, x_all, gain_a, wqkv, cos, sin, hc, kvc,
        qkv_cargo, (pack_up,), (), (g_out, g_gate, g_up),
    )

    def attend_cargo(cargo, moved, bufs):
        (cot,), (g_out, g_gate, g_up, cot_all) = moved, bufs
        own_y(cargo, cot, cot_all, early)
        for slot, step in ((out_slot(cargo, g_out), 3), (by_owner(g_gate), 2), (by_owner(g_up), 1)):
            ring_outer(cargo, slot, step)
            pass_inner(cargo, slot, step - 1)

    g_out, g_gate, g_up, cot_all, att, lse = attend_call(
        z, q, k, v, qdoc, kdoc, hc, kvc, attend_cargo, (cotangent,), (sds((ctx, m, r, d)),), (g_out, g_gate, g_up)
    )

    def second_script(link, ins, outs, scratch):
        att, cot = ins[:2]
        g_out, g_gate, g_up, g_down, cot_all, att_all = outs
        (hold,) = scratch
        load = pltpu.make_async_copy(cot, hold, link.sems[2].at[15])
        load.start()
        link.keep(att.at[link.c], att_all.at[link.c])
        first = len(link.inflight)
        pass_inner(link, out_slot(link, g_out), 3)
        last_out = link.inflight[first:]
        exchange_ctx(link, att, lambda s: att_all.at[s])
        for slot, step in ((by_owner(g_gate), 3), (by_owner(g_up), 2)):
            ring_outer(link, slot, step)
        pass_inner(link, by_owner(g_gate), 2)
        pass_inner(link, by_owner(g_down), 0)
        pass_core(link, cot_all, early)
        load.wait()
        store = pltpu.make_async_copy(hold, cot_all.at[link.slot(link.y, True)], link.sems[2].at[14])
        store.start()
        for copy in last_out:
            link.arrived(copy)
        both = g_out.at[:, :, link.k]
        link.put(both, both, link.ctx_dev(link.y, 1 - link.k))
        store.wait()

    g_out, g_gate, g_up, g_down, cot_all, att_all = communicate(
        z,
        "exchange_heads",
        2,
        second_script,
        (att, cotangent),
        (sds(att.shape),),
        [pltpu.VMEM((m, r, d), BF)],
        (g_out, g_gate, g_up, g_down, cot_all),
    )
    wo = g_out.reshape(d, d)

    def mix_cargo(cargo, moved, bufs):
        (cot,), (g_gate, g_up, g_down, cot_all) = moved, bufs
        own_y(cargo, cot, cot_all, late)
        ring_outer(cargo, by_owner(g_up), 3)
        ring_columns(cargo, g_down, 1)
        pass_inner(cargo, by_owner(g_gate), 3)
        pass_inner(cargo, by_owner(g_up), 1)

    g_gate, g_up, g_down, cot_all, mid, normed, att_rows = mix_call(
        z, att_all, inputs, gain_f, wo, mix_cargo, (cotangent,), (), (g_gate, g_up, g_down, cot_all)
    )
    att_rows = att_rows.reshape(m * r, H * HD)

    def third_script(link, ins, outs, scratch):
        x, (g_up, g_down, cot_all, x_all), (hold,) = ins[0], outs, scratch
        load = pltpu.make_async_copy(x, hold, link.sems[2].at[15])
        load.start()
        ways = gather_ctx_start(link, x, x_all, True)
        way = ring_columns(link, g_down, 2)
        pass_inner(link, by_owner(g_up), 2)
        pass_inner(link, by_owner(g_up), 3)
        pass_core(link, cot_all, late)
        load.wait()
        store = pltpu.make_async_copy(hold, x_all.at[link.slot(link.y, True)], link.sems[2].at[14])
        store.start()
        for step in steps[2:]:
            link.arrived(way)
            way = ring_columns(link, g_down, step)
        gather_ctx_forward(link, x_all, ways, True)
        store.wait()

    g_up, g_down, cot_all, normed_all = communicate(
        z,
        "gather_third",
        3,
        third_script,
        (normed,),
        (sds((ctx, m, r, d)),),
        [pltpu.VMEM((m, r, d), BF)],
        (g_up, g_down, cot_all),
    )
    w_gate_c, w_up_c, w_down_c = g_gate.reshape(d, f), g_up.reshape(d, f), g_down.reshape(f, d)

    hidden, d_gate, d_up, dn_pair, out_pair = mlp_call(z, normed_all, cot_all, w_gate_c, w_up_c, w_down_c)

    dp_perm = lambda fn: [(o * inner + i, fn(o, i)) for o in range(outer) for i in range(inner)]
    ctx_perm = lambda fn: [(y * 2 + k, fn(y, k)) for y in range(ys) for k in range(2)]
    wide = lambda a: a.astype(F32)
    flat = lambda a: a.reshape(ctx * m * r, a.shape[-1])

    def after(a, dep):
        return lax.optimization_barrier((a, dep))[0]

    def to_core(a):
        return lax.ppermute(a, "ctx", ctx_perm(lambda y, k: y * 2 + 1 - k))

    def to_y(pair):
        return [
            lax.ppermute(
                dyn(pair, (yi + j) % ys, 0), "ctx", ctx_perm(lambda y, k: (y + j) % ys * 2 + k)
            )
            for j in range(1, ys)
        ]

    def to_inner(part):
        return [
            lax.ppermute(
                dyn(part, (ii + j) % inner, 1), "dp", dp_perm(lambda o, i: o * inner + (i + j) % inner)
            )
            for j in range(1, inner)
        ]

    column = lambda part, came: (wide(dyn(part, ii, 1)) + sum(wide(a) for a in came)).astype(BF)
    close = lambda own, came: wide(own) + sum(wide(a) for a in came)

    dn_came = to_y(dn_pair)
    part_down = dot_tn(flat(hidden), flat(cot_all)).astype(BF).reshape(outer, inner, frows, d)
    par = oi % 2
    by_parity = part_down.reshape(outer // 2, 2, inner, frows, d)
    down_near, down_rest = dyn(by_parity, 1 - par, 1), dyn(by_parity, par, 1)
    near_x = to_inner(down_near)
    rest_x = to_inner(down_rest)
    shape_g = (outer, inner, ctx, rows, f)
    part_gate = dot_tn(flat(normed_all), flat(d_gate)).astype(BF).reshape(shape_g)
    gate_x = to_inner(part_gate)
    part_up = dot_tn(flat(normed_all), flat(after(d_up, part_gate))).astype(BF).reshape(shape_g)
    near = [j for j in steps if j in (1, outer - 1)]
    mid_way = [j for j in steps if j not in near]
    near_col = column(down_near, after(near_x, part_up))

    def to_near(link, col, dst):
        for j in near:
            to = link.outer_to(j)
            link.put(col.at[lax.div(to, 2)], dst.at[j - 1], link.dp_dev(to, link.i))

    def to_rest(link, col, dst):
        for j in mid_way:
            to = link.outer_to(j)
            link.put(col.at[lax.div(to, 2)], dst.at[j - 1], link.dp_dev(to, link.i))

    def turn_cargo(cargo, moved, bufs):
        to_near(cargo, moved[0], bufs[0])

    down_z, d_mid, d_mid_low, d_att_all = turn_call(
        z, dn_pair, dn_came, mid, cotangent, gain_f, wo, hc * HD,
        turn_cargo, (near_col,), (sds((outer - 1, frows, d)),), (),
    )

    part_out = dot_tn(att_rows, d_mid_low.reshape(m * r, d)).astype(BF).reshape(dp, ys, 2, rows, d)
    rest_col = column(down_rest, after(rest_x, d_att_all))
    gate_col = column(part_gate, after(gate_x, d_att_all))

    def back_cargo(cargo, moved, bufs):
        (rest_col, gate_col, part_up, part_out, out_pair), (down_z, gate_z, up_x, po_in, out_came) = moved, bufs
        scatter_y(cargo, out_pair, out_came)
        scatter_inner(cargo, part_up, up_x)
        to_rest(cargo, rest_col, down_z)
        scatter_outer(cargo, gate_col, gate_z, near)
        cargo.put(part_out.at[:, :, 1 - cargo.k], po_in, cargo.ctx_dev(cargo.y, 1 - cargo.k))

    down_z, gate_z, up_x, po_in, out_came, dq, dkv = attend_back_call(
        z, q, k, v, qdoc, kdoc, att, d_att_all, lse, cos, sin, hc, kvc,
        back_cargo,
        (rest_col, gate_col, part_up, part_out, out_pair),
        (
            sds((outer - 1,) + gate_col.shape[1:]),
            sds((inner - 1, outer) + gate_col.shape[1:]),
            sds((dp, ys, rows, d)),
            sds((ys - 1, m, r, d)),
        ),
        (down_z,),
    )
    po_both = lambda at: wide(dyn(dyn(part_out, ki, 2), at, 1)) + wide(dyn(po_in, at, 1))
    po_send = jnp.stack([po_both((yi + j) % ys).astype(BF) for j in range(1, ys)])
    po_send = po_send.reshape(ys - 1, outer, inner, rows, d)
    gate_far = [
        lax.ppermute(
            dyn(after(gate_col, dq), (oi + j) % outer, 0), "dp", dp_perm(lambda o, i: (o + j) % outer * inner + i)
        )
        for j in mid_way
    ]
    part_q = dot_tn(flat(normed_a), flat(dq)).astype(BF).reshape(outer, inner, ctx, rows, hc * LANES)
    part_kv = dot_tn(flat(normed_a), flat(dkv)).astype(BF).reshape(outer, inner, ctx, rows, 2 * kvc * LANES)
    up_col = column(part_up, [up_x[j] for j in range(inner - 1)])
    po = po_both(yi).astype(BF).reshape(outer, inner, rows, d)
    gate_near = [gate_z[j - 1] for j in near]
    gate_mine = close(dyn(gate_col, oi, 0), gate_near + gate_far).astype(BF)

    outputs, input_grad, grad_out, q_all, kv_all, gate_all, up_all = tail_call(
        z, hc, dq, dkv, wqkv, part_q, part_kv, po, po_send, up_col, gain_a, gate_mine,
        inputs, d_mid, mid, out_pair, out_came,
    )
    grad_down = close(dyn(rest_col, oi // 2, 0), [down_z[j - 1] for j in steps])
    spread = lambda a: wide(a).reshape(ctx, rows, dp, frows).transpose(1, 2, 0, 3).reshape(rows, ff)
    grad_gate, grad_up = spread(gate_all), spread(up_all)
    cols = lambda a, heads, split: (
        unpad_heads(wide(a), heads, split).transpose(1, 0, 2).reshape(rows, ctx * heads * HD)
    )
    grad_query = cols(q_all, hc, True)
    grad_key = cols(kv_all[:, :, : kvc * LANES], kvc, True)
    grad_value = cols(kv_all[:, :, kvc * LANES :], kvc, False)

    along = lambda pairs, gain: sum(jnp.sum(wide(w) * g, axis=1) for w, g in pairs) / wide(gain)
    grad_gain_a = along(((w_query, grad_query), (w_key, grad_key), (w_value, grad_value)), gain_attn)
    grad_gain_f = along(((w_gate, grad_gate), (w_up, grad_up)), gain_ffn)
    return (
        outputs,
        input_grad,
        grad_query,
        grad_key,
        grad_value,
        grad_out,
        grad_gate,
        grad_up,
        grad_down,
        grad_gain_a,
        grad_gain_f,
    )


def solution(mesh):
    rows, vec, tok = P(("dp", "ctx"), None), P(("dp", "ctx")), P("dp", "ctx", None)
    return jax.shard_map(
        per_device,
        mesh=mesh,
        in_specs=(tok, P("dp", "ctx"), tok) + (rows,) * 7 + (vec, vec),
        out_specs=(tok, tok) + (rows,) * 7 + (vec, vec),
        check_vma=False,
    )
```

```python
import functools

import jax
import jax.numpy as jnp
from jax import lax
from jax.experimental import pallas as pl
from jax.experimental.pallas import tpu as pltpu
from jax.sharding import PartitionSpec as P

H = 16
KV = 8
HD = 96
HALF = HD // 2
LANES = 128
SPAN = 512

EPS = 1e-05
THETA = 100000.0
MASKED = -1e30

BF = jnp.bfloat16
F32 = jnp.float32
MESH = pl.DeviceIdType.MESH
VMEM_LIMIT = 60 * 1024 * 1024


def sds(shape, dtype=BF):
    return jax.ShapeDtypeStruct(tuple(shape), dtype)


def dot_nn(a, b):
    return lax.dot_general(a, b, (((1,), (0,)), ((), ())), preferred_element_type=F32)


def dot_nt(a, b):
    return lax.dot_general(a, b, (((1,), (1,)), ((), ())), preferred_element_type=F32)


def dot_tn(a, b):
    return lax.dot_general(a, b, (((0,), (0,)), ((), ())), preferred_element_type=F32)


class Sizes:
    def __init__(self, dp, ctx):
        self.dp, self.ctx = dp, ctx
        self.outer = 4 if dp % 4 == 0 else dp
        self.inner = dp // self.outer
        self.ys = ctx // 2


class Link:
    def __init__(self, z, send_sems, recv_sems, local_sems):
        self.z = z
        self.d = lax.axis_index("dp")
        self.c = lax.axis_index("ctx")
        self.o, self.i = lax.div(self.d, z.inner), lax.rem(self.d, z.inner)
        self.y, self.k = lax.div(self.c, 2), lax.rem(self.c, 2)
        self.sems = (send_sems, recv_sems, local_sems)
        self.sent, self.inflight, self.local = 0, [], []

    def ctx_dev(self, y, k):
        return (self.d, y * 2 + k)

    def slot(self, y, rel):
        return y + self.z.ys if rel else y * 2 + self.k

    def slot_across(self, y, rel):
        return y if rel else y * 2 + self.k

    def ctx_peers(self):
        n = self.z.ctx
        return [lax.rem(self.c + j, n) for j in range(1, n)]

    def y_peers(self):
        n = self.z.ys
        return [lax.rem(self.y + j, n) for j in range(1, n)]

    def outer_to(self, j):
        return lax.rem(self.o + j, self.z.outer)

    def outer_from(self, j):
        return lax.rem(self.o + self.z.outer - j, self.z.outer)

    def inner_to(self, j):
        return lax.rem(self.i + j, self.z.inner)

    def dp_dev(self, o, i):
        return (o * self.z.inner + i, self.c)

    def barrier(self, core_only=False):
        devices = [(self.d, c) for c in self.ctx_peers()]
        if core_only:
            devices = [self.ctx_dev(self.y, 1 - self.k)]
            self.signal_all(devices)
            return
        devices += [self.dp_dev(self.outer_to(j), self.i) for j in range(1, self.z.outer)]
        devices += [self.dp_dev(self.o, self.inner_to(j)) for j in range(1, self.z.inner)]
        self.signal_all(devices)

    def signal_all(self, devices):
        barrier = pltpu.get_barrier_semaphore()
        for device in devices:
            pl.semaphore_signal(barrier, inc=1, device_id=device, device_id_type=MESH)
        pl.semaphore_wait(barrier, len(devices))

    def put(self, src, dst, device):
        n = self.sent
        self.sent += 1
        copy = pltpu.make_async_remote_copy(
            src_ref=src,
            dst_ref=dst,
            send_sem=self.sems[0].at[n],
            recv_sem=self.sems[1].at[n],
            device_id=device,
            device_id_type=MESH,
        )
        copy.start()
        self.inflight.append(copy)
        return copy

    def keep(self, src, dst):
        copy = pltpu.make_async_copy(src, dst, self.sems[2].at[len(self.local)])
        copy.start()
        self.local.append(copy)
        return copy

    def arrived(self, copy):
        copy.wait_recv()
        self.inflight = [other for other in self.inflight if other is not copy]
        self.landed.append(copy)

    def finish(self):
        for copy in self.inflight:
            copy.wait_recv()
        for copy in self.landed + self.inflight:
            copy.wait_send()
        for copy in self.local:
            copy.wait()

    landed = None


def communicate(z, name, cid, script, ins, outs, scratch=(), filled=()):
    filled = tuple(filled)
    outs = [sds(a.shape, a.dtype) for a in filled] + list(outs)
    ins = tuple(ins) + filled
    n_in, n_out = len(ins), len(outs)
    aliases = {n_in - len(filled) + n: n for n in range(len(filled))}

    def kernel(*refs):
        in_refs, out_refs = refs[:n_in], refs[n_in : n_in + n_out]
        send, recv, local = refs[n_in + n_out : n_in + n_out + 3]
        link = Link(z, send, recv, local)
        link.landed = []
        link.barrier()
        script(link, in_refs, out_refs, refs[n_in + n_out + 3 :])
        link.finish()

    hbm = pl.BlockSpec(memory_space=pltpu.HBM)
    return pl.pallas_call(
        kernel,
        name=name,
        out_shape=list(outs),
        in_specs=[hbm] * n_in,
        out_specs=[hbm] * n_out,
        input_output_aliases=aliases,
        scratch_shapes=[
            pltpu.SemaphoreType.DMA((64,)),
            pltpu.SemaphoreType.DMA((64,)),
            pltpu.SemaphoreType.DMA((16,)),
        ]
        + list(scratch),
        compiler_params=pltpu.CompilerParams(
            collective_id=cid, has_side_effects=True, vmem_limit_bytes=VMEM_LIMIT
        ),
    )(*ins)


def gather_ctx_start(link, src, buf, rel=False):
    ways = []
    slot = buf.at[link.slot(link.y, rel)]
    for j in range(1, link.z.ys):
        to = lax.rem(link.y + j, link.z.ys)
        frm = lax.rem(link.y + link.z.ys - j, link.z.ys)
        ways.append((frm, link.put(src, slot, link.ctx_dev(to, link.k))))
    link.put(src, buf.at[link.slot_across(link.y, rel)], link.ctx_dev(link.y, 1 - link.k))
    return ways


def gather_ctx_forward(link, buf, ways, rel=False):
    for frm, copy in ways:
        link.arrived(copy)
        link.put(
            buf.at[link.slot(frm, rel)], buf.at[link.slot_across(frm, rel)], link.ctx_dev(link.y, 1 - link.k)
        )


def exchange_ctx(link, pack, slot_of):
    return [link.put(pack.at[c], slot_of(link.c), (link.d, c)) for c in link.ctx_peers()]


def gather_dp_start(link, slot_of):
    own = slot_of(link.d)
    ways = []
    for j in range(1, link.z.outer):
        copy = link.put(own, own, link.dp_dev(link.outer_to(j), link.i))
        ways.append((link.outer_from(j), copy))
    for j in range(1, link.z.inner):
        link.put(own, own, link.dp_dev(link.o, link.inner_to(j)))
    return ways


def gather_dp_forward(link, slot_of, ways):
    for frm, copy in ways:
        link.arrived(copy)
        slot = slot_of(frm * link.z.inner + link.i)
        for j in range(1, link.z.inner):
            link.put(slot, slot, link.dp_dev(link.o, link.inner_to(j)))


def scatter_inner(link, src, dst):
    for j in range(1, link.z.inner):
        to = link.inner_to(j)
        link.put(src.at[:, to], dst.at[j - 1], link.dp_dev(link.o, to))


def scatter_outer(link, src, dst, js):
    for j in js:
        to = link.outer_to(j)
        link.put(src.at[to], dst.at[j - 1], link.dp_dev(to, link.i))


def scatter_core(link, src, dst):
    link.put(src.at[:, 1 - link.k], dst, link.ctx_dev(link.y, 1 - link.k))


def scatter_y(link, src, dst):
    for j in range(1, link.z.ys):
        to = lax.rem(link.y + j, link.z.ys)
        link.put(src.at[to], dst.at[j - 1], link.ctx_dev(to, link.k))


class Cargo(Link):
    def put(self, src, dst, device):
        n = self.sent
        self.sent += 1
        copy = pltpu.make_async_remote_copy(
            src_ref=src,
            dst_ref=dst,
            send_sem=self.sems[0].at[n],
            recv_sem=self.sems[1].at[n],
            device_id=device,
            device_id_type=MESH,
        )
        self.inflight.append(copy)
        return copy


def fused_call(z, name, cid, body, grid, in_specs, out_specs, out_shape, args, script, moved, new=(), filled=(), scratch=()):
    filled, moved = tuple(filled), tuple(moved)
    n_arg, n_moved, n_fill = len(args), len(moved), len(filled)
    n_cargo = n_fill + len(new)
    n_out = n_cargo + len(out_shape)
    steps = 1
    for extent in grid:
        steps *= extent

    def kernel(*refs):
        step = 0
        for axis, extent in enumerate(grid):
            step = step * extent + pl.program_id(axis)
        n_in = n_arg + n_moved + n_fill
        arg_refs, moved_refs = refs[:n_arg], refs[n_arg : n_arg + n_moved]
        cargo_refs, out_refs = refs[n_in : n_in + n_cargo], refs[n_in + n_cargo : n_in + n_out]
        send, recv = refs[n_in + n_out : n_in + n_out + 2]
        cargo = Cargo(z, send, recv, None)
        script(cargo, moved_refs, cargo_refs)

        @pl.when(step == 0)
        def _():
            cargo.barrier()
            for copy in cargo.inflight:
                copy.start()

        body(*arg_refs, *out_refs, *refs[n_in + n_out + 2 :])

        @pl.when(step == steps - 1)
        def _():
            for copy in cargo.inflight:
                copy.wait_recv()
            for copy in cargo.inflight:
                copy.wait_send()

    hbm = pl.BlockSpec(memory_space=pltpu.HBM)
    first = n_arg + n_moved
    return pl.pallas_call(
        kernel,
        name=name,
        grid=grid,
        in_specs=list(in_specs) + [hbm] * (n_moved + n_fill),
        out_specs=[hbm] * n_cargo + list(out_specs),
        out_shape=[sds(a.shape, a.dtype) for a in filled] + list(new) + list(out_shape),
        input_output_aliases={first + n: n for n in range(n_fill)},
        scratch_shapes=[pltpu.SemaphoreType.DMA((32,)), pltpu.SemaphoreType.DMA((32,))] + list(scratch),
        compiler_params=pltpu.CompilerParams(
            collective_id=cid, has_side_effects=True, vmem_limit_bytes=VMEM_LIMIT
        ),
    )(*args, *moved, *filled)


def ring_outer(link, slot_of, step):
    slot = slot_of(link.outer_from(step - 1) * link.z.inner + link.i)
    return link.put(slot, slot, link.dp_dev(link.outer_to(1), link.i))


def ring_columns(link, buf, step):
    slot = buf.at[pl.ds(link.outer_from(step - 1) * link.z.inner, link.z.inner)]
    return link.put(slot, slot, link.dp_dev(link.outer_to(1), link.i))


def pass_inner(link, slot_of, step):
    slot = slot_of(link.outer_from(step) * link.z.inner + link.i)
    for j in range(1, link.z.inner):
        link.put(slot, slot, link.dp_dev(link.o, link.inner_to(j)))


def pass_core(link, buf, parts):
    for j in range(1, link.z.ys):
        at = lax.rem(link.y + link.z.ys - j, link.z.ys)
        for part in parts:
            src, dst = buf.at[link.slot(at, True), part], buf.at[link.slot_across(at, True), part]
            link.put(src, dst, link.ctx_dev(link.y, 1 - link.k))


def own_y(link, src, buf, parts):
    for part in parts:
        slot = buf.at[link.slot(link.y, True), part]
        for j in range(1, link.z.ys):
            to = lax.rem(link.y + j, link.z.ys)
            link.put(src.at[part], slot, link.ctx_dev(to, link.k))
        slot = buf.at[link.slot_across(link.y, True), part]
        link.put(src.at[part], slot, link.ctx_dev(link.y, 1 - link.k))


def turns(table):
    half = LANES // 2
    cos, sin = table[:, :half], table[:, half:]
    return jnp.concatenate([cos, cos], axis=1), jnp.concatenate([-sin, sin], axis=1)


def rotated(u, cos, sin):
    return u * cos + pltpu.roll(u, LANES // 2, 1) * sin


def qkv_kernel(hc, kvc, x_ref, gain_ref, w_ref, table_ref, n_ref, q_ref, k_ref, v_ref):
    x = x_ref[0, 0].astype(F32)
    scale = lax.rsqrt(jnp.mean(x * x, axis=-1, keepdims=True) + EPS)
    normed = (x * scale * gain_ref[...]).astype(BF)
    n_ref[0, 0] = normed
    full = dot_nn(normed, w_ref[...])
    cos, sin = turns(table_ref[0])
    for h in range(hc + kvc):
        piece = rotated(full[:, h * LANES : (h + 1) * LANES], cos, sin).astype(BF)
        if h < hc:
            q_ref[0, 0, :, h * LANES : (h + 1) * LANES] = piece
        else:
            k_ref[0, 0, :, (h - hc) * LANES : (h - hc + 1) * LANES] = piece
    v_ref[0, 0] = full[:, (hc + kvc) * LANES :].astype(BF)


def qkv_call(z, x_all, gain, w, positions, hc, kvc, script, moved, new, filled):
    ctx, m, r, d = x_all.shape
    row = lambda s, b: (s, b, 0, 0)
    whole = lambda s, b: (0, 0)
    table = pl.BlockSpec((1, r, LANES), lambda s, b: (s, 0, 0))
    return fused_call(
        z,
        "qkv",
        11,
        functools.partial(qkv_kernel, hc, kvc),
        (ctx, m),
        [
            pl.BlockSpec((1, 1, r, d), row),
            pl.BlockSpec((1, d), whole),
            pl.BlockSpec(w.shape, whole, pipeline_mode=pl.Buffered(1)),
            table,
        ],
        [
            pl.BlockSpec((1, 1, r, d), row),
            pl.BlockSpec((1, 1, r, hc * LANES), row),
            pl.BlockSpec((1, 1, r, kvc * LANES), row),
            pl.BlockSpec((1, 1, r, kvc * LANES), row),
        ],
        [
            sds((ctx, m, r, d)),
            sds((ctx, m, r, hc * LANES)),
            sds((ctx, m, r, kvc * LANES)),
            sds((ctx, m, r, kvc * LANES)),
        ],
        (x_all, gain, w, positions),
        script,
        moved,
        new,
        filled,
    )


def window_of(s, r, ctx):
    blocks = min(ctx, SPAN // r + 1)
    return jnp.maximum(s - (blocks - 1), 0), blocks


def bias_of(s, first, blocks, r, qdoc_ref, kdoc_ref):
    qdoc = qdoc_ref[0, 0]
    pieces = []
    for b in range(blocks):
        kdoc = kdoc_ref[first + b, 0]
        rows = lax.broadcasted_iota(jnp.int32, (r, r), 0) + s * r
        cols = lax.broadcasted_iota(jnp.int32, (r, r), 1) + (first + b) * r
        pieces.append(jnp.where((qdoc == kdoc) & (cols <= rows), 0.0, MASKED))
    return jnp.concatenate(pieces, axis=1)


def attend_kernel(hc, kvc, ctx, q_ref, k_ref, v_ref, qdoc_ref, kdoc_ref, out_ref, lse_ref):
    s = pl.program_id(1)
    r = q_ref.shape[2]
    first, blocks = window_of(s, r, ctx)
    bias = bias_of(s, first, blocks, r, qdoc_ref, kdoc_ref)
    lane = lax.broadcasted_iota(jnp.int32, (r, LANES), 1)
    lse_all = jnp.zeros((r, LANES), F32)
    outs = []
    for h in range(hc):
        g = h * kvc // hc
        q = q_ref[0, 0, :, h * LANES : (h + 1) * LANES]
        k = k_ref[pl.ds(first, blocks), 0, :, g * LANES : (g + 1) * LANES].reshape(blocks * r, LANES)
        v = v_ref[pl.ds(first, blocks), 0, :, g * LANES : (g + 1) * LANES].reshape(blocks * r, LANES)
        scores = dot_nt(q, k) * HD ** (-0.5) + bias
        top = jnp.max(scores, axis=-1, keepdims=True)
        e = jnp.exp(scores - top)
        total = jnp.sum(e, axis=-1, keepdims=True)
        probs = (e * (1.0 / total)).astype(BF)
        outs.append(dot_nn(probs, v)[:, :HD])
        lse_all = jnp.where(lane == h, top + jnp.log(total), lse_all)
    out_ref[0, 0] = jnp.concatenate(outs, axis=1).astype(BF)
    lse_ref[0, 0] = lse_all


def attend_call(z, q, k, v, qdoc, kdoc, hc, kvc, script, moved, new, filled):
    ctx, m, r, _ = q.shape
    row = lambda b, s: (s, b, 0, 0)
    seq = lambda b, s: (0, b, 0, 0)
    return fused_call(
        z,
        "attend",
        12,
        functools.partial(attend_kernel, hc, kvc, ctx),
        (m, ctx),
        [
            pl.BlockSpec((1, 1, r, hc * LANES), row),
            pl.BlockSpec((ctx, 1, r, kvc * LANES), seq),
            pl.BlockSpec((ctx, 1, r, kvc * LANES), seq),
            pl.BlockSpec((1, 1, r, 1), row),
            pl.BlockSpec((ctx, 1, 1, r), seq),
        ],
        [pl.BlockSpec((1, 1, r, hc * HD), row), pl.BlockSpec((1, 1, r, LANES), row)],
        [sds((ctx, m, r, hc * HD)), sds((ctx, m, r, LANES), F32)],
        (q, k, v, qdoc, kdoc),
        script,
        moved,
        new,
        filled,
    )


def attend_back_kernel(
    hc, kvc, ctx, q_ref, k_ref, v_ref, qdoc_ref, kdoc_ref, o_ref, do_ref, lse_ref, table_ref,
    dq_ref, dkv_ref, dk_acc, dv_acc,
):
    s = pl.program_id(1)
    r = q_ref.shape[2]
    first, blocks = window_of(s, r, ctx)
    bias = bias_of(s, first, blocks, r, qdoc_ref, kdoc_ref)

    @pl.when(s == 0)
    def _():
        dk_acc[...] = jnp.zeros_like(dk_acc)
        dv_acc[...] = jnp.zeros_like(dv_acc)

    cos, sin = turns(table_ref[s])
    lse_all = lse_ref[0, 0]
    for h in range(hc):
        g = h * kvc // hc
        q = q_ref[0, 0, :, h * LANES : (h + 1) * LANES]
        k = k_ref[pl.ds(first, blocks), 0, :, g * LANES : (g + 1) * LANES].reshape(blocks * r, LANES)
        v = v_ref[pl.ds(first, blocks), 0, :, g * LANES : (g + 1) * LANES].reshape(blocks * r, LANES)
        o = o_ref[0, 0, :, h * HD : (h + 1) * HD].astype(F32)
        do = do_ref[0, 0, :, h * HD : (h + 1) * HD]
        delta = jnp.sum(o * do.astype(F32), axis=-1, keepdims=True)
        do = jnp.concatenate([do, jnp.zeros((r, LANES - HD), BF)], axis=1)
        scores = dot_nt(q, k) * HD ** (-0.5) + bias
        probs = jnp.exp(scores - lse_all[:, h : h + 1])
        d_probs = dot_nt(do, v)
        d_scores = (probs * (d_probs - delta) * HD ** (-0.5)).astype(BF)
        dq = dot_nn(d_scores, k)
        dq_ref[0, 0, :, h * LANES : (h + 1) * LANES] = rotated(dq, cos, -sin).astype(BF)
        dk = dot_tn(d_scores, q).reshape(blocks, r, LANES)
        dv = dot_tn(probs.astype(BF), do).reshape(blocks, r, LANES)
        here = slice(g * LANES, (g + 1) * LANES)
        dk_acc[pl.ds(first, blocks), :, here] += dk
        dv_acc[pl.ds(first, blocks), :, here] += dv

    @pl.when(s == ctx - 1)
    def _():
        for b in range(ctx):
            cos_b, sin_b = turns(table_ref[b])
            for g in range(kvc):
                here = slice(g * LANES, (g + 1) * LANES)
                at = g * LANES
                dk = rotated(dk_acc[b, :, here], cos_b, -sin_b)
                dkv_ref[b, 0, :, at : at + LANES] = dk.astype(BF)
                at += kvc * LANES
                dkv_ref[b, 0, :, at : at + LANES] = dv_acc[b, :, here].astype(BF)


def attend_back_call(z, q, k, v, qdoc, kdoc, o, do, lse, positions, hc, kvc, script, moved, new, filled):
    ctx, m, r, _ = q.shape
    row = lambda b, s: (s, b, 0, 0)
    seq = lambda b, s: (0, b, 0, 0)
    table = pl.BlockSpec((ctx, r, LANES), lambda b, s: (0, 0, 0))
    return fused_call(
        z,
        "attend_back",
        14,
        functools.partial(attend_back_kernel, hc, kvc, ctx),
        (m, ctx),
        [
            pl.BlockSpec((1, 1, r, hc * LANES), row),
            pl.BlockSpec((ctx, 1, r, kvc * LANES), seq),
            pl.BlockSpec((ctx, 1, r, kvc * LANES), seq),
            pl.BlockSpec((1, 1, r, 1), row),
            pl.BlockSpec((ctx, 1, 1, r), seq),
            pl.BlockSpec((1, 1, r, hc * HD), row),
            pl.BlockSpec((1, 1, r, hc * HD), row),
            pl.BlockSpec((1, 1, r, LANES), row),
            table,
        ],
        [
            pl.BlockSpec((1, 1, r, hc * LANES), row),
            pl.BlockSpec((ctx, 1, r, 2 * kvc * LANES), seq),
        ],
        [sds((ctx, m, r, hc * LANES)), sds((ctx, m, r, 2 * kvc * LANES))],
        (q, k, v, qdoc, kdoc, o, do, lse, positions),
        script,
        moved,
        new,
        filled,
        [pltpu.VMEM((ctx, r, kvc * LANES), F32), pltpu.VMEM((ctx, r, kvc * LANES), F32)],
    )


def mix_kernel(ctx, att_ref, x_ref, gain_ref, w_ref, mid_ref, normed_ref, rows_ref):
    rows = jnp.concatenate([att_ref[c, 0] for c in range(ctx)], axis=1)
    rows_ref[0] = rows
    mid = x_ref[0].astype(F32) + dot_nn(rows, w_ref[...])
    mid_ref[0] = mid
    scale = lax.rsqrt(jnp.mean(mid * mid, axis=-1, keepdims=True) + EPS)
    normed_ref[0] = (mid * scale * gain_ref[...]).astype(BF)


def mix_call(z, att, x, gain, w, script, moved, new, filled):
    ctx, m, r, cols = att.shape
    d = x.shape[-1]
    seq = pl.BlockSpec((1, r, d), lambda b: (b, 0, 0))
    whole = lambda b: (0, 0)
    return fused_call(
        z,
        "mix",
        16,
        functools.partial(mix_kernel, ctx),
        (m,),
        [
            pl.BlockSpec((ctx, 1, r, cols), lambda b: (0, b, 0, 0)),
            seq,
            pl.BlockSpec((1, d), whole),
            pl.BlockSpec(w.shape, whole, pipeline_mode=pl.Buffered(1)),
        ],
        [seq, seq, seq],
        [sds((m, r, d), F32), sds((m, r, d)), sds((m, r, d))],
        (att, x, gain, w),
        script,
        moved,
        new,
        filled,
    )


def turn_kernel(z, dn_ref, *refs):
    came_refs = refs[: z.ys - 1]
    mid_ref, cot_ref, gain_ref, w_ref = refs[z.ys - 1 : z.ys + 3]
    d_mid_ref, low_ref, all_ref, hold, send_sems, recv_sems, own_sems = refs[z.ys + 3 :]
    b, last = pl.program_id(0), pl.num_programs(0) - 1
    link = Link(z, send_sems, recv_sems, own_sems)
    cols = hold.shape[-1]

    def copies(n):
        remote = [
            pltpu.make_async_remote_copy(
                src_ref=hold.at[p, n],
                dst_ref=all_ref.at[link.c, n],
                send_sem=send_sems.at[n, j],
                recv_sem=recv_sems.at[n, j],
                device_id=(link.d, p),
                device_id_type=MESH,
            )
            for j, p in enumerate(link.ctx_peers())
        ]
        return remote, pltpu.make_async_copy(hold.at[link.c, n], all_ref.at[link.c, n], own_sems.at[n])

    d_normed = dn_ref[link.y, 0].astype(F32)
    for ref in came_refs:
        d_normed += ref[0].astype(F32)
    mid = mid_ref[0]
    scale = lax.rsqrt(jnp.mean(mid * mid, axis=-1, keepdims=True) + EPS)
    e = d_normed * gain_ref[...]
    d_mid = cot_ref[0].astype(F32) + (
        scale * e - mid * (scale * scale * scale) * jnp.mean(e * mid, axis=-1, keepdims=True)
    )
    d_mid_ref[0] = d_mid
    low = d_mid.astype(BF)
    low_ref[0] = low
    d_att = dot_nt(low, w_ref[...]).astype(BF)
    for c in range(z.ctx):
        hold[c, b] = d_att[:, c * cols : (c + 1) * cols]
    remote, own = copies(b)
    for copy in remote:
        copy.start()
    own.start()

    @pl.when(b == last)
    def _():
        for n in range(hold.shape[1]):
            remote, own = copies(n)
            for copy in remote:
                copy.wait_recv()
            for copy in remote:
                copy.wait_send()
            own.wait()


def turn_call(z, dn, came, mid, cot, gain, w, cols, script, moved, new, filled):
    ys, m, r, d = dn.shape
    seq = pl.BlockSpec((1, r, d), lambda b: (b, 0, 0))
    whole = lambda b: (0, 0)
    return fused_call(
        z,
        "turn",
        6,
        functools.partial(turn_kernel, z),
        (m,),
        [pl.BlockSpec((ys, 1, r, d), lambda b: (0, b, 0, 0))]
        + [seq] * (ys + 1)
        + [pl.BlockSpec((1, d), whole), pl.BlockSpec(w.shape, whole, pipeline_mode=pl.Buffered(1))],
        [seq, seq, pl.BlockSpec(memory_space=pltpu.HBM)],
        [sds((m, r, d), F32), sds((m, r, d)), sds((z.ctx, m, r, cols))],
        (dn, *came, mid, cot, gain, w),
        script,
        moved,
        new,
        filled,
        [
            pltpu.VMEM((z.ctx, m, r, cols), BF),
            pltpu.SemaphoreType.DMA((m, z.ctx)),
            pltpu.SemaphoreType.DMA((m, z.ctx)),
            pltpu.SemaphoreType.DMA((m,)),
        ],
    )


def mlp_kernel(
    z, x_ref, cot_ref, gate_ref, up_ref, down_ref,
    hid_ref, dg_ref, du_ref, dn_ref, out_ref,
    dn_send, dn_got, out_send, out_got, send_sems, recv_sems,
):
    other, y, b = pl.program_id(0) == 0, pl.program_id(1), pl.program_id(2)
    link = Link(z, send_sems, recv_sems, None)
    at = y * pl.num_programs(2) + b

    def copies(n):
        return [
            pltpu.make_async_remote_copy(
                src_ref=src.at[n],
                dst_ref=dst.at[n],
                send_sem=send_sems.at[which, n],
                recv_sem=recv_sems.at[which, n],
                device_id=link.ctx_dev(link.y, 1 - link.k),
                device_id_type=MESH,
            )
            for which, (src, dst) in enumerate(((dn_send, dn_got), (out_send, out_got)))
        ]

    @pl.when(other & (at == 0))
    def _():
        link.barrier(core_only=True)

    x, cot = x_ref[0, 0], cot_ref[0, 0]
    gate, up = dot_nn(x, gate_ref[...]), dot_nn(x, up_ref[...])
    d_hidden = dot_nt(cot, down_ref[...])
    sg = jax.nn.sigmoid(gate)
    act = gate * sg
    hidden = (act * up).astype(BF)
    hid_ref[0, 0] = hidden
    d_gate = (d_hidden * up * sg * (1.0 + gate * (1.0 - sg))).astype(BF)
    d_up = (d_hidden * act).astype(BF)
    dg_ref[0, 0] = d_gate
    du_ref[0, 0] = d_up
    out = dot_nn(hidden, down_ref[...])
    dn = dot_nt(d_gate, gate_ref[...]) + dot_nt(d_up, up_ref[...])

    @pl.when(other)
    def _():
        dn_send[at] = dn.astype(BF)
        out_send[at] = out.astype(BF)
        for copy in copies(at):
            copy.start()

    @pl.when(jnp.logical_not(other))
    def _():
        for copy in copies(at):
            copy.wait_recv()
        dn_ref[0, 0] = (dn + dn_got[at].astype(F32)).astype(BF)
        out_ref[0, 0] = (out + out_got[at].astype(F32)).astype(BF)
        for copy in copies(at):
            copy.wait_send()


def mlp_call(z, x, cot, gate, up, down):
    ctx, m, r, d = x.shape
    f = down.shape[0]
    row = lambda a, y, b: (a * z.ys + y, b, 0, 0)
    whole = lambda a, y, b: (0, 0)
    mine = lambda a, y, b: (a * y, a * b, 0, 0)
    block = lambda width, at: pl.BlockSpec((1, 1, r, width), at)
    resident = lambda w: pl.BlockSpec(w.shape, whole, pipeline_mode=pl.Buffered(1))
    held = pltpu.VMEM((z.ys * m, r, d), BF)
    return pl.pallas_call(
        functools.partial(mlp_kernel, z),
        name="mlp",
        grid=(2, z.ys, m),
        in_specs=[block(d, row), block(d, row), resident(gate), resident(up), resident(down)],
        out_specs=[block(f, row), block(f, row), block(f, row), block(d, mine), block(d, mine)],
        scratch_shapes=[held] * 4
        + [pltpu.SemaphoreType.DMA((2, z.ys * m)), pltpu.SemaphoreType.DMA((2, z.ys * m))],
        out_shape=[sds((ctx, m, r, f))] * 3 + [sds((z.ys, m, r, d))] * 2,
        compiler_params=pltpu.CompilerParams(
            collective_id=13, has_side_effects=True, vmem_limit_bytes=VMEM_LIMIT
        ),
    )(x, cot, gate, up, down)


def tail_kernel(
    z, hc, dq_hbm, dkv_hbm, w_ref, q_ref, kv_ref, po_own, po_send, up_ref, gain_ref, gate_hbm,
    x_hbm, d_mid_hbm, mid_hbm, out_hbm, came_hbm,
    outputs_ref, grad_ref, po_out, q_out, kv_out, gate_out, up_out,
    dq, dkv, x, d_mid, mid, out_own, out_came, da_core, da_got, da_send, da_came,
    po_came, po_ref, q_x, q_col, q_z, kv_x, kv_col, kv_z, po_x, po_col, po_z, up_z, mine_q, mine_kv, mine_up,
    send_sems, recv_sems, local_sems,
):
    link = Link(z, send_sems, recv_sems, local_sems)
    link.landed = []
    wide = lambda a: a.astype(F32)
    ys, seqs, r = z.ys, x.shape[0], x.shape[1]
    half = dq.shape[-1]
    loads = [link.keep(dq_hbm, dq), link.keep(dkv_hbm, dkv)]
    later = [
        link.keep(x_hbm, x),
        link.keep(d_mid_hbm, d_mid),
        link.keep(mid_hbm, mid),
        link.keep(out_hbm.at[link.y], out_own),
        link.keep(came_hbm, out_came),
    ]
    link.barrier()

    def inner_puts(src, dst):
        return [
            link.put(src.at[:, link.inner_to(j)], dst.at[j - 1], link.dp_dev(link.o, link.inner_to(j)))
            for j in range(1, z.inner)
        ]

    def ring(col, got, step, copies):
        if copies:
            link.arrived(copies[-1])
            total = wide(got[step - 2]) + wide(col[link.outer_from(step)])
            if step == z.outer:
                return total
            got[step - 2] = total.astype(BF)
            src = got.at[step - 2]
        else:
            src = col.at[link.outer_from(1)]
        copies.append(link.put(src, got.at[step - 1], link.dp_dev(link.outer_to(1), link.i)))

    def columns(part, came, col, copies):
        for copy in copies:
            link.arrived(copy)
        for o in range(z.outer):
            total = wide(part[o, link.i])
            for j in range(z.inner - 1):
                total += wide(came[j, o])
            col[o] = total.astype(BF)

    up_way, q_way, kv_way, po_way = [], [], [], []
    ring(up_ref, up_z, 1, up_way)
    q_in = inner_puts(q_ref, q_x)
    exchange_ctx(link, gate_hbm, lambda s: gate_out.at[s])
    link.keep(gate_hbm.at[link.c], gate_out.at[link.c])
    po_y = []
    for j in range(1, ys):
        to = lax.rem(link.y + j, ys)
        po_y.append(link.put(po_send.at[j - 1], po_came.at[j - 1], link.ctx_dev(to, link.k)))
    for copy in loads:
        copy.wait()

    def home(mine, out):
        exchange_ctx(link, mine, lambda s: out.at[s])
        link.keep(mine.at[link.c], out.at[link.c])

    def da_of(place, b):
        left = dot_nt(dq[place, b], w_ref[:, :half])
        return left + dot_nt(dkv[place, b], w_ref[:, half:])

    core = []
    for y in range(ys):
        for b in range(seqs):
            da_core[y, b] = da_of(y * 2 + 1 - link.k, b).astype(BF)
            core.append(link.put(da_core.at[y, b], da_got.at[y, b], link.ctx_dev(link.y, 1 - link.k)))
    for copy in core:
        link.arrived(copy)
    for j in list(range(1, ys)) + [0]:
        y = lax.rem(link.y + j, ys)
        for b in range(seqs):
            total = da_of(y * 2 + link.k, b) + wide(da_got[y, b])
            if j == 0:
                grad_ref[b] = total
            else:
                da_send[j - 1, b] = total.astype(BF)
    ring(up_ref, up_z, 2, up_way)
    columns(q_ref, q_x, q_col, q_in)
    ring(q_col, q_z, 1, q_way)
    kv_in = inner_puts(kv_ref, kv_x)
    for copy in later:
        copy.wait()
    link.local = link.local[len(loads) + len(later) :]

    rows = 32 if r % 32 == 0 else r
    count = r // rows
    at_of = lambda step: (lax.div(step, count), pl.ds(pl.multiple_of(lax.rem(step, count) * rows, rows), rows))

    def finish_outputs(step, _):
        b, at = at_of(step)
        total = mid[b, at] + wide(out_own[b, at])
        for j in range(ys - 1):
            total += wide(out_came[j, b, at])
        outputs_ref[b, at] = total
        return 0

    lax.fori_loop(0, seqs * count, finish_outputs, 0)
    for step in range(3, z.outer):
        ring(up_ref, up_z, step, up_way)
    for copy in po_y:
        link.arrived(copy)
    y_ways = []
    for j in range(1, ys):
        to = lax.rem(link.y + j, ys)
        y_ways.append(link.put(da_send.at[j - 1], da_came.at[j - 1], link.ctx_dev(to, link.k)))
    for o in range(z.outer):
        total = wide(po_own[o])
        for j in range(ys - 1):
            total += wide(po_came[j, o])
        po_ref[o] = total.astype(BF)
    ring(q_col, q_z, 2, q_way)
    mine_up[...] = ring(up_ref, up_z, z.outer, up_way).astype(BF)
    home(mine_up, up_out)
    for step in range(3, z.outer):
        ring(q_col, q_z, step, q_way)
    columns(kv_ref, kv_x, kv_col, kv_in)
    ring(kv_col, kv_z, 1, kv_way)
    po_in = inner_puts(po_ref, po_x)
    mine_q[...] = ring(q_col, q_z, z.outer, q_way).astype(BF)
    home(mine_q, q_out)
    ring(kv_col, kv_z, 2, kv_way)
    columns(po_ref, po_x, po_col, po_in)
    ring(po_col, po_z, 1, po_way)
    for step in range(3, z.outer + 1):
        if step < z.outer:
            ring(kv_col, kv_z, step, kv_way)
        else:
            mine_kv[...] = ring(kv_col, kv_z, step, kv_way).astype(BF)
            home(mine_kv, kv_out)
        ring(po_col, po_z, step - 1, po_way)
    for copy in y_ways:
        link.arrived(copy)
    gain = gain_ref[...]

    def finish_grad(step, _):
        b, at = at_of(step)
        total = grad_ref[b, at]
        for j in range(ys - 1):
            total += wide(da_came[j, b, at])
        value = wide(x[b, at])
        scale = lax.rsqrt(jnp.mean(value * value, axis=-1, keepdims=True) + EPS)
        e = total * gain
        grad_ref[b, at] = d_mid[b, at] + (
            scale * e - value * (scale * scale * scale) * jnp.mean(e * value, axis=-1, keepdims=True)
        )
        return 0

    lax.fori_loop(0, seqs * count, finish_grad, 0)
    po_out[...] = ring(po_col, po_z, z.outer, po_way)
    link.finish()


def tail_call(z, hc, dq, dkv, w, part_q, part_kv, po, po_send, up_col, gain, gate_mine, x, d_mid, mid, out_pair, out_came):
    m, r, d = x.shape
    one = lambda a: a.shape[2:]
    q1, kv1, po1, up1 = one(part_q), one(part_kv), one(po), up_col.shape[1:]
    vm = lambda shape, dtype=BF: pltpu.VMEM(tuple(shape), dtype)
    hbm, vmem = pl.BlockSpec(memory_space=pltpu.HBM), pl.BlockSpec(memory_space=pltpu.VMEM)
    scratch = [vm(dq.shape), vm(dkv.shape), vm(x.shape), vm(x.shape, F32), vm(x.shape, F32), vm(x.shape)]
    scratch += [vm((z.ys - 1,) + x.shape), vm((z.ys,) + x.shape), vm((z.ys,) + x.shape)]
    scratch += [vm((z.ys - 1,) + x.shape), vm((z.ys - 1,) + x.shape)]
    scratch += [vm(po_send.shape), vm(po.shape)]
    for shape in (q1, kv1, po1):
        scratch += [vm((z.inner - 1, z.outer) + shape), vm((z.outer,) + shape), vm((z.outer - 1,) + shape)]
    scratch += [vm((z.outer - 1,) + up1), vm(q1), vm(kv1), vm(up1)]
    scratch += [
        pltpu.SemaphoreType.DMA((64,)),
        pltpu.SemaphoreType.DMA((64,)),
        pltpu.SemaphoreType.DMA((16,)),
    ]
    return pl.pallas_call(
        functools.partial(tail_kernel, z, hc),
        name="tail",
        in_specs=[hbm, hbm] + [vmem] * 7 + [hbm] * 6,
        out_specs=[vmem, vmem, vmem, hbm, hbm, hbm, hbm],
        out_shape=[
            sds(x.shape, F32),
            sds(x.shape, F32),
            sds(po1, F32),
            sds(q1),
            sds(kv1),
            sds(gate_mine.shape),
            sds(up1),
        ],
        scratch_shapes=scratch,
        compiler_params=pltpu.CompilerParams(
            collective_id=15, has_side_effects=True, vmem_limit_bytes=VMEM_LIMIT
        ),
    )(dq, dkv, w, part_q, part_kv, po, po_send, up_col, gain, gate_mine, x, d_mid, mid, out_pair, out_came)


def pad_heads(w, heads, split):
    rows = w.shape[0]
    if split:
        w = jnp.pad(w.reshape(rows, heads, 2, HALF), ((0, 0), (0, 0), (0, 0), (0, LANES // 2 - HALF)))
    else:
        w = jnp.pad(w.reshape(rows, heads, HD), ((0, 0), (0, 0), (0, LANES - HD)))
    return w.reshape(rows, heads * LANES)


def unpad_heads(w, heads, split):
    if split:
        w = w.reshape(w.shape[:-1] + (heads, 2, LANES // 2))[..., :HALF]
    else:
        w = w.reshape(w.shape[:-1] + (heads, LANES))[..., :HD]
    return w.reshape(w.shape[: w.ndim - (3 if split else 2)] + (heads * HD,))


def rope_table(ctx, r):
    frequency = THETA ** (-(jnp.arange(HALF, dtype=F32) * (2.0 / HD)))
    angles = jnp.arange(ctx * r, dtype=jnp.int32).astype(F32)[:, None] * frequency[None, :]
    pad = ((0, 0), (0, LANES // 2 - HALF))
    table = jnp.concatenate([jnp.pad(jnp.cos(angles), pad), jnp.pad(jnp.sin(angles), pad)], axis=1)
    return table.reshape(ctx, r, LANES)


def per_device(
    inputs, segments, cotangent, w_query, w_key, w_value, w_out, w_gate, w_up, w_down, gain_attn, gain_ffn
):
    z = Sizes(lax.axis_size("dp"), lax.axis_size("ctx"))
    dp, ctx, outer, inner, ys = z.dp, z.ctx, z.outer, z.inner, z.ys
    m, r, d = inputs.shape
    rows = w_query.shape[0]
    frows, ff = w_down.shape[0], w_gate.shape[1]
    f = ff // ctx
    hc, kvc = H // ctx, KV // ctx
    width = (hc + 2 * kvc) * LANES
    c = lax.axis_index("ctx")
    di = lax.axis_index("dp")
    oi, ii = di // inner, di % inner
    yi, ki = c // 2, c % 2
    dyn = lambda a, at, axis: lax.dynamic_index_in_dim(a, at, axis, keepdims=False)

    pack_qkv = jnp.concatenate(
        [
            pad_heads(w_query, H, True).reshape(rows, ctx, hc * LANES),
            pad_heads(w_key, KV, True).reshape(rows, ctx, kvc * LANES),
            pad_heads(w_value, KV, False).reshape(rows, ctx, kvc * LANES),
        ],
        axis=2,
    ).transpose(1, 0, 2)
    by_rank = lambda w: w.reshape(rows, dp, ctx, frows).transpose(2, 0, 1, 3).reshape(ctx, rows, f)
    pack_gate, pack_up = by_rank(w_gate), by_rank(w_up)
    gains = jnp.stack([gain_attn, gain_ffn]).astype(F32)
    gains = jnp.pad(gains, ((0, 6), (0, LANES - rows)))

    steps = list(range(1, outer))
    by_owner = lambda buf: lambda s: buf.at[s]
    out_slot = lambda link, buf: lambda s: buf.at[s, :, link.k]

    def first_script(link, ins, outs, scratch):
        x, seg, qkv, gain, wo, pg, pu, wd = ins
        x_all, seg_all, g_qkv, g_gain, g_out, g_gate, g_up, g_down = outs
        (hold,) = scratch
        load = pltpu.make_async_copy(x, hold, link.sems[2].at[15])
        load.start()
        mine = [
            link.keep(qkv.at[link.c], g_qkv.at[link.d, link.c]),
            link.keep(gain, g_gain.at[link.d, link.c]),
            link.keep(wo, g_out.at[link.d, link.y, link.k]),
            link.keep(seg, seg_all.at[link.c]),
        ]
        a2a = exchange_ctx(link, qkv, lambda s: g_qkv.at[link.d, s])
        a2a += [link.put(gain, g_gain.at[link.d, link.c], (link.d, p)) for p in link.ctx_peers()]
        for p in link.ctx_peers():
            link.put(seg, seg_all.at[link.c], (link.d, p))
        over_y = [
            link.put(wo, g_out.at[link.d, link.y, link.k], link.ctx_dev(p, link.k)) for p in link.y_peers()
        ]
        ways_x = gather_ctx_start(link, x, x_all)
        exchange_ctx(link, pg, lambda s: g_gate.at[link.d, s])
        for copy in a2a:
            link.arrived(copy)
        for copy in mine:
            copy.wait()
        link.local = []
        split = ctx // 2
        small = [lambda s: g_qkv.at[s, :split], lambda s: g_qkv.at[s, split:], by_owner(g_gain)]
        ways = [ring_outer(link, slot, 1) for slot in small]
        for slot in small:
            pass_inner(link, slot, 0)
        link.keep(pg.at[link.c], g_gate.at[link.d, link.c])
        link.keep(pu.at[link.c], g_up.at[link.d, link.c])
        link.keep(wd, g_down.at[link.d])
        load.wait()
        store = pltpu.make_async_copy(hold, x_all.at[link.c], link.sems[2].at[14])
        store.start()
        for step in steps:
            came, ways = ways, []
            for copy, slot in zip(came, small):
                link.arrived(copy)
                if step < steps[-1]:
                    ways.append(ring_outer(link, slot, step + 1))
                pass_inner(link, slot, step)
        for copy in over_y:
            link.arrived(copy)
        ring_outer(link, out_slot(link, g_out), 1)
        pass_inner(link, out_slot(link, g_out), 0)
        gather_ctx_forward(link, x_all, ways_x)
        store.wait()

    x_all, seg_all, g_qkv, g_gain, g_out, g_gate, g_up, g_down = communicate(
        z,
        "gather_first",
        1,
        first_script,
        (inputs, segments, pack_qkv, gains, w_out, pack_gate, pack_up, w_down),
        (
            sds((ctx, m, r, d)),
            sds((ctx, m, r), jnp.int32),
            sds((dp, ctx, rows, width)),
            sds((dp, ctx, 8, LANES), F32),
            sds((dp, ys, 2, rows, d)),
            sds((dp, ctx, rows, f)),
            sds((dp, ctx, rows, f)),
            sds((dp, frows, d)),
        ),
        [pltpu.VMEM((m, r, d), BF)],
    )
    gain_a = g_gain[:, :, 0, :rows].reshape(1, d)
    gain_f = g_gain[:, :, 1, :rows].reshape(1, d)
    wqkv = g_qkv.reshape(d, width)
    table = rope_table(ctx, r)
    qdoc = seg_all.reshape(ctx, m, r, 1)
    kdoc = seg_all.reshape(ctx, m, 1, r)
    early, late = range(m // 2), range(m // 2, m)

    def qkv_cargo(cargo, moved, bufs):
        (pu,), (g_out, g_gate, g_up) = moved, bufs
        exchange_ctx(cargo, pu, lambda s: g_up.at[cargo.d, s])
        for slot, step in ((out_slot(cargo, g_out), 2), (by_owner(g_gate), 1)):
            ring_outer(cargo, slot, step)
            pass_inner(cargo, slot, step - 1)

    g_out, g_gate, g_up, normed_a, q, k, v = qkv_call(
        z, x_all, gain_a, wqkv, table, hc, kvc,
        qkv_cargo, (pack_up,), (), (g_out, g_gate, g_up),
    )

    def attend_cargo(cargo, moved, bufs):
        (cot,), (g_out, g_gate, g_up, cot_all) = moved, bufs
        own_y(cargo, cot, cot_all, early)
        for slot, step in ((out_slot(cargo, g_out), 3), (by_owner(g_gate), 2), (by_owner(g_up), 1)):
            ring_outer(cargo, slot, step)
            pass_inner(cargo, slot, step - 1)

    g_out, g_gate, g_up, cot_all, att, lse = attend_call(
        z, q, k, v, qdoc, kdoc, hc, kvc, attend_cargo, (cotangent,), (sds((ctx, m, r, d)),), (g_out, g_gate, g_up)
    )

    def second_script(link, ins, outs, scratch):
        att, cot = ins[:2]
        g_out, g_gate, g_up, g_down, cot_all, att_all = outs
        (hold,) = scratch
        load = pltpu.make_async_copy(cot, hold, link.sems[2].at[15])
        load.start()
        link.keep(att.at[link.c], att_all.at[link.c])
        first = len(link.inflight)
        pass_inner(link, out_slot(link, g_out), 3)
        last_out = link.inflight[first:]
        exchange_ctx(link, att, lambda s: att_all.at[s])
        for slot, step in ((by_owner(g_gate), 3), (by_owner(g_up), 2)):
            ring_outer(link, slot, step)
        pass_inner(link, by_owner(g_gate), 2)
        pass_inner(link, by_owner(g_down), 0)
        pass_core(link, cot_all, early)
        load.wait()
        store = pltpu.make_async_copy(hold, cot_all.at[link.slot(link.y, True)], link.sems[2].at[14])
        store.start()
        for copy in last_out:
            link.arrived(copy)
        both = g_out.at[:, :, link.k]
        link.put(both, both, link.ctx_dev(link.y, 1 - link.k))
        store.wait()

    g_out, g_gate, g_up, g_down, cot_all, att_all = communicate(
        z,
        "exchange_heads",
        2,
        second_script,
        (att, cotangent),
        (sds(att.shape),),
        [pltpu.VMEM((m, r, d), BF)],
        (g_out, g_gate, g_up, g_down, cot_all),
    )
    wo = g_out.reshape(d, d)

    def mix_cargo(cargo, moved, bufs):
        (cot,), (g_gate, g_up, g_down, cot_all) = moved, bufs
        own_y(cargo, cot, cot_all, late)
        ring_outer(cargo, by_owner(g_up), 3)
        ring_columns(cargo, g_down, 1)
        pass_inner(cargo, by_owner(g_gate), 3)
        pass_inner(cargo, by_owner(g_up), 1)

    g_gate, g_up, g_down, cot_all, mid, normed, att_rows = mix_call(
        z, att_all, inputs, gain_f, wo, mix_cargo, (cotangent,), (), (g_gate, g_up, g_down, cot_all)
    )
    att_rows = att_rows.reshape(m * r, H * HD)

    def third_script(link, ins, outs, scratch):
        x, (g_up, g_down, cot_all, x_all), (hold,) = ins[0], outs, scratch
        load = pltpu.make_async_copy(x, hold, link.sems[2].at[15])
        load.start()
        ways = gather_ctx_start(link, x, x_all, True)
        way = ring_columns(link, g_down, 2)
        pass_inner(link, by_owner(g_up), 2)
        pass_inner(link, by_owner(g_up), 3)
        pass_core(link, cot_all, late)
        load.wait()
        store = pltpu.make_async_copy(hold, x_all.at[link.slot(link.y, True)], link.sems[2].at[14])
        store.start()
        for step in steps[2:]:
            link.arrived(way)
            way = ring_columns(link, g_down, step)
        gather_ctx_forward(link, x_all, ways, True)
        store.wait()

    g_up, g_down, cot_all, normed_all = communicate(
        z,
        "gather_third",
        3,
        third_script,
        (normed,),
        (sds((ctx, m, r, d)),),
        [pltpu.VMEM((m, r, d), BF)],
        (g_up, g_down, cot_all),
    )
    w_gate_c, w_up_c, w_down_c = g_gate.reshape(d, f), g_up.reshape(d, f), g_down.reshape(f, d)

    hidden, d_gate, d_up, dn_pair, out_pair = mlp_call(z, normed_all, cot_all, w_gate_c, w_up_c, w_down_c)

    dp_perm = lambda fn: [(o * inner + i, fn(o, i)) for o in range(outer) for i in range(inner)]
    ctx_perm = lambda fn: [(y * 2 + k, fn(y, k)) for y in range(ys) for k in range(2)]
    wide = lambda a: a.astype(F32)
    flat = lambda a: a.reshape(ctx * m * r, a.shape[-1])

    def after(a, dep):
        return lax.optimization_barrier((a, dep))[0]

    def to_core(a):
        return lax.ppermute(a, "ctx", ctx_perm(lambda y, k: y * 2 + 1 - k))

    def to_y(pair):
        return [
            lax.ppermute(
                dyn(pair, (yi + j) % ys, 0), "ctx", ctx_perm(lambda y, k: (y + j) % ys * 2 + k)
            )
            for j in range(1, ys)
        ]

    def to_inner(part):
        return [
            lax.ppermute(
                dyn(part, (ii + j) % inner, 1), "dp", dp_perm(lambda o, i: o * inner + (i + j) % inner)
            )
            for j in range(1, inner)
        ]

    column = lambda part, came: (wide(dyn(part, ii, 1)) + sum(wide(a) for a in came)).astype(BF)
    close = lambda own, came: wide(own) + sum(wide(a) for a in came)

    dn_send = [dyn(dn_pair, (yi + j) % ys, 0) for j in range(1, ys)]
    dn_came = [
        lax.ppermute(a, "ctx", ctx_perm(lambda y, k: (y + j) % ys * 2 + k)) for j, a in enumerate(dn_send, 1)
    ]
    part_down = dot_tn(flat(after(hidden, dn_send)), flat(cot_all)).astype(BF).reshape(outer, inner, frows, d)
    par = oi % 2

    def by_parity(part):
        part = part.reshape((outer // 2, 2) + part.shape[1:])
        return dyn(part, 1 - par, 1), dyn(part, par, 1)

    down_near, down_rest = by_parity(part_down)
    near_x = to_inner(down_near)
    rest_x = to_inner(down_rest)
    shape_g = (outer, inner, ctx, rows, f)
    part_gate = dot_tn(flat(normed_all), flat(d_gate)).astype(BF).reshape(shape_g)
    gate_near, gate_rest = by_parity(part_gate)
    gate_near_x = to_inner(gate_near)
    gate_rest_x = to_inner(after(gate_rest, near_x))
    part_up = dot_tn(flat(normed_all), flat(after(d_up, part_gate))).astype(BF).reshape(shape_g)
    near = [j for j in steps if j in (1, outer - 1)]
    mid_way = [j for j in steps if j not in near]
    near_col = column(down_near, after(near_x, part_up))

    def to_near(link, col, dst):
        for j in near:
            to = link.outer_to(j)
            link.put(col.at[lax.div(to, 2)], dst.at[j - 1], link.dp_dev(to, link.i))

    def to_rest(link, col, dst):
        for j in mid_way:
            to = link.outer_to(j)
            link.put(col.at[lax.div(to, 2)], dst.at[j - 1], link.dp_dev(to, link.i))

    def turn_cargo(cargo, moved, bufs):
        to_near(cargo, moved[0], bufs[0])

    down_z, d_mid, d_mid_low, d_att_all = turn_call(
        z, dn_pair, dn_came, mid, cotangent, gain_f, wo, hc * HD,
        turn_cargo, (near_col,), (sds((outer - 1, frows, d)),), (),
    )

    part_out = dot_tn(att_rows, d_mid_low.reshape(m * r, d)).astype(BF).reshape(dp, ys, 2, rows, d)
    rest_col = column(down_rest, after(rest_x, d_att_all))
    gate_near_col = column(gate_near, after(gate_near_x, d_att_all))

    def back_cargo(cargo, moved, bufs):
        (rest_col, gate_near_col, part_up, part_out, out_pair), (down_z, gate_z, up_x, po_in, out_came) = moved, bufs
        scatter_y(cargo, out_pair, out_came)
        scatter_inner(cargo, part_up, up_x)
        to_rest(cargo, rest_col, down_z)
        to_near(cargo, gate_near_col, gate_z)
        cargo.put(part_out.at[:, :, 1 - cargo.k], po_in, cargo.ctx_dev(cargo.y, 1 - cargo.k))

    down_z, gate_z, up_x, po_in, out_came, dq, dkv = attend_back_call(
        z, q, k, v, qdoc, kdoc, att, d_att_all, lse, table, hc, kvc,
        back_cargo,
        (rest_col, gate_near_col, part_up, part_out, out_pair),
        (
            sds((outer - 1,) + gate_near_col.shape[1:]),
            sds((inner - 1, outer) + gate_near_col.shape[1:]),
            sds((dp, ys, rows, d)),
            sds((ys - 1, m, r, d)),
        ),
        (down_z,),
    )
    po_both = lambda at: wide(dyn(dyn(part_out, ki, 2), at, 1)) + wide(dyn(po_in, at, 1))
    po_send = jnp.stack([po_both((yi + j) % ys).astype(BF) for j in range(1, ys)])
    po_send = po_send.reshape(ys - 1, outer, inner, rows, d)
    gate_rest_col = column(gate_rest, after(gate_rest_x, dq))
    gate_far = [
        lax.ppermute(
            dyn(gate_rest_col, (oi + j) % outer // 2, 0), "dp", dp_perm(lambda o, i: (o + j) % outer * inner + i)
        )
        for j in mid_way
    ]
    part_q = dot_tn(flat(normed_a), flat(dq)).astype(BF).reshape(outer, inner, ctx, rows, hc * LANES)
    part_kv = dot_tn(flat(normed_a), flat(dkv)).astype(BF).reshape(outer, inner, ctx, rows, 2 * kvc * LANES)
    up_col = column(part_up, [up_x[j] for j in range(inner - 1)])
    po = po_both(yi).astype(BF).reshape(outer, inner, rows, d)
    gate_mine = close(dyn(gate_rest_col, oi // 2, 0), [gate_z[j - 1] for j in near] + gate_far).astype(BF)

    outputs, input_grad, grad_out, q_all, kv_all, gate_all, up_all = tail_call(
        z, hc, dq, dkv, wqkv, part_q, part_kv, po, po_send, up_col, gain_a, gate_mine,
        inputs, d_mid, mid, out_pair, out_came,
    )
    grad_down = close(dyn(rest_col, oi // 2, 0), [down_z[j - 1] for j in steps])
    spread = lambda a: wide(a).reshape(ctx, rows, dp, frows).transpose(1, 2, 0, 3).reshape(rows, ff)
    grad_gate, grad_up = spread(gate_all), spread(up_all)
    cols = lambda a, heads, split: (
        unpad_heads(wide(a), heads, split).transpose(1, 0, 2).reshape(rows, ctx * heads * HD)
    )
    grad_query = cols(q_all, hc, True)
    grad_key = cols(kv_all[:, :, : kvc * LANES], kvc, True)
    grad_value = cols(kv_all[:, :, kvc * LANES :], kvc, False)

    along = lambda pairs, gain: sum(jnp.sum(wide(w) * g, axis=1) for w, g in pairs) / wide(gain)
    grad_gain_a = along(((w_query, grad_query), (w_key, grad_key), (w_value, grad_value)), gain_attn)
    grad_gain_f = along(((w_gate, grad_gate), (w_up, grad_up)), gain_ffn)
    return (
        outputs,
        input_grad,
        grad_query,
        grad_key,
        grad_value,
        grad_out,
        grad_gate,
        grad_up,
        grad_down,
        grad_gain_a,
        grad_gain_f,
    )


def solution(mesh):
    rows, vec, tok = P(("dp", "ctx"), None), P(("dp", "ctx")), P("dp", "ctx", None)
    return jax.shard_map(
        per_device,
        mesh=mesh,
        in_specs=(tok, P("dp", "ctx"), tok) + (rows,) * 7 + (vec, vec),
        out_specs=(tok, tok) + (rows,) * 7 + (vec, vec),
        check_vma=False,
    )
```
